32 devices in a mesh: dp: 4 (over y, z), tp: 8 (over x, core).
Axes of the slice: x: 4, y: 2, z: 2, core: 2. Of those that a mesh axis runs over, the one named last changes fastest.
The devices are a block of a 4x4x8 slice.
Arguments:
- token_ids: int32 [8, 2048], P('dp'), parts along dimension 0
- word_table: bfloat16 [51200, 3072], P('tp')
- pos_table: bfloat16 [2048, 3072], replicated
- ln_gain: float32 [3072], replicated
- ln_bias: float32 [3072], replicated
- w_qkv: bfloat16 [3072, 3, 32, 96], P(None, None, 'tp')
- b_qkv: float32 [3, 32, 96], P(None, 'tp')
- w_out: bfloat16 [32, 96, 3072], P('tp')
- b_out: float32 [3072], replicated
Outputs:
- output 1: bfloat16 [8, 2048, 3072], P('dp', 'tp'), parts along dimension 0
- output 2: bfloat16 [8, 2048, 3072], P('dp', 'tp'), parts along dimension 0
There are 4 independent parts. The reference program is written for one: setup_inputs(seed, part) draws one part's arguments, and reference() takes and returns one part's arrays. A program takes and returns all parts, laid end to end along the dimension named above; an argument that names none is the same for every part.
All inputs are finite; a program needn't handle non-finite values.
Results may differ from the reference program's by a relative error of at most 0.00775296.
Values are sent between devices in bfloat16 or wider.
A program may use at most 768 MiB of HBM per device.

```python
import math
import jax
import jax.numpy as jnp
from jax import lax

VOCAB_SIZE = 51200
MODEL_DIM = 3072
NUM_HEADS = 32
HEAD_DIM = 96
SEQ_LEN = 2048
GROUP_BATCH = 2
OCTAVES = math.ceil(math.log2(VOCAB_SIZE))
LN_EPS = 1e-5


def draw_token_ids(key):
    key_octave, key_rank, key_order = jax.random.split(key, 3)
    id_shape = (GROUP_BATCH, SEQ_LEN)
    octave = jax.random.randint(key_octave, id_shape, 0, OCTAVES + 1)
    rank_span = jnp.minimum(jnp.left_shift(jnp.ones(id_shape, jnp.int32), octave), VOCAB_SIZE)
    rank = jax.random.randint(key_rank, id_shape, 0, rank_span)
    vocab_order = jax.random.permutation(key_order, VOCAB_SIZE)
    return jnp.take(vocab_order, rank).astype(jnp.int32)


def setup_inputs(seed: int = 0, part: int = 0) -> dict:
    base_key = jax.random.key(seed)
    part_key = jax.random.fold_in(base_key, part)
    keys = jax.random.split(base_key, 8)
    token_ids = draw_token_ids(part_key)
    word_table = (0.8 * jax.random.normal(keys[0], (VOCAB_SIZE, MODEL_DIM), jnp.float32)).astype(jnp.bfloat16)
    pos_table = (0.6 * jax.random.normal(keys[1], (SEQ_LEN, MODEL_DIM), jnp.float32)).astype(jnp.bfloat16)
    ln_gain = 1.0 + 0.2 * jax.random.normal(keys[2], (MODEL_DIM,), jnp.float32)
    ln_bias = 0.2 * jax.random.normal(keys[3], (MODEL_DIM,), jnp.float32)
    qkv_scale = jnp.array([3.0 ** 0.5, 3.0 ** 0.5, 1.0], jnp.float32) * MODEL_DIM ** -0.5
    w_qkv = (jax.random.normal(keys[4], (MODEL_DIM, 3, NUM_HEADS, HEAD_DIM), jnp.float32) * qkv_scale[None, :, None, None]).astype(jnp.bfloat16)
    b_qkv = 0.3 * jax.random.normal(keys[5], (3, NUM_HEADS, HEAD_DIM), jnp.float32)
    w_out = (jax.random.normal(keys[6], (NUM_HEADS, HEAD_DIM, MODEL_DIM), jnp.float32) * (NUM_HEADS * HEAD_DIM) ** -0.5).astype(jnp.bfloat16)
    b_out = 0.3 * jax.random.normal(keys[7], (MODEL_DIM,), jnp.float32)
    return {"token_ids": token_ids, "word_table": word_table, "pos_table": pos_table, "ln_gain": ln_gain, "ln_bias": ln_bias, "w_qkv": w_qkv, "b_qkv": b_qkv, "w_out": w_out, "b_out": b_out}


def layer_norm(values, gain, bias):
    feat_mean = jnp.mean(values, axis=-1, keepdims=True)
    centered = values - feat_mean
    feat_variance = jnp.mean(centered * centered, axis=-1, keepdims=True)
    return centered * lax.rsqrt(feat_variance + LN_EPS) * gain + bias


def reference(token_ids, word_table, pos_table, ln_gain, ln_bias, w_qkv, b_qkv, w_out, b_out):
    table_rows = jnp.take(word_table, token_ids, axis=0).astype(jnp.float32)
    embed = (table_rows + pos_table.astype(jnp.float32)[None]).astype(jnp.bfloat16)
    normed = layer_norm(embed.astype(jnp.float32), ln_gain, ln_bias).astype(jnp.bfloat16)
    inner_width = NUM_HEADS * HEAD_DIM
    projected = jnp.dot(normed.reshape(GROUP_BATCH * SEQ_LEN, MODEL_DIM), w_qkv.reshape(MODEL_DIM, 3 * inner_width), preferred_element_type=jnp.float32)
    projected = (projected.reshape(GROUP_BATCH, SEQ_LEN, 3, NUM_HEADS, HEAD_DIM) + b_qkv).astype(jnp.bfloat16)
    heads_first = jnp.transpose(projected, (2, 0, 3, 1, 4)).reshape(3, GROUP_BATCH * NUM_HEADS, SEQ_LEN, HEAD_DIM)
    positions = jnp.arange(SEQ_LEN)
    causal_mask = positions[:, None] >= positions[None, :]

    def one_head(operands):
        query_h, key_h, value_h = operands
        attn_scores = jnp.dot(query_h, key_h.T, preferred_element_type=jnp.float32) * HEAD_DIM ** -0.5
        attn_scores = jnp.where(causal_mask, attn_scores, -jnp.inf)
        attn_probs = jax.nn.softmax(attn_scores, axis=-1).astype(jnp.bfloat16)
        return jnp.dot(attn_probs, value_h, preferred_element_type=jnp.float32).astype(jnp.bfloat16)

    context = lax.map(one_head, (heads_first[0], heads_first[1], heads_first[2]))
    context = context.reshape(GROUP_BATCH, NUM_HEADS, SEQ_LEN, HEAD_DIM)
    attn_out = jnp.einsum("bhse,hed->bsd", context.astype(jnp.float32), w_out.astype(jnp.float32))
    resid_out = (embed.astype(jnp.float32) + attn_out + b_out).astype(jnp.bfloat16)
    return resid_out, embed
```

```python
import functools

import jax
import jax.numpy as jnp
from jax import lax
from jax.experimental import pallas as pl
from jax.experimental.pallas import tpu as pltpu
from jax.sharding import PartitionSpec as P

MESH = pl.DeviceIdType.MESH


def gather_all_kernel(n, S, src_ref, all_ref, loc_sem, send_sem, recv_sem):
    cap = src_ref.shape[0]

    def of(d):
        return all_ref.at[pl.ds(d * cap, cap)]
    chips = n // 2
    me = lax.axis_index("tp")
    chip, core = me // 2, lax.rem(me, 2)
    def at(c):
        return lax.rem(c + chips, chips) * 2 + core
    plus, minus, opp = at(chip + 1), at(chip - 1), at(chip + 2)
    partner = me + 1 - 2 * core
    P = 2 * S
    step = src_ref.shape[0] // P

    barrier = pltpu.get_barrier_semaphore()
    for d in (plus, minus, partner):
        pl.semaphore_signal(barrier, inc=1, device_id={"tp": d}, device_id_type=MESH)
    pl.semaphore_wait(barrier, 3)

    started = []
    def rc(src, dst, ch, k, dev):
        return pltpu.make_async_remote_copy(src_ref=src, dst_ref=dst, send_sem=send_sem.at[ch, k], recv_sem=recv_sem.at[ch, k],
                                            device_id={"tp": dev}, device_id_type=MESH)
    def go(src, dst, ch, k, dev):
        c = rc(src, dst, ch, k, dev)
        c.start()
        started.append(c)
    def piece(ref, k):
        return ref.at[pl.ds(k * step, step)]
    first, last = list(range(S)), list(range(S, P))
    for a, b in zip(first, last):
        go(piece(src_ref, a), piece(of(me), a), 0, a, plus)
        go(piece(src_ref, b), piece(of(me), b), 1, b, minus)
    for a, b in zip(first, last):
        go(piece(src_ref, b), piece(of(me), b), 0, b, plus)
        go(piece(src_ref, a), piece(of(me), a), 1, a, minus)
    go(src_ref, of(me), 4, 0, partner)
    loc = pltpu.make_async_copy(src_ref, of(me), loc_sem)
    loc.start()
    def got(owner, ch, k):
        r = piece(of(owner), k)
        rc(r, r, ch, k, partner).wait_recv()
        return r
    for a, b in zip(first, last):
        r = got(minus, 0, a)
        go(r, r, 2, a, plus)
        go(r, r, 5, a, partner)
        r = got(plus, 1, b)
        go(r, r, 3, b, minus)
        go(r, r, 6, b, partner)
    for a, b in zip(first, last):
        r = got(minus, 0, b)
        go(r, r, 5, b, partner)
        r = got(plus, 1, a)
        go(r, r, 6, a, partner)
    for a, b in zip(first, last):
        r = got(opp, 2, a)
        go(r, r, 7, a, partner)
        r = got(opp, 3, b)
        go(r, r, 7, b, partner)
    other = lambda d: d + 1 - 2 * core
    r = of(partner)
    rc(r, r, 4, 0, partner).wait_recv()
    for k in range(P):
        got(other(minus), 5, k)
        got(other(plus), 6, k)
        got(other(opp), 7, k)
    loc.wait()
    for c in started:
        c.wait_send()


def gather_all(n, rows, total, S=2, cid=0):
    return pl.pallas_call(
        functools.partial(gather_all_kernel, n, S),
        out_shape=jax.ShapeDtypeStruct((total,) + rows.shape[1:], rows.dtype),
        in_specs=[pl.BlockSpec(memory_space=pltpu.VMEM)],
        out_specs=pl.BlockSpec(memory_space=pl.ANY),
        scratch_shapes=[pltpu.SemaphoreType.DMA, pltpu.SemaphoreType.DMA((8, 2 * S)), pltpu.SemaphoreType.DMA((8, 2 * S))],
        compiler_params=pltpu.CompilerParams(collective_id=cid, has_side_effects=True),
        name="gather_all",
    )(rows)


def exchange_kernel(n, src_ref, out_ref, loc_sem, send_sem, recv_sem):
    me = lax.axis_index("tp")
    barrier = pltpu.get_barrier_semaphore()
    for s in range(1, n):
        pl.semaphore_signal(barrier, inc=1, device_id={"tp": lax.rem(me + s, n)}, device_id_type=MESH)
    pl.semaphore_wait(barrier, n - 1)
    cs = []
    for s in range(1, n):
        to = lax.rem(me + s, n)
        c = pltpu.make_async_remote_copy(src_ref=src_ref.at[to], dst_ref=out_ref.at[me], send_sem=send_sem.at[s], recv_sem=recv_sem.at[s],
                                         device_id={"tp": to}, device_id_type=MESH)
        c.start()
        cs.append(c)
    loc = pltpu.make_async_copy(src_ref.at[me], out_ref.at[me], loc_sem)
    loc.start()
    loc.wait()
    for s in range(1, n):
        fr = lax.rem(me - s + n, n)
        r = out_ref.at[fr]
        pltpu.make_async_remote_copy(src_ref=r, dst_ref=r, send_sem=send_sem.at[s], recv_sem=recv_sem.at[s],
                                     device_id={"tp": fr}, device_id_type=MESH).wait_recv()
    for c in cs:
        c.wait_send()


def exchange(n, x, cid=1):
    return pl.pallas_call(
        functools.partial(exchange_kernel, n),
        out_shape=jax.ShapeDtypeStruct(x.shape, x.dtype),
        in_specs=[pl.BlockSpec(memory_space=pltpu.VMEM)],
        out_specs=pl.BlockSpec(memory_space=pl.ANY),
        scratch_shapes=[pltpu.SemaphoreType.DMA, pltpu.SemaphoreType.DMA((n,)), pltpu.SemaphoreType.DMA((n,))],
        compiler_params=pltpu.CompilerParams(collective_id=cid, has_side_effects=True),
        name="exchange",
    )(x)


SPAN = 8192


def index_kernel(n, shard_rows, cap, ids_ref, code_ref, list_ref, cnt_ref, col, wcol, first):
    me = lax.axis_index("tp")
    R, L = ids_ref.shape
    G = 8
    lane = lax.broadcasted_iota(jnp.int32, (8, L), 1)
    sub = lax.broadcasted_iota(jnp.int32, (8, L), 0)

    def spread(src, dst):
        @pl.loop(0, R)
        def _(a):
            row = jnp.broadcast_to(src[pl.ds(a, 1), :], (L, L))
            dst[pl.ds(pl.multiple_of(a * L, L), L), :] = row.T
    spread(ids_ref, col)

    for bg in range(R // G):
        rows = [jnp.broadcast_to(ids_ref[bg * G + i:bg * G + i + 1, :], (8, L)) for i in range(G)]
        def body(a, acc):
            acc = list(acc)
            for k in range(L // 8):
                c = col[pl.ds(pl.multiple_of(a * L + k * 8, 8), 8), :]
                for i in range(G):
                    acc[i] = jnp.where(c == rows[i], 1, acc[i])
            return tuple(acc)
        acc = lax.fori_loop(0, bg * G, body, tuple(jnp.zeros((8, L), jnp.int32) for _ in range(G)))
        def diag(a, acc):
            acc = list(acc)
            for k in range(L // 8):
                c = col[pl.ds(pl.multiple_of(a * L + k * 8, 8), 8), :]
                t = a * L + k * 8 + sub
                for i in range(G):
                    s = lane + (bg * G + i) * L
                    acc[i] = jnp.where((c == rows[i]) & (t < s), 1, acc[i])
            return tuple(acc)
        acc = lax.fori_loop(bg * G, bg * G + G, diag, acc)
        for i in range(G):
            first[bg * G + i:bg * G + i + 1, :] = 1 - jnp.max(acc[i], axis=0, keepdims=True)

    ids = ids_ref[...]
    owner = jnp.zeros((R, L), jnp.int32)
    for o in range(1, n):
        owner = owner + jnp.where(ids >= o * shard_rows, 1, 0)
    isf = first[...] == 1
    one = jnp.concatenate([jnp.where(isf & (owner == o), 1.0, 0.0) for o in range(n)], axis=0).astype(jnp.bfloat16)
    up = (lax.broadcasted_iota(jnp.int32, (L, L), 0) < lax.broadcasted_iota(jnp.int32, (L, L), 1)).astype(jnp.float32).astype(jnp.bfloat16)
    prefix = jnp.dot(one, up, preferred_element_type=jnp.float32)
    tot = jnp.dot(one, jnp.ones((L, L), jnp.bfloat16), preferred_element_type=jnp.float32)
    r = lax.broadcasted_iota(jnp.int32, (n * R, n * R), 0)
    c = lax.broadcasted_iota(jnp.int32, (n * R, n * R), 1)
    low = ((r // R == c // R) & (c < r)).astype(jnp.float32).astype(jnp.bfloat16)
    off = jnp.dot(low, tot.astype(jnp.bfloat16), preferred_element_type=jnp.float32)
    pos = prefix + off
    slot = jnp.zeros((R, L), jnp.float32)
    most = jnp.zeros((1, L), jnp.float32)
    for o in range(n):
        slot = jnp.where(owner == o, pos[o * R:(o + 1) * R], slot)
        most = jnp.maximum(most, (off + tot)[(o + 1) * R - 1:(o + 1) * R])
    cnt_ref[...] = most.astype(jnp.int32)
    first[...] = jnp.where(isf, owner * SPAN + slot.astype(jnp.int32) + 1, 0)
    spread(first, wcol)

    for bg in range(R // G):
        rows = [jnp.broadcast_to(ids_ref[bg * G + i:bg * G + i + 1, :], (8, L)) for i in range(G)]
        def body(a, acc):
            acc = list(acc)
            for k in range(L // 8):
                at = pl.ds(pl.multiple_of(a * L + k * 8, 8), 8)
                c, w = col[at, :], wcol[at, :]
                for i in range(G):
                    acc[i] = jnp.where(c == rows[i], jnp.maximum(acc[i], w), acc[i])
            return tuple(acc)
        acc = lax.fori_loop(0, bg * G + G, body, tuple(jnp.zeros((8, L), jnp.int32) for _ in range(G)))
        for i in range(G):
            code_ref[bg * G + i:bg * G + i + 1, :] = jnp.max(acc[i], axis=0, keepdims=True) - 1

    K = list_ref.shape[0]
    want = [me * SPAN + 1 + i * L + lane for i in range(K)]
    def body(a, acc):
        acc = list(acc)
        for k in range(L // 8):
            at = pl.ds(pl.multiple_of(a * L + k * 8, 8), 8)
            c, w = col[at, :], wcol[at, :]
            for i in range(K):
                acc[i] = jnp.where(w == want[i], c, acc[i])
        return tuple(acc)
    acc = lax.fori_loop(0, R, body, tuple(jnp.zeros((8, L), jnp.int32) for _ in range(K)))
    for i in range(K):
        list_ref[i:i + 1, :] = jnp.maximum(jnp.max(acc[i], axis=0, keepdims=True) - me * shard_rows, 0)


def index(n, shard_rows, cap, ids):
    R, L = ids.size // 128, 128
    K = -(-cap // L)
    return pl.pallas_call(
        functools.partial(index_kernel, n, shard_rows, cap),
        out_shape=(jax.ShapeDtypeStruct((R, L), jnp.int32), jax.ShapeDtypeStruct((K, L), jnp.int32), jax.ShapeDtypeStruct((1, L), jnp.int32)),
        scratch_shapes=[pltpu.VMEM((R * L, L), jnp.int32), pltpu.VMEM((R * L, L), jnp.int32), pltpu.VMEM((R, L), jnp.int32)],
        name="index",
    )(ids.reshape(R, L))


def rows_kernel(cap, nb, list_ref, table_ref, out_ref, buf, scr, sem):
    T = table_ref.shape[1] // 128
    U = 8
    def copy(k):
        row = list_ref[k]
        base = pl.multiple_of((row // 8) * 8, 8)
        s = lax.rem(k, nb)
        return pltpu.make_async_copy(table_ref.at[pl.ds(base, 8)], buf.at[s], sem.at[s])
    for k in range(nb):
        copy(k).start()
    @pl.loop(0, cap // U)
    def _(q):
        for u in range(U):
            k = q * U + u
            s = lax.rem(k, nb)
            copy(k).wait()
            for j in range(T):
                scr[u, j * 8:(j + 1) * 8, :] = buf[s, :, j * 128:(j + 1) * 128].astype(jnp.float32)
            r = lax.rem(list_ref[k], 8)
            out_ref[k] = scr[u, pl.ds(r, T, stride=8), :].astype(jnp.bfloat16)
        for u in range(U):
            k = q * U + u
            @pl.when(k + nb < cap)
            def _():
                copy(k + nb).start()


def rows(cap, lst, table, nb=32):
    T = table.shape[1] // 128
    return pl.pallas_call(
        functools.partial(rows_kernel, cap, nb),
        out_shape=jax.ShapeDtypeStruct((cap, T, 128), table.dtype),
        grid_spec=pltpu.PrefetchScalarGridSpec(
            num_scalar_prefetch=1, grid=(),
            in_specs=[pl.BlockSpec(memory_space=pl.ANY)],
            out_specs=pl.BlockSpec(memory_space=pltpu.VMEM),
            scratch_shapes=[pltpu.VMEM((nb, 8, table.shape[1]), table.dtype), pltpu.VMEM((8, T * 8, 128), jnp.float32), pltpu.SemaphoreType.DMA((nb,))]),
        name="rows",
    )(lst, table)


EPS = 1e-5


def project_kernel(cap, span, tb, seq, blk, nsteps, meta, code, u_ref, pos_ref, own_pos_ref, gain_ref, bias_ref, wa_ref, wb_ref, ba_ref, bb_ref,
                   qkv_ref, emb_ref, xs, hs):
    step = pl.program_id(0)
    T = u_ref.shape[1]
    D = T * 128
    inv = 1.0 / D

    def fetch(base, t16):
        for half in range(2):
            for r in range(8):
                c = code[base + t16 * 16 + half * 8 + r]
                at = lax.div(c, span) * cap + lax.rem(c, span)
                xs[half, pl.ds(r, T, stride=8), :] = u_ref[at].astype(jnp.float32)

    def embed(half, p):
        return [(xs[half, j * 8:(j + 1) * 8, :] + p[half * 8:half * 8 + 8, j * 128:(j + 1) * 128].astype(jnp.float32)).astype(jnp.bfloat16) for j in range(T)]

    @pl.when(step < nsteps)
    def _():
        base = meta[1] * seq + step * tb
        @pl.loop(0, tb // 16)
        def _(g):
            fetch(base, g)
            t = pl.multiple_of(g * 16, 16)
            p = pos_ref.at[pl.ds(t, 16), :]
            out = []
            for half in range(2):
                e = [v.astype(jnp.float32) for v in embed(half, p)]
                s = e[0]
                for j in range(1, T):
                    s = s + e[j]
                mean = jnp.sum(s, axis=1, keepdims=True) * inv
                mb = jnp.broadcast_to(mean, (8, 128))
                e = [v - mb for v in e]
                s = e[0] * e[0]
                for j in range(1, T):
                    s = s + e[j] * e[j]
                var = jnp.sum(s, axis=1, keepdims=True) * inv
                rs = jnp.broadcast_to(lax.rsqrt(var + EPS), (8, 128))
                out.append([e[j] * rs * gain_ref[:, j * 128:(j + 1) * 128] + bias_ref[:, j * 128:(j + 1) * 128] for j in range(T)])
            for j in range(T):
                hs[pl.ds(t, 16), j * 128:(j + 1) * 128] = jnp.concatenate([out[0][j], out[1][j]], axis=0).astype(jnp.bfloat16)
        M = 384
        for k, (w, b) in enumerate(((wa_ref, ba_ref), (wb_ref, bb_ref))):
            for m in range(0, w.shape[0], M):
                o = lax.dot_general(w[m:m + M, :], hs[...], (((1,), (1,)), ((), ())), preferred_element_type=jnp.float32)
                qkv_ref[k, m:m + M, :] = (o + b[m:m + M, :]).astype(jnp.bfloat16)

    @pl.when(step == nsteps)
    def _():
        for b in range(2):
            base = b * seq + meta[0] * blk
            @pl.loop(0, blk // 16)
            def _(g):
                fetch(base, g)
                t = pl.multiple_of(g * 16, 16)
                p = own_pos_ref.at[pl.ds(t, 16), :]
                e0, e1 = embed(0, p), embed(1, p)
                for j in range(T):
                    emb_ref[b, pl.ds(t, 16), j * 128:(j + 1) * 128] = jnp.concatenate([e0[j], e1[j]], axis=0)


def project(n, cap, span, meta, code, u, pos, gain, bias, wa, wb, ba, bb, tb=512):
    seq, D = pos.shape
    blk = seq // n
    nsteps = seq // tb
    M = wa.shape[0]
    last = nsteps - 1
    one = lambda shape: pl.BlockSpec(shape, lambda i, *_: (0,) * len(shape), pipeline_mode=pl.Buffered(1))
    return pl.pallas_call(
        functools.partial(project_kernel, cap, span, tb, seq, blk, nsteps),
        out_shape=(jax.ShapeDtypeStruct((2, M, seq), jnp.bfloat16), jax.ShapeDtypeStruct((2, blk, D), jnp.bfloat16)),
        grid_spec=pltpu.PrefetchScalarGridSpec(
            num_scalar_prefetch=2, grid=(nsteps + 1,),
            in_specs=[one(u.shape),
                      pl.BlockSpec((tb, D), lambda i, *_: (jnp.minimum(i, last), 0)),
                      pl.BlockSpec((blk, D), lambda i, meta, code: (meta[0], 0), pipeline_mode=pl.Buffered(1)),
                      one((1, D)), one((1, D)), one(wa.shape), one(wb.shape), one(ba.shape), one(bb.shape)],
            out_specs=(pl.BlockSpec((2, M, tb), lambda i, *_: (0, 0, jnp.minimum(i, last))), pl.BlockSpec((2, blk, D), lambda i, *_: (0, 0, 0), pipeline_mode=pl.Buffered(1))),
            scratch_shapes=[pltpu.VMEM((2, D // 128 * 8, 128), jnp.float32), pltpu.VMEM((tb, D), jnp.bfloat16)]),
        compiler_params=pltpu.CompilerParams(vmem_limit_bytes=60 * 2**20),
        name="project",
    )(meta, code, u, pos, pos, gain, bias, wa, wb, ba, bb)


def attention_kernel(scale, qb, meta, qkv_ref, out_ref, kk, vv, sc):
    E, S = qkv_ref.shape[3:]
    c = scale * 1.4426950408889634
    for t in range(0, S, 128):
        kk[t:t + 128, :] = qkv_ref[0, 1, 0, :, t:t + 128].astype(jnp.float32).T.astype(jnp.bfloat16)
    vv[0:E, :] = qkv_ref[0, 2, 0]
    vv[E:, :] = jnp.where(lax.broadcasted_iota(jnp.int32, (vv.shape[0] - E, S), 0) == 0, 1.0, 0.0).astype(jnp.bfloat16)
    keep = lax.broadcasted_iota(jnp.int32, (qb, qb), 0) <= lax.broadcasted_iota(jnp.int32, (qb, qb), 1)
    for i in range(S // qb):
        n = (i + 1) * qb
        q = qkv_ref[0, 0, 0, :, i * qb:n]
        s = jnp.dot(kk[0:n, :], q, preferred_element_type=jnp.float32)
        d = jnp.where(keep, s[n - qb:n], -jnp.inf)
        s = d if i == 0 else jnp.concatenate([s[:n - qb], d], axis=0)
        m = jnp.max(s, axis=0, keepdims=True) * c
        p = jnp.exp2(s * c - m).astype(jnp.bfloat16)
        o = jnp.dot(vv[:, 0:n], p, preferred_element_type=jnp.float32)
        out_ref[i, 0, 0] = (o[0:E] * (1.0 / o[E:E + 1])).astype(jnp.bfloat16)


def attention(n, meta, qkv, qb=256):
    _, _, H, E, S = qkv.shape
    return pl.pallas_call(
        functools.partial(attention_kernel, E ** -0.5, qb),
        out_shape=jax.ShapeDtypeStruct((n, 2, H, E, S // n), jnp.bfloat16),
        grid_spec=pltpu.PrefetchScalarGridSpec(
            num_scalar_prefetch=1, grid=(2, H),
            in_specs=[pl.BlockSpec((1, 3, 1, E, S), lambda k, h, meta: (k, 0, h, 0, 0))],
            out_specs=pl.BlockSpec((n, 1, 1, E, S // n), lambda k, h, meta: (0, lax.rem(meta[1] + k, 2), h, 0, 0)),
            scratch_shapes=[pltpu.VMEM((S, E), jnp.bfloat16), pltpu.VMEM((E + 16, S), jnp.bfloat16), pltpu.VMEM((S, qb), jnp.float32)]),
        compiler_params=pltpu.CompilerParams(vmem_limit_bytes=48 * 2**20),
        name="attention",
    )(meta, qkv)


def output_kernel(n, nb, owners, lows, meta, ctx_ref, emb_ref, bias_ref, *refs):
    pieces, (out_ref, w, a, sem) = refs[:-4], refs[-4:]
    K, blk = ctx_ref.shape[1:]
    D = w.shape[2]
    def copy(i, j):
        rows = pieces[i].shape[0]
        return pltpu.make_async_copy(pieces[i].at[:, pl.ds(j * nb, nb)], w.at[meta[owners[i]], pl.ds(lows[i], rows), pl.ds(j * nb, nb)], sem.at[i, j])
    for j in range(D // nb):
        for i in range(len(pieces)):
            copy(i, j).start()
    for s in range(n):
        for k in range(0, K, 128):
            for t in range(0, blk, 128):
                a[(s % 2) * blk + t:(s % 2) * blk + t + 128, (s // 2) * K + k:(s // 2) * K + k + 128] = ctx_ref[s, k:k + 128, t:t + 128].astype(jnp.float32).T.astype(jnp.bfloat16)
    for j in range(D // nb):
        for i in range(len(pieces)):
            copy(i, j).wait()
        cols = slice(j * nb, (j + 1) * nb)
        o = jnp.dot(a[...], w[:, :, cols].reshape(n * w.shape[1], nb), preferred_element_type=jnp.float32)
        for b in range(2):
            out_ref[b, :, cols] = (emb_ref[b, :, cols].astype(jnp.float32) + o[b * blk:(b + 1) * blk] + bias_ref[:, cols]).astype(jnp.bfloat16)


def output(n, meta, ctx, emb, bias, pieces, owners, lows, nb=512):
    D = emb.shape[2]
    rows = sum(p.shape[0] for p in pieces) // n
    V = pl.BlockSpec(memory_space=pltpu.VMEM)
    return pl.pallas_call(
        functools.partial(output_kernel, n, nb, owners, lows),
        out_shape=jax.ShapeDtypeStruct(emb.shape, jnp.bfloat16),
        grid_spec=pltpu.PrefetchScalarGridSpec(
            num_scalar_prefetch=1, grid=(),
            in_specs=[V, V, V] + [pl.BlockSpec(memory_space=pl.ANY)] * len(pieces),
            out_specs=V,
            scratch_shapes=[pltpu.VMEM((n, rows, D), jnp.bfloat16), pltpu.VMEM((2 * emb.shape[1], D), jnp.bfloat16), pltpu.SemaphoreType.DMA((len(pieces), D // nb))]),
        compiler_params=pltpu.CompilerParams(vmem_limit_bytes=60 * 2**20),
        name="output",
    )(meta, ctx, emb, bias, *pieces)


CAP = 264


def place_kernel(code_ref, u_ref, x_ref, out_ref, sem):
    @pl.loop(0, code_ref.shape[0])
    def _(t):
        c = code_ref[t]

        @pl.when(c >= 0)
        def _():
            copy = pltpu.make_async_copy(u_ref.at[c], out_ref.at[t], sem)
            copy.start()
            copy.wait()


def place(at, u, x):
    A = pl.BlockSpec(memory_space=pl.ANY)
    return pl.pallas_call(
        place_kernel,
        out_shape=jax.ShapeDtypeStruct(x.shape, x.dtype),
        grid_spec=pltpu.PrefetchScalarGridSpec(num_scalar_prefetch=1, grid=(), in_specs=[A, A], out_specs=A, scratch_shapes=[pltpu.SemaphoreType.DMA]),
        input_output_aliases={2: 0},
        name="place",
    )(at, u, x)


def solution(mesh):
    n = mesh.shape["tp"]
    chips = n // 2

    def ring(step):
        return [((c * 2 + k), ((c + step) % chips) * 2 + k) for c in range(chips) for k in range(2)]

    swap = [(d, d ^ 1) for d in range(n)]
    permute = lambda x, perm: lax.ppermute(x, "tp", perm)

    def local_step(token_ids, word_shard, pos_table, ln_gain, ln_bias, w_qkv, b_qkv, w_out, b_out):
        me = lax.axis_index("tp")
        core = lax.rem(me, 2)
        seq, D = pos_table.shape
        H, E = w_qkv.shape[2:]
        shard_rows = word_shard.shape[0]
        w_own = jnp.transpose(w_qkv, (1, 2, 3, 0)).reshape(3 * H * E, D)
        b_own = b_qkv.reshape(3 * H * E, 1)
        w_par, b_par = permute(w_own, swap), permute(b_own, swap)

        v_own = w_out.reshape(H * E, D)
        half = v_own.shape[0] // 2
        v_minus, v_plus = permute(v_own, ring(1)), permute(v_own, ring(-1))
        v_opp_a, v_opp_b = permute(v_minus[:half], ring(1)), permute(v_plus[half:], ring(-1))
        pieces = [v_own, v_minus, v_plus, v_opp_a, v_opp_b]
        pieces = pieces + [permute(p, swap) for p in pieces]
        owners, lows = [0, 3, 4, 5, 5, 6, 7, 8, 9, 9], [0, 0, 0, 0, half] * 2
        at = lambda c, k: lax.rem(c + chips, chips) * 2 + k
        chip = me // 2
        meta = [me, core, chip] + [at(chip + s, k) for k in (core, 1 - core) for s in (-1, 1, 2)]
        meta = meta[:6] + [me + 1 - 2 * core] + meta[6:]
        meta = jnp.stack(meta).astype(jnp.int32)

        blk = seq // n
        total = max(n * CAP, seq + blk)
        code, rows_list, most = index(n, shard_rows, CAP, token_ids)
        code, most = code.reshape(-1), most[0, 0]
        u = gather_all(n, rows(CAP, rows_list.reshape(-1), word_shard), total)

        rounds = jnp.where(most > CAP, (most + CAP - 1) // CAP, 0)

        def wanted(x):
            x = x.reshape(2, seq)
            own = lax.dynamic_index_in_dim(x, core, 0, keepdims=False)
            other = lax.dynamic_index_in_dim(x, 1 - core, 0, keepdims=False)
            return jnp.concatenate([own, lax.dynamic_slice_in_dim(other, me * blk, blk)])

        def more(carry):
            r, u = carry
            slot = code % SPAN - r * CAP
            hit = (slot >= 0) & (slot < CAP)
            mine = jnp.where(hit & (code // SPAN == me), slot, -1)
            ids = token_ids.reshape(-1) - me * shard_rows
            chosen = jnp.max(jnp.where(mine[None, :] == jnp.arange(rows_list.size)[:, None], ids[None, :], 0), axis=1)
            v = gather_all(n, rows(CAP, chosen, word_shard), total)
            return r + 1, place(wanted(jnp.where(hit, code // SPAN * CAP + slot, -1)), v, u)

        _, u = lax.while_loop(lambda c: c[0] < rounds, more, (jnp.int32(0), u))
        t = jnp.arange(code.size, dtype=jnp.int32)
        t = jnp.where(t // seq == core, t % seq, jnp.clip(t % seq - me * blk, 0, blk - 1) + seq)
        code = jnp.where(rounds > 0, t // CAP * SPAN + t % CAP, code)

        qkv, embed = project(n, CAP, SPAN, meta, code, u, pos_table, ln_gain[None], ln_bias[None], w_own, w_par, b_own, b_par)
        ctx = attention(n, meta, qkv.reshape(2, 3, H, E, seq))
        ctx = exchange(n, ctx.reshape(n, 2 * H * E, seq // n))
        resid_out = output(n, meta, ctx, embed, b_out[None], pieces, owners, lows)
        return resid_out, embed

    in_specs = (P("dp", None), P("tp", None), P(None, None), P(None), P(None), P(None, None, "tp", None), P(None, "tp", None), P("tp", None, None), P(None))
    out_specs = (P("dp", "tp", None), P("dp", "tp", None))
    return jax.shard_map(local_step, mesh=mesh, in_specs=in_specs, out_specs=out_specs, check_vma=False)
```

```python
import functools

import jax
import jax.numpy as jnp
from jax import lax
from jax.experimental import pallas as pl
from jax.experimental.pallas import tpu as pltpu
from jax.sharding import PartitionSpec as P

MESH = pl.DeviceIdType.MESH


def gather_all_kernel(n, S, src_ref, all_ref, loc_sem, send_sem, recv_sem):
    cap = src_ref.shape[0]

    def of(d):
        return all_ref.at[pl.ds(d * cap, cap)]
    chips = n // 2
    me = lax.axis_index("tp")
    chip, core = me // 2, lax.rem(me, 2)
    def at(c):
        return lax.rem(c + chips, chips) * 2 + core
    plus, minus, opp = at(chip + 1), at(chip - 1), at(chip + 2)
    partner = me + 1 - 2 * core
    P = 2 * S
    step = src_ref.shape[0] // P

    barrier = pltpu.get_barrier_semaphore()
    for d in (plus, minus, partner):
        pl.semaphore_signal(barrier, inc=1, device_id={"tp": d}, device_id_type=MESH)
    pl.semaphore_wait(barrier, 3)

    started = []
    def rc(src, dst, ch, k, dev):
        return pltpu.make_async_remote_copy(src_ref=src, dst_ref=dst, send_sem=send_sem.at[ch, k], recv_sem=recv_sem.at[ch, k],
                                            device_id={"tp": dev}, device_id_type=MESH)
    def go(src, dst, ch, k, dev):
        c = rc(src, dst, ch, k, dev)
        c.start()
        started.append(c)
    def piece(ref, k):
        return ref.at[pl.ds(k * step, step)]
    first, last = list(range(S)), list(range(S, P))
    for a, b in zip(first, last):
        go(piece(src_ref, a), piece(of(me), a), 0, a, plus)
        go(piece(src_ref, b), piece(of(me), b), 1, b, minus)
    for a, b in zip(first, last):
        go(piece(src_ref, b), piece(of(me), b), 0, b, plus)
        go(piece(src_ref, a), piece(of(me), a), 1, a, minus)
    go(src_ref, of(me), 4, 0, partner)
    loc = pltpu.make_async_copy(src_ref, of(me), loc_sem)
    loc.start()
    def got(owner, ch, k):
        r = piece(of(owner), k)
        rc(r, r, ch, k, partner).wait_recv()
        return r
    for a, b in zip(first, last):
        r = got(minus, 0, a)
        go(r, r, 2, a, plus)
        go(r, r, 5, a, partner)
        r = got(plus, 1, b)
        go(r, r, 3, b, minus)
        go(r, r, 6, b, partner)
    for a, b in zip(first, last):
        r = got(minus, 0, b)
        go(r, r, 5, b, partner)
        r = got(plus, 1, a)
        go(r, r, 6, a, partner)
    for a, b in zip(first, last):
        r = got(opp, 2, a)
        go(r, r, 7, a, partner)
        r = got(opp, 3, b)
        go(r, r, 7, b, partner)
    other = lambda d: d + 1 - 2 * core
    r = of(partner)
    rc(r, r, 4, 0, partner).wait_recv()
    for k in range(P):
        got(other(minus), 5, k)
        got(other(plus), 6, k)
        got(other(opp), 7, k)
    loc.wait()
    for c in started:
        c.wait_send()


def gather_all(n, rows, total, S=2, cid=0):
    return pl.pallas_call(
        functools.partial(gather_all_kernel, n, S),
        out_shape=jax.ShapeDtypeStruct((total,) + rows.shape[1:], rows.dtype),
        in_specs=[pl.BlockSpec(memory_space=pltpu.VMEM)],
        out_specs=pl.BlockSpec(memory_space=pl.ANY),
        scratch_shapes=[pltpu.SemaphoreType.DMA, pltpu.SemaphoreType.DMA((8, 2 * S)), pltpu.SemaphoreType.DMA((8, 2 * S))],
        compiler_params=pltpu.CompilerParams(collective_id=cid, has_side_effects=True),
        name="gather_all",
    )(rows)


def exchange_kernel(n, src_ref, out_ref, loc_sem, send_sem, recv_sem):
    me = lax.axis_index("tp")
    barrier = pltpu.get_barrier_semaphore()
    for s in range(1, n):
        pl.semaphore_signal(barrier, inc=1, device_id={"tp": lax.rem(me + s, n)}, device_id_type=MESH)
    pl.semaphore_wait(barrier, n - 1)
    cs = []
    for s in range(1, n):
        to = lax.rem(me + s, n)
        c = pltpu.make_async_remote_copy(src_ref=src_ref.at[to], dst_ref=out_ref.at[me], send_sem=send_sem.at[s], recv_sem=recv_sem.at[s],
                                         device_id={"tp": to}, device_id_type=MESH)
        c.start()
        cs.append(c)
    loc = pltpu.make_async_copy(src_ref.at[me], out_ref.at[me], loc_sem)
    loc.start()
    loc.wait()
    for s in range(1, n):
        fr = lax.rem(me - s + n, n)
        r = out_ref.at[fr]
        pltpu.make_async_remote_copy(src_ref=r, dst_ref=r, send_sem=send_sem.at[s], recv_sem=recv_sem.at[s],
                                     device_id={"tp": fr}, device_id_type=MESH).wait_recv()
    for c in cs:
        c.wait_send()


def exchange(n, x, cid=1):
    return pl.pallas_call(
        functools.partial(exchange_kernel, n),
        out_shape=jax.ShapeDtypeStruct(x.shape, x.dtype),
        in_specs=[pl.BlockSpec(memory_space=pltpu.VMEM)],
        out_specs=pl.BlockSpec(memory_space=pl.ANY),
        scratch_shapes=[pltpu.SemaphoreType.DMA, pltpu.SemaphoreType.DMA((n,)), pltpu.SemaphoreType.DMA((n,))],
        compiler_params=pltpu.CompilerParams(collective_id=cid, has_side_effects=True),
        name="exchange",
    )(x)


SPAN = 8192


def index_kernel(n, shard_rows, cap, ids_ref, code_ref, list_ref, cnt_ref, col, wcol, first):
    me = lax.axis_index("tp")
    R, L = ids_ref.shape
    G = 8
    lane = lax.broadcasted_iota(jnp.int32, (8, L), 1)
    sub = lax.broadcasted_iota(jnp.int32, (8, L), 0)

    def spread(src, dst):
        @pl.loop(0, R)
        def _(a):
            row = jnp.broadcast_to(src[pl.ds(a, 1), :], (L, L))
            dst[pl.ds(pl.multiple_of(a * L, L), L), :] = row.T
    spread(ids_ref, col)

    for bg in range(R // G):
        rows = [jnp.broadcast_to(ids_ref[bg * G + i:bg * G + i + 1, :], (8, L)) for i in range(G)]
        def body(a, acc):
            acc = list(acc)
            for k in range(L // 8):
                c = col[pl.ds(pl.multiple_of(a * L + k * 8, 8), 8), :]
                for i in range(G):
                    acc[i] = jnp.where(c == rows[i], 1, acc[i])
            return tuple(acc)
        acc = lax.fori_loop(0, bg * G, body, tuple(jnp.zeros((8, L), jnp.int32) for _ in range(G)))
        def diag(a, acc):
            acc = list(acc)
            for k in range(L // 8):
                c = col[pl.ds(pl.multiple_of(a * L + k * 8, 8), 8), :]
                t = a * L + k * 8 + sub
                for i in range(G):
                    s = lane + (bg * G + i) * L
                    acc[i] = jnp.where((c == rows[i]) & (t < s), 1, acc[i])
            return tuple(acc)
        acc = lax.fori_loop(bg * G, bg * G + G, diag, acc)
        for i in range(G):
            first[bg * G + i:bg * G + i + 1, :] = 1 - jnp.max(acc[i], axis=0, keepdims=True)

    ids = ids_ref[...]
    owner = jnp.zeros((R, L), jnp.int32)
    for o in range(1, n):
        owner = owner + jnp.where(ids >= o * shard_rows, 1, 0)
    isf = first[...] == 1
    one = jnp.concatenate([jnp.where(isf & (owner == o), 1.0, 0.0) for o in range(n)], axis=0).astype(jnp.bfloat16)
    up = (lax.broadcasted_iota(jnp.int32, (L, L), 0) < lax.broadcasted_iota(jnp.int32, (L, L), 1)).astype(jnp.float32).astype(jnp.bfloat16)
    prefix = jnp.dot(one, up, preferred_element_type=jnp.float32)
    tot = jnp.dot(one, jnp.ones((L, L), jnp.bfloat16), preferred_element_type=jnp.float32)
    r = lax.broadcasted_iota(jnp.int32, (n * R, n * R), 0)
    c = lax.broadcasted_iota(jnp.int32, (n * R, n * R), 1)
    low = ((r // R == c // R) & (c < r)).astype(jnp.float32).astype(jnp.bfloat16)
    off = jnp.dot(low, tot.astype(jnp.bfloat16), preferred_element_type=jnp.float32)
    pos = prefix + off
    slot = jnp.zeros((R, L), jnp.float32)
    most = jnp.zeros((1, L), jnp.float32)
    for o in range(n):
        slot = jnp.where(owner == o, pos[o * R:(o + 1) * R], slot)
        most = jnp.maximum(most, (off + tot)[(o + 1) * R - 1:(o + 1) * R])
    cnt_ref[...] = most.astype(jnp.int32)
    first[...] = jnp.where(isf, owner * SPAN + slot.astype(jnp.int32) + 1, 0)
    spread(first, wcol)

    for bg in range(R // G):
        rows = [jnp.broadcast_to(ids_ref[bg * G + i:bg * G + i + 1, :], (8, L)) for i in range(G)]
        def body(a, acc):
            acc = list(acc)
            for k in range(L // 8):
                at = pl.ds(pl.multiple_of(a * L + k * 8, 8), 8)
                c, w = col[at, :], wcol[at, :]
                for i in range(G):
                    acc[i] = jnp.where(c == rows[i], jnp.maximum(acc[i], w), acc[i])
            return tuple(acc)
        acc = lax.fori_loop(0, bg * G + G, body, tuple(jnp.zeros((8, L), jnp.int32) for _ in range(G)))
        for i in range(G):
            code_ref[bg * G + i:bg * G + i + 1, :] = jnp.max(acc[i], axis=0, keepdims=True) - 1

    K = list_ref.shape[0]
    want = [me * SPAN + 1 + i * L + lane for i in range(K)]
    def body(a, acc):
        acc = list(acc)
        for k in range(L // 8):
            at = pl.ds(pl.multiple_of(a * L + k * 8, 8), 8)
            c, w = col[at, :], wcol[at, :]
            for i in range(K):
                acc[i] = jnp.where(w == want[i], c, acc[i])
        return tuple(acc)
    acc = lax.fori_loop(0, R, body, tuple(jnp.zeros((8, L), jnp.int32) for _ in range(K)))
    for i in range(K):
        list_ref[i:i + 1, :] = jnp.maximum(jnp.max(acc[i], axis=0, keepdims=True) - me * shard_rows, 0)


def index(n, shard_rows, cap, ids):
    R, L = ids.size // 128, 128
    K = -(-cap // L)
    return pl.pallas_call(
        functools.partial(index_kernel, n, shard_rows, cap),
        out_shape=(jax.ShapeDtypeStruct((R, L), jnp.int32), jax.ShapeDtypeStruct((K, L), jnp.int32), jax.ShapeDtypeStruct((1, L), jnp.int32)),
        scratch_shapes=[pltpu.VMEM((R * L, L), jnp.int32), pltpu.VMEM((R * L, L), jnp.int32), pltpu.VMEM((R, L), jnp.int32)],
        name="index",
    )(ids.reshape(R, L))


def rows_kernel(cap, nb, list_ref, table_ref, out_ref, buf, scr, sem):
    T = table_ref.shape[1] // 128
    U = 8
    def copy(k):
        row = list_ref[k]
        base = pl.multiple_of((row // 8) * 8, 8)
        s = lax.rem(k, nb)
        return pltpu.make_async_copy(table_ref.at[pl.ds(base, 8)], buf.at[s], sem.at[s])
    for k in range(nb):
        copy(k).start()
    @pl.loop(0, cap // U)
    def _(q):
        for u in range(U):
            k = q * U + u
            s = lax.rem(k, nb)
            copy(k).wait()
            for j in range(T):
                scr[u, j * 8:(j + 1) * 8, :] = buf[s, :, j * 128:(j + 1) * 128].astype(jnp.float32)
            r = lax.rem(list_ref[k], 8)
            out_ref[k] = scr[u, pl.ds(r, T, stride=8), :].astype(jnp.bfloat16)
        for u in range(U):
            k = q * U + u
            @pl.when(k + nb < cap)
            def _():
                copy(k + nb).start()


def rows(cap, lst, table, nb=32):
    T = table.shape[1] // 128
    return pl.pallas_call(
        functools.partial(rows_kernel, cap, nb),
        out_shape=jax.ShapeDtypeStruct((cap, T, 128), table.dtype),
        grid_spec=pltpu.PrefetchScalarGridSpec(
            num_scalar_prefetch=1, grid=(),
            in_specs=[pl.BlockSpec(memory_space=pl.ANY)],
            out_specs=pl.BlockSpec(memory_space=pltpu.VMEM),
            scratch_shapes=[pltpu.VMEM((nb, 8, table.shape[1]), table.dtype), pltpu.VMEM((8, T * 8, 128), jnp.float32), pltpu.SemaphoreType.DMA((nb,))]),
        name="rows",
    )(lst, table)


EPS = 1e-5


def project_kernel(tb, seq, blk, steps, chunk, meta, code, u_hbm, pos_hbm, gain_ref, bias_ref, wa_hbm, wb_hbm, ba_ref, bb_ref,
                   qkv_ref, emb_ref, u, w, pos, xs, hs, usem, wsem, psem):
    step = pl.program_id(0)
    T = u.shape[1]
    M = wa_hbm.shape[0]
    inv = 1.0 / (T * 128)
    base = meta[1] * seq

    def load_u():
        return pltpu.make_async_copy(u_hbm, u, usem)
    def load_w(k):
        return pltpu.make_async_copy((wa_hbm, wb_hbm)[k], w.at[pl.ds(k * M, M)], wsem.at[k])
    def load_pos(i):
        return pltpu.make_async_copy(pos_hbm.at[pl.ds(i * tb, tb)], pos.at[lax.rem(i, 2)], psem.at[lax.rem(i, 2)])
    def load_own():
        return pltpu.make_async_copy(pos_hbm.at[pl.ds(meta[0] * blk, blk)], pos.at[steps % 2, pl.ds(0, blk)], psem.at[steps % 2])

    def fetch(slot, first):
        for r in range(8):
            xs[slot, pl.ds(r, T, stride=8), :] = u[code[first + r]].astype(jnp.float32)

    def tile(slot, j):
        return xs[slot, j * 8:(j + 1) * 8, :]

    def lanes(j):
        return slice(j * 128, (j + 1) * 128)

    def norm(i, g, lane_slot):
        t = pl.multiple_of(g * 16, 16)
        out = []
        for half in range(2):
            slot = lane_slot * 2 + half
            fetch(slot, base + i * tb + g * 16 + half * 8)
            p = pos.at[lax.rem(i, 2), pl.ds(t, 16), :]
            s = None
            for j in range(T):
                e = (tile(slot, j) + p[half * 8:half * 8 + 8, lanes(j)].astype(jnp.float32)).astype(jnp.bfloat16).astype(jnp.float32)
                xs[slot, j * 8:(j + 1) * 8, :] = e
                s = e if s is None else s + e
            mean = jnp.broadcast_to(jnp.sum(s, axis=1, keepdims=True) * inv, (8, 128))
            s = None
            for j in range(T):
                c = tile(slot, j) - mean
                s = c * c if s is None else s + c * c
            var = jnp.sum(s, axis=1, keepdims=True) * inv
            rs = jnp.broadcast_to(lax.rsqrt(var + EPS), (8, 128))
            out.append((slot, mean, rs))
        for j in range(T):
            y = [(tile(slot, j) - mean) * rs * gain_ref[:, lanes(j)] + bias_ref[:, lanes(j)] for slot, mean, rs in out]
            hs[lax.rem(i, 2), pl.ds(t, 16), lanes(j)] = jnp.concatenate(y, axis=0).astype(jnp.bfloat16)

    def embed(g, lane_slot):
        per = blk // 16
        b = lax.div(g, per)
        t = pl.multiple_of(lax.rem(g, per) * 16, 16)
        for half in range(2):
            fetch(lane_slot * 2 + half, b * seq + meta[0] * blk + t + half * 8)
        p = pos.at[steps % 2, pl.ds(t, 16), :]
        for j in range(T):
            e = jnp.concatenate([tile(lane_slot * 2, j), tile(lane_slot * 2 + 1, j)], axis=0) + p[:, lanes(j)].astype(jnp.float32)
            emb_ref[b, pl.ds(t, 16), lanes(j)] = e.astype(jnp.bfloat16)

    @pl.when(step == 0)
    def _():
        load_u().start()
        load_pos(0).start()
        for k in range(2):
            load_w(k).start()
        load_pos(1).start()
        load_u().wait()
        load_pos(0).wait()
        @pl.loop(0, tb // 64)
        def _(g):
            for j in range(4):
                norm(0, g * 4 + j, j)
        for k in range(2):
            load_w(k).wait()

    def sweep(beside):
        per = M // chunk
        h = hs.at[lax.rem(step, 2)]
        for k, b in enumerate((ba_ref, bb_ref)):
            @pl.loop(0, per)
            def _(m):
                at = pl.multiple_of(m * chunk, 32)
                o = lax.dot_general(w[pl.ds(k * M + at, chunk), :], h[...], (((1,), (1,)), ((), ())), preferred_element_type=jnp.float32)
                qkv_ref[k, pl.ds(at, chunk), :] = (o + b[pl.ds(at, chunk), :]).astype(jnp.bfloat16)
                n = tb // 16 // (2 * per)
                for j in range(n):
                    beside((k * per + m) * n + j, j)

    @pl.when(step < steps - 1)
    def _():
        load_pos(step + 1).wait()
        @pl.when(step + 2 < steps)
        def _():
            load_pos(step + 2).start()
        @pl.when(step + 2 == steps)
        def _():
            load_own().start()
        sweep(lambda g, j: norm(step + 1, g, j))

    @pl.when(step == steps - 1)
    def _():
        load_own().wait()
        sweep(embed)


def project(n, meta, code, u, pos, gain, bias, wa, wb, ba, bb, tb=512, chunk=288):
    seq, D = pos.shape
    blk = seq // n
    steps = seq // tb
    M = wa.shape[0]
    A = pl.BlockSpec(memory_space=pl.ANY)
    one = lambda shape: pl.BlockSpec(shape, lambda i, *_: (0,) * len(shape), pipeline_mode=pl.Buffered(1))
    return pl.pallas_call(
        functools.partial(project_kernel, tb, seq, blk, steps, chunk),
        out_shape=(jax.ShapeDtypeStruct((2, M, seq), jnp.bfloat16), jax.ShapeDtypeStruct((2, blk, D), jnp.bfloat16)),
        grid_spec=pltpu.PrefetchScalarGridSpec(
            num_scalar_prefetch=2, grid=(steps,),
            in_specs=[A, A, one((1, D)), one((1, D)), A, A, one(ba.shape), one(bb.shape)],
            out_specs=(pl.BlockSpec((2, M, tb), lambda i, *_: (0, 0, i)), pl.BlockSpec((2, blk, D), lambda i, *_: (0, 0, 0), pipeline_mode=pl.Buffered(1))),
            scratch_shapes=[pltpu.VMEM(u.shape, u.dtype), pltpu.VMEM((2 * M, D), wa.dtype), pltpu.VMEM((2, tb, D), pos.dtype),
                            pltpu.VMEM((8, D // 128 * 8, 128), jnp.float32), pltpu.VMEM((2, tb, D), jnp.bfloat16),
                            pltpu.SemaphoreType.DMA, pltpu.SemaphoreType.DMA((2,)), pltpu.SemaphoreType.DMA((2,))]),
        compiler_params=pltpu.CompilerParams(vmem_limit_bytes=63 * 2**20),
        name="project",
    )(meta, code, u, pos, gain, bias, wa, wb, ba, bb)


def attention_kernel(n, scale, qb, qkv_ref, out_ref, kk, vv, sc, ctx, loc_sem, send_sem, recv_sem):
    E, S = qkv_ref.shape[3:]
    H = out_ref.shape[2]
    N = S // qb
    c = scale * 1.4426950408889634
    me = lax.axis_index("tp")
    core = lax.rem(me, 2)
    k_id, h_id = pl.program_id(0), pl.program_id(1)
    head = lax.rem(k_id + core, 2) * H + h_id
    first = (k_id == 0) & (h_id == 0)
    last = (k_id == 1) & (h_id == H - 1)

    @pl.when(first)
    def _():
        barrier = pltpu.get_barrier_semaphore()
        for s in range(1, n):
            pl.semaphore_signal(barrier, inc=1, device_id={"tp": lax.rem(me + s, n)}, device_id_type=MESH)
        pl.semaphore_wait(barrier, n - 1)
        vv[E:, :] = jnp.where(lax.broadcasted_iota(jnp.int32, (vv.shape[0] - E, S), 0) == 0, 1.0, 0.0).astype(jnp.bfloat16)

    def send(s):
        to = lax.rem(me + s, n)
        return pltpu.make_async_remote_copy(src_ref=ctx.at[head, to], dst_ref=out_ref.at[me, lax.div(head, H), lax.rem(head, H)],
                                            send_sem=send_sem.at[s], recv_sem=recv_sem.at[s], device_id={"tp": to}, device_id_type=MESH)

    for t in range(0, S, 128):
        kk[t:t + 128, :] = qkv_ref[0, 1, 0, :, t:t + 128].astype(jnp.float32).T.astype(jnp.bfloat16)
    vv[0:E, :] = qkv_ref[0, 2, 0]
    keep = lax.broadcasted_iota(jnp.int32, (qb, qb), 0) <= lax.broadcasted_iota(jnp.int32, (qb, qb), 1)

    def scores(i, k, m):
        s = jnp.dot(kk[k * qb:(k + 1) * qb, :], qkv_ref[0, 0, 0, :, i * qb:(i + 1) * qb], preferred_element_type=jnp.float32)
        if k == i:
            s = jnp.where(keep, s, -jnp.inf)
        sc[i % 2, k * qb:(k + 1) * qb, :] = s
        top = jnp.max(s.reshape(qb // 8, 8, qb), axis=0)
        return top if m is None else jnp.maximum(m, top)

    def weigh(i, k, mc, o):
        s = sc[i % 2, k * qb:(k + 1) * qb, :]
        p = jnp.exp2(s * c - mc).astype(jnp.bfloat16)
        d = jnp.dot(vv[:, k * qb:(k + 1) * qb], p, preferred_element_type=jnp.float32)
        return d if o is None else o + d

    m = scores(0, 0, None)
    for i in range(N):
        mc = jnp.max(m, axis=0, keepdims=True) * c
        o = m = None
        for k in range(i + 2):
            if i + 1 < N:
                m = scores(i + 1, k, m)
            if k <= i:
                o = weigh(i, k, mc, o)
        ctx[head, i] = (o[0:E] * (1.0 / o[E:E + 1])).astype(jnp.bfloat16)

    for s in range(1, n):
        send(s).start()
    local = pltpu.make_async_copy(ctx.at[head, me], out_ref.at[me, lax.div(head, H), lax.rem(head, H)], loc_sem)
    local.start()
    local.wait()

    @pl.when(last)
    def _():
        for s in range(1, n):
            fr = lax.rem(me - s + n, n)
            r = out_ref.at[fr]
            got = pltpu.make_async_remote_copy(src_ref=r, dst_ref=r, send_sem=send_sem.at[s], recv_sem=recv_sem.at[s], device_id={"tp": fr}, device_id_type=MESH)
            got.wait_recv()
            got.wait_send()


def attention(n, qkv, cid=1, qb=256):
    _, _, H, E, S = qkv.shape
    return pl.pallas_call(
        functools.partial(attention_kernel, n, E ** -0.5, qb),
        out_shape=jax.ShapeDtypeStruct((n, 2, H, E, S // n), jnp.bfloat16),
        grid=(2, H),
        in_specs=[pl.BlockSpec((1, 3, 1, E, S), lambda k, h: (k, 0, h, 0, 0))],
        out_specs=pl.BlockSpec(memory_space=pl.ANY),
        scratch_shapes=[pltpu.VMEM((S, E), jnp.bfloat16), pltpu.VMEM((E + 16, S), jnp.bfloat16), pltpu.VMEM((2, S, qb), jnp.float32),
                        pltpu.VMEM((2 * H, n, E, qb), jnp.bfloat16), pltpu.SemaphoreType.DMA, pltpu.SemaphoreType.DMA((n,)), pltpu.SemaphoreType.DMA((n,))],
        compiler_params=pltpu.CompilerParams(collective_id=cid, has_side_effects=True, vmem_limit_bytes=48 * 2**20),
        name="attention",
    )(qkv)


def output_kernel(n, nb, owners, lows, meta, ctx_ref, emb_ref, bias_ref, *refs):
    pieces, (out_ref, w, a, sem) = refs[:-4], refs[-4:]
    K, blk = ctx_ref.shape[1:]
    D = w.shape[2]
    def copy(i, j):
        rows = pieces[i].shape[0]
        return pltpu.make_async_copy(pieces[i].at[:, pl.ds(j * nb, nb)], w.at[meta[owners[i]], pl.ds(lows[i], rows), pl.ds(j * nb, nb)], sem.at[i, j])
    for j in range(D // nb):
        for i in range(len(pieces)):
            copy(i, j).start()
    for s in range(n):
        for k in range(0, K, 128):
            for t in range(0, blk, 128):
                a[(s % 2) * blk + t:(s % 2) * blk + t + 128, (s // 2) * K + k:(s // 2) * K + k + 128] = ctx_ref[s, k:k + 128, t:t + 128].astype(jnp.float32).T.astype(jnp.bfloat16)
    for j in range(D // nb):
        for i in range(len(pieces)):
            copy(i, j).wait()
        cols = slice(j * nb, (j + 1) * nb)
        o = jnp.dot(a[...], w[:, :, cols].reshape(n * w.shape[1], nb), preferred_element_type=jnp.float32)
        for b in range(2):
            out_ref[b, :, cols] = (emb_ref[b, :, cols].astype(jnp.float32) + o[b * blk:(b + 1) * blk] + bias_ref[:, cols]).astype(jnp.bfloat16)


def output(n, meta, ctx, emb, bias, pieces, owners, lows, nb=512):
    D = emb.shape[2]
    rows = sum(p.shape[0] for p in pieces) // n
    V = pl.BlockSpec(memory_space=pltpu.VMEM)
    return pl.pallas_call(
        functools.partial(output_kernel, n, nb, owners, lows),
        out_shape=jax.ShapeDtypeStruct(emb.shape, jnp.bfloat16),
        grid_spec=pltpu.PrefetchScalarGridSpec(
            num_scalar_prefetch=1, grid=(),
            in_specs=[V, V, V] + [pl.BlockSpec(memory_space=pl.ANY)] * len(pieces),
            out_specs=V,
            scratch_shapes=[pltpu.VMEM((n, rows, D), jnp.bfloat16), pltpu.VMEM((2 * emb.shape[1], D), jnp.bfloat16), pltpu.SemaphoreType.DMA((len(pieces), D // nb))]),
        compiler_params=pltpu.CompilerParams(vmem_limit_bytes=60 * 2**20),
        name="output",
    )(meta, ctx, emb, bias, *pieces)


CAP = 264


def place_kernel(code_ref, u_ref, x_ref, out_ref, sem):
    @pl.loop(0, code_ref.shape[0])
    def _(t):
        c = code_ref[t]

        @pl.when(c >= 0)
        def _():
            copy = pltpu.make_async_copy(u_ref.at[c], out_ref.at[t], sem)
            copy.start()
            copy.wait()


def place(at, u, x):
    A = pl.BlockSpec(memory_space=pl.ANY)
    return pl.pallas_call(
        place_kernel,
        out_shape=jax.ShapeDtypeStruct(x.shape, x.dtype),
        grid_spec=pltpu.PrefetchScalarGridSpec(num_scalar_prefetch=1, grid=(), in_specs=[A, A], out_specs=A, scratch_shapes=[pltpu.SemaphoreType.DMA]),
        input_output_aliases={2: 0},
        name="place",
    )(at, u, x)


def solution(mesh):
    n = mesh.shape["tp"]
    chips = n // 2

    def ring(step):
        return [((c * 2 + k), ((c + step) % chips) * 2 + k) for c in range(chips) for k in range(2)]

    swap = [(d, d ^ 1) for d in range(n)]
    permute = lambda x, perm: lax.ppermute(x, "tp", perm)

    def local_step(token_ids, word_shard, pos_table, ln_gain, ln_bias, w_qkv, b_qkv, w_out, b_out):
        me = lax.axis_index("tp")
        core = lax.rem(me, 2)
        seq, D = pos_table.shape
        H, E = w_qkv.shape[2:]
        shard_rows = word_shard.shape[0]
        w_own = jnp.transpose(w_qkv, (1, 2, 3, 0)).reshape(3 * H * E, D)
        b_own = b_qkv.reshape(3 * H * E, 1)
        w_par, b_par = permute(w_own, swap), permute(b_own, swap)

        v_own = w_out.reshape(H * E, D)
        half = v_own.shape[0] // 2
        v_minus, v_plus = permute(v_own, ring(1)), permute(v_own, ring(-1))
        v_opp_a, v_opp_b = permute(v_minus[:half], ring(1)), permute(v_plus[half:], ring(-1))
        pieces = [v_own, v_minus, v_plus, v_opp_a, v_opp_b]
        pieces = pieces + [permute(p, swap) for p in pieces]
        owners, lows = [0, 3, 4, 5, 5, 6, 7, 8, 9, 9], [0, 0, 0, 0, half] * 2
        place_of = lambda c, k: lax.rem(c + chips, chips) * 2 + k
        chip = me // 2
        meta = [me, core, chip] + [place_of(chip + s, k) for k in (core, 1 - core) for s in (-1, 1, 2)]
        meta = meta[:6] + [me + 1 - 2 * core] + meta[6:]
        meta = jnp.stack(meta).astype(jnp.int32)

        blk = seq // n
        total = max(n * CAP, seq + blk)
        code, rows_list, most = index(n, shard_rows, CAP, token_ids)
        code, most = code.reshape(-1), most[0, 0]
        u = gather_all(n, rows(CAP, rows_list.reshape(-1), word_shard), total)

        rounds = jnp.where(most > CAP, (most + CAP - 1) // CAP, 0)

        def wanted(x):
            x = x.reshape(2, seq)
            own = lax.dynamic_index_in_dim(x, core, 0, keepdims=False)
            other = lax.dynamic_index_in_dim(x, 1 - core, 0, keepdims=False)
            return jnp.concatenate([own, lax.dynamic_slice_in_dim(other, me * blk, blk)])

        def more(carry):
            r, u = carry
            slot = code % SPAN - r * CAP
            hit = (slot >= 0) & (slot < CAP)
            mine = jnp.where(hit & (code // SPAN == me), slot, -1)
            ids = token_ids.reshape(-1) - me * shard_rows
            chosen = jnp.max(jnp.where(mine[None, :] == jnp.arange(rows_list.size)[:, None], ids[None, :], 0), axis=1)
            v = gather_all(n, rows(CAP, chosen, word_shard), total)
            return r + 1, place(wanted(jnp.where(hit, code // SPAN * CAP + slot, -1)), v, u)

        _, u = lax.while_loop(lambda c: c[0] < rounds, more, (jnp.int32(0), u))
        t = jnp.arange(code.size, dtype=jnp.int32)
        t = jnp.where(t // seq == core, t % seq, jnp.clip(t % seq - me * blk, 0, blk - 1) + seq)
        at = jnp.where(rounds > 0, t, code // SPAN * CAP + jnp.minimum(code % SPAN, CAP - 1))

        qkv, embed = project(n, meta, at, u, pos_table, ln_gain[None], ln_bias[None], w_own, w_par, b_own, b_par)
        ctx = attention(n, qkv.reshape(2, 3, H, E, seq)).reshape(n, 2 * H * E, seq // n)
        resid_out = output(n, meta, ctx, embed, b_out[None], pieces, owners, lows)
        return resid_out, embed

    in_specs = (P("dp", None), P("tp", None), P(None, None), P(None), P(None), P(None, None, "tp", None), P(None, "tp", None), P("tp", None, None), P(None))
    out_specs = (P("dp", "tp", None), P("dp", "tp", None))
    return jax.shard_map(local_step, mesh=mesh, in_specs=in_specs, out_specs=out_specs, check_vma=False)
```

```python
import functools

import jax
import jax.numpy as jnp
from jax import lax
from jax.experimental import pallas as pl
from jax.experimental.pallas import tpu as pltpu
from jax.sharding import PartitionSpec as P

MESH = pl.DeviceIdType.MESH


class Peers:
    def __init__(self, n):
        self.n = n
        self.me = lax.axis_index("tp")
        self.chip, self.core = lax.div(self.me, 2), lax.rem(self.me, 2)
        self.plus, self.minus, self.opp = self.near(1), self.near(-1), self.near(2)
        self.partner = self.other(self.me)

    def near(self, s):
        chips = self.n // 2
        return lax.rem(self.chip + s + chips, chips) * 2 + self.core

    def other(self, d):
        return d + 1 - 2 * self.core

    def greet(self, devices):
        barrier = pltpu.get_barrier_semaphore()
        for d in devices:
            pl.semaphore_signal(barrier, inc=1, device_id={"tp": d}, device_id_type=MESH)
        pl.semaphore_wait(barrier, len(devices))


def gather_all_kernel(n, S, src_ref, all_ref, loc_sem, send_sem, recv_sem):
    cap = src_ref.shape[0]

    def of(d):
        return all_ref.at[pl.ds(d * cap, cap)]
    chips = n // 2
    me = lax.axis_index("tp")
    chip, core = me // 2, lax.rem(me, 2)
    def at(c):
        return lax.rem(c + chips, chips) * 2 + core
    plus, minus, opp = at(chip + 1), at(chip - 1), at(chip + 2)
    partner = me + 1 - 2 * core
    P = 2 * S
    step = src_ref.shape[0] // P

    barrier = pltpu.get_barrier_semaphore()
    for d in (plus, minus, partner):
        pl.semaphore_signal(barrier, inc=1, device_id={"tp": d}, device_id_type=MESH)
    pl.semaphore_wait(barrier, 3)

    started = []
    def rc(src, dst, ch, k, dev):
        return pltpu.make_async_remote_copy(src_ref=src, dst_ref=dst, send_sem=send_sem.at[ch, k], recv_sem=recv_sem.at[ch, k],
                                            device_id={"tp": dev}, device_id_type=MESH)
    def go(src, dst, ch, k, dev):
        c = rc(src, dst, ch, k, dev)
        c.start()
        started.append(c)
    def piece(ref, k):
        return ref.at[pl.ds(k * step, step)]
    first, last = list(range(S)), list(range(S, P))
    for a, b in zip(first, last):
        go(piece(src_ref, a), piece(of(me), a), 0, a, plus)
        go(piece(src_ref, b), piece(of(me), b), 1, b, minus)
    for a, b in zip(first, last):
        go(piece(src_ref, b), piece(of(me), b), 0, b, plus)
        go(piece(src_ref, a), piece(of(me), a), 1, a, minus)
    go(src_ref, of(me), 4, 0, partner)
    loc = pltpu.make_async_copy(src_ref, of(me), loc_sem)
    loc.start()
    def got(owner, ch, k):
        r = piece(of(owner), k)
        rc(r, r, ch, k, partner).wait_recv()
        return r
    for a, b in zip(first, last):
        r = got(minus, 0, a)
        go(r, r, 2, a, plus)
        go(r, r, 5, a, partner)
        r = got(plus, 1, b)
        go(r, r, 3, b, minus)
        go(r, r, 6, b, partner)
    for a, b in zip(first, last):
        r = got(minus, 0, b)
        go(r, r, 5, b, partner)
        r = got(plus, 1, a)
        go(r, r, 6, a, partner)
    for a, b in zip(first, last):
        r = got(opp, 2, a)
        go(r, r, 7, a, partner)
        r = got(opp, 3, b)
        go(r, r, 7, b, partner)
    other = lambda d: d + 1 - 2 * core
    r = of(partner)
    rc(r, r, 4, 0, partner).wait_recv()
    for k in range(P):
        got(other(minus), 5, k)
        got(other(plus), 6, k)
        got(other(opp), 7, k)
    loc.wait()
    for c in started:
        c.wait_send()


def gather_all(n, rows, total, S=2, cid=0):
    return pl.pallas_call(
        functools.partial(gather_all_kernel, n, S),
        out_shape=jax.ShapeDtypeStruct((total,) + rows.shape[1:], rows.dtype),
        in_specs=[pl.BlockSpec(memory_space=pltpu.VMEM)],
        out_specs=pl.BlockSpec(memory_space=pl.ANY),
        scratch_shapes=[pltpu.SemaphoreType.DMA, pltpu.SemaphoreType.DMA((8, 2 * S)), pltpu.SemaphoreType.DMA((8, 2 * S))],
        compiler_params=pltpu.CompilerParams(collective_id=cid, has_side_effects=True),
        name="gather_all",
    )(rows)


SPAN_BITS = 13
SPAN = 1 << SPAN_BITS


def pick_kernel(n, shard_rows, cap, nb, ids_ref, table_ref, code_ref, at_ref, cnt_ref, out_ref,
                ids, col, wcol, first, wanted, list_ref, buf, scr, list_sem, sem):
    me = lax.axis_index("tp")
    R, L = ids.shape
    G, Q = 8, 4
    lane = lax.broadcasted_iota(jnp.int32, (8, L), 1)
    sub = lax.broadcasted_iota(jnp.int32, (8, L), 0)
    for r in range(R):
        b, o = divmod(r * L, ids_ref.shape[1])
        ids[r:r + 1, :] = ids_ref[b:b + 1, o:o + L]

    def columns(*pairs):
        @pl.loop(0, R // Q)
        def _(g):
            for k in range(Q):
                a = g * Q + k
                for src, dst in pairs:
                    dst[pl.ds(pl.multiple_of(a * L, L), L), :] = jnp.broadcast_to(src[pl.ds(a, 1), :], (L, L)).T

    def against(bg, start, step):
        acc = start
        def body(a, acc):
            acc = list(acc)
            for k in range(L // 8):
                at = pl.ds(pl.multiple_of(a * L + k * 8, 8), 8)
                step(acc, at, k, range(G), -1)
            return tuple(acc)
        acc = list(lax.fori_loop(0, bg * G, body, tuple(acc)))
        for d in range(G):
            for k in range(L // 8):
                step(acc, pl.ds((bg * G + d) * L + k * 8, 8), k, range(d, G), d)
        return acc

    def wide(ref, bg):
        return [jnp.broadcast_to(ref[bg * G + i:bg * G + i + 1, :], (8, L)) for i in range(G)]

    columns((ids, col))
    for bg in range(R // G):
        rows = wide(ids, bg)
        def seen(acc, at, k, which, same):
            c = col[at, :]
            for i in which:
                hit = c == rows[i]
                if i == same:
                    hit = hit & (k * 8 + sub < lane)
                acc[i] = jnp.where(hit, 1, acc[i])
        acc = against(bg, [jnp.zeros((8, L), jnp.int32)] * G, seen)
        for i in range(G):
            first[bg * G + i:bg * G + i + 1, :] = 1 - jnp.max(acc[i], axis=0, keepdims=True)

    x = ids[...]
    owner = jnp.zeros((R, L), jnp.int32)
    for o in range(1, n):
        owner = owner + jnp.where(x >= o * shard_rows, 1, 0)
    isf = first[...] == 1
    one = jnp.concatenate([jnp.where(isf & (owner == o), 1.0, 0.0) for o in range(n)], axis=0).astype(jnp.bfloat16)
    up = (lax.broadcasted_iota(jnp.int32, (L, L), 0) < lax.broadcasted_iota(jnp.int32, (L, L), 1)).astype(jnp.float32).astype(jnp.bfloat16)
    prefix = jnp.dot(one, up, preferred_element_type=jnp.float32)
    tot = jnp.dot(one, jnp.ones((L, L), jnp.bfloat16), preferred_element_type=jnp.float32)
    r = lax.broadcasted_iota(jnp.int32, (n * R, n * R), 0)
    c = lax.broadcasted_iota(jnp.int32, (n * R, n * R), 1)
    low = ((r // R == c // R) & (c < r)).astype(jnp.float32).astype(jnp.bfloat16)
    off = jnp.dot(low, tot.astype(jnp.bfloat16), preferred_element_type=jnp.float32)
    pos = prefix + off
    slot = jnp.zeros((R, L), jnp.float32)
    most = jnp.zeros((1, L), jnp.float32)
    for o in range(n):
        slot = jnp.where(owner == o, pos[o * R:(o + 1) * R], slot)
        most = jnp.maximum(most, (off + tot)[(o + 1) * R - 1:(o + 1) * R])
    cnt_ref[...] = most.astype(jnp.int32)
    code_ref[...] = jnp.where(isf, owner * SPAN + slot.astype(jnp.int32), -1)
    first[...] = jnp.where(isf, x, -1)
    columns((first, col), (code_ref, wcol))

    for bg in range(R // G):
        rows = wide(ids, bg)
        def take(acc, at, k, which, same):
            c, w = col[at, :], wcol[at, :]
            for i in which:
                acc[i] = jnp.where(c == rows[i], w, acc[i])
        acc = against(bg, [jnp.zeros((8, L), jnp.int32)] * G, take)
        for i in range(G):
            code_ref[bg * G + i:bg * G + i + 1, :] = jnp.max(acc[i], axis=0, keepdims=True)
    code = code_ref[...]
    at_ref[...] = lax.shift_right_logical(code, SPAN_BITS) * cap + jnp.minimum(lax.bitwise_and(code, SPAN - 1), cap - 1)

    K = wanted.shape[0]
    want = [me * SPAN + i * L + lane for i in range(K)]
    def body(a, acc):
        acc = list(acc)
        for k in range(L // 8):
            at = pl.ds(pl.multiple_of(a * L + k * 8, 8), 8)
            c, w = col[at, :], wcol[at, :]
            for i in range(K):
                acc[i] = jnp.where(w == want[i], c, acc[i])
        return tuple(acc)
    acc = lax.fori_loop(0, R, body, tuple(jnp.zeros((8, L), jnp.int32) for _ in range(K)))
    for i in range(K):
        wanted[i:i + 1, :] = jnp.maximum(jnp.max(acc[i], axis=0, keepdims=True) - me * shard_rows, 0)
    listed = pltpu.make_async_copy(wanted, list_ref, list_sem)
    listed.start()
    listed.wait()
    take_rows(cap, nb, lambda k: list_ref[lax.shift_right_logical(k, 7), lax.bitwise_and(k, L - 1)], table_ref, out_ref, buf, scr, sem)


def take_rows(cap, nb, row_of, table_ref, out_ref, buf, scr, sem):
    T = table_ref.shape[1] // 128
    U = 8

    def copy(k):
        base = pl.multiple_of(lax.bitwise_and(row_of(k), -8), 8)
        s = lax.bitwise_and(k, nb - 1)
        return pltpu.make_async_copy(table_ref.at[pl.ds(base, 8)], buf.at[s], sem.at[s])

    @pl.loop(0, nb)
    def _(k):
        copy(k).start()

    def group(q, more):
        for u in range(U):
            k = q * U + u
            s = lax.bitwise_and(k, nb - 1)
            copy(k).wait()
            for j in range(T):
                scr[u, j * 8:(j + 1) * 8, :] = buf[s, :, j * 128:(j + 1) * 128].astype(jnp.float32)
            r = lax.bitwise_and(row_of(k), 7)
            out_ref[k] = scr[u, pl.ds(r, T, stride=8), :].astype(jnp.bfloat16)
        if more:
            for u in range(U):
                copy(q * U + u + nb).start()

    pl.loop(0, (cap - nb) // U)(lambda q: group(q, True))
    pl.loop((cap - nb) // U, cap // U)(lambda q: group(q, False))


def pick(n, shard_rows, cap, ids, table, nb=32):
    R, L = ids.size // 128, 128
    K = -(-cap // L)
    T = table.shape[1] // 128
    V = pl.BlockSpec(memory_space=pltpu.VMEM)
    i32 = lambda *shape: jax.ShapeDtypeStruct(shape, jnp.int32)
    vm = lambda *shape: pltpu.VMEM(shape, jnp.int32)
    return pl.pallas_call(
        functools.partial(pick_kernel, n, shard_rows, cap, nb),
        out_shape=(i32(R, L), i32(R, L), i32(1, L), jax.ShapeDtypeStruct((cap, T, 128), table.dtype)),
        in_specs=[V, pl.BlockSpec(memory_space=pl.ANY)],
        out_specs=(V, V, V, V),
        scratch_shapes=[vm(R, L), vm(R * L, L), vm(R * L, L), vm(R, L), vm(K, L), pltpu.SMEM((K, L), jnp.int32),
                        pltpu.VMEM((nb, 8, T * 128), table.dtype), pltpu.VMEM((8, T * 8, 128), jnp.float32), pltpu.SemaphoreType.DMA, pltpu.SemaphoreType.DMA((nb,))],
        cost_estimate=pl.CostEstimate(flops=2 * 10**10, bytes_accessed=cap * 8 * T * 256, transcendentals=0),
        name="pick",
    )(ids, table)


def rows_kernel(cap, nb, list_ref, table_ref, out_ref, buf, scr, sem):
    take_rows(cap, nb, lambda k: list_ref[k], table_ref, out_ref, buf, scr, sem)


def rows(cap, lst, table, nb=32):
    T = table.shape[1] // 128
    return pl.pallas_call(
        functools.partial(rows_kernel, cap, nb),
        out_shape=jax.ShapeDtypeStruct((cap, T, 128), table.dtype),
        grid_spec=pltpu.PrefetchScalarGridSpec(
            num_scalar_prefetch=1, grid=(),
            in_specs=[pl.BlockSpec(memory_space=pl.ANY)],
            out_specs=pl.BlockSpec(memory_space=pltpu.VMEM),
            scratch_shapes=[pltpu.VMEM((nb, 8, table.shape[1]), table.dtype), pltpu.VMEM((8, T * 8, 128), jnp.float32), pltpu.SemaphoreType.DMA((nb,))]),
        name="rows",
    )(lst, table)


EPS = 1e-5


def project_kernel(n, tb, seq, blk, steps, chunk, code, u_hbm, pos_hbm, gain_ref, bias_ref, wa_hbm, wb_hbm, ba_ref, bb_ref,
                   qkv_ref, emb_ref, u, w, bc, pos, xs, hs, usem, wsem, psem):
    step = pl.program_id(0)
    q = Peers(n)
    me = q.me
    base = q.core * seq
    T = u.shape[1]
    M = wa_hbm.shape[0]
    inv = 1.0 / (T * 128)

    def load_u():
        return pltpu.make_async_copy(u_hbm, u, usem)
    def load_w(k):
        return pltpu.make_async_copy((wa_hbm, wb_hbm)[k], w.at[lax.rem(q.core + k, 2)], wsem.at[k])
    def load_pos(i):
        return pltpu.make_async_copy(pos_hbm.at[pl.ds(i * tb, tb)], pos.at[lax.rem(i, 2)], psem.at[lax.rem(i, 2)])
    def load_own():
        return pltpu.make_async_copy(pos_hbm.at[pl.ds(me * blk, blk)], pos.at[steps % 2, pl.ds(0, blk)], psem.at[steps % 2])

    def fetch(slot, first):
        for r in range(8):
            xs[slot, pl.ds(r, T, stride=8), :] = u[code[first + r]].astype(jnp.float32)

    def tile(slot, j):
        return xs[slot, j * 8:(j + 1) * 8, :]

    def lanes(j):
        return slice(j * 128, (j + 1) * 128)

    def norm(i, g, lane_slot):
        t = pl.multiple_of(g * 16, 16)
        out = []
        for half in range(2):
            slot = lane_slot * 2 + half
            fetch(slot, base + i * tb + g * 16 + half * 8)
            p = pos.at[lax.rem(i, 2), pl.ds(t, 16), :]
            s = None
            for j in range(T):
                e = (tile(slot, j) + p[half * 8:half * 8 + 8, lanes(j)].astype(jnp.float32)).astype(jnp.bfloat16).astype(jnp.float32)
                xs[slot, j * 8:(j + 1) * 8, :] = e
                s = e if s is None else s + e
            mean = jnp.broadcast_to(jnp.sum(s, axis=1, keepdims=True) * inv, (8, 128))
            s = None
            for j in range(T):
                c = tile(slot, j) - mean
                s = c * c if s is None else s + c * c
            var = jnp.sum(s, axis=1, keepdims=True) * inv
            rs = jnp.broadcast_to(lax.rsqrt(var + EPS), (8, 128))
            out.append((slot, mean, rs))
        for j in range(T):
            y = [(tile(slot, j) - mean) * rs * gain_ref[:, lanes(j)] + bias_ref[:, lanes(j)] for slot, mean, rs in out]
            hs[lax.rem(i, 2), pl.ds(t, 16), lanes(j)] = jnp.concatenate(y, axis=0).astype(jnp.bfloat16)

    def embed(g, lane_slot):
        per = blk // 16
        b = lax.div(g, per)
        t = pl.multiple_of(lax.rem(g, per) * 16, 16)
        for half in range(2):
            fetch(lane_slot * 2 + half, b * seq + me * blk + t + half * 8)
        p = pos.at[steps % 2, pl.ds(t, 16), :]
        for j in range(T):
            e = jnp.concatenate([tile(lane_slot * 2, j), tile(lane_slot * 2 + 1, j)], axis=0) + p[:, lanes(j)].astype(jnp.float32)
            emb_ref[b, pl.ds(t, 16), lanes(j)] = e.astype(jnp.bfloat16)

    @pl.when(step == 0)
    def _():
        load_u().start()
        heads, E = 12, M // 12
        for k, b in enumerate((ba_ref, bb_ref)):
            for r in range(heads):
                bc[lax.rem(q.core + k, 2), r * E:(r + 1) * E, :] = jnp.broadcast_to(b[r:r + 1, :], (128, 128)).T[0:E, :]
        load_pos(0).start()
        for k in range(2):
            load_w(k).start()
        load_pos(1).start()
        load_u().wait()
        load_pos(0).wait()
        @pl.loop(0, tb // 64)
        def _(g):
            for j in range(4):
                norm(0, g * 4 + j, j)
        for k in range(2):
            load_w(k).wait()

    def sweep(beside):
        per = M // chunk
        h = hs.at[lax.rem(step, 2)]
        for k in range(2):
            @pl.loop(0, per)
            def _(m):
                at = pl.multiple_of(m * chunk, 32)
                o = lax.dot_general(w[k, pl.ds(at, chunk), :], h[...], (((1,), (1,)), ((), ())), preferred_element_type=jnp.float32)
                b = jnp.concatenate([bc[k, pl.ds(at, chunk), :]] * (tb // 128), axis=1)
                qkv_ref[k, pl.ds(at, chunk), :] = (o + b).astype(jnp.bfloat16)
                n = tb // 16 // (2 * per)
                for j in range(n):
                    beside((k * per + m) * n + j, j % 4)

    @pl.when(step < steps - 1)
    def _():
        load_pos(step + 1).wait()
        @pl.when(step + 2 < steps)
        def _():
            load_pos(step + 2).start()
        @pl.when(step + 2 == steps)
        def _():
            load_own().start()
        sweep(lambda g, j: norm(step + 1, g, j))

    @pl.when(step == steps - 1)
    def _():
        load_own().wait()
        sweep(embed)


def project(n, at, u, pos, gain, bias, wa, wb, ba, bb, tb=512, chunk=288):
    seq, D = pos.shape
    blk = seq // n
    steps = seq // tb
    M = wa.shape[0]
    A = pl.BlockSpec(memory_space=pl.ANY)
    one = lambda shape: pl.BlockSpec(shape, lambda i, *_: (0,) * len(shape), pipeline_mode=pl.Buffered(1))
    return pl.pallas_call(
        functools.partial(project_kernel, n, tb, seq, blk, steps, chunk),
        out_shape=(jax.ShapeDtypeStruct((2, M, seq), jnp.bfloat16), jax.ShapeDtypeStruct((2, blk, D), jnp.bfloat16)),
        grid_spec=pltpu.PrefetchScalarGridSpec(
            num_scalar_prefetch=1, grid=(steps,),
            in_specs=[A, A, one((1, D)), one((1, D)), A, A, one(ba.shape), one(bb.shape)],
            out_specs=(pl.BlockSpec((2, M, tb), lambda i, *_: (0, 0, i)), pl.BlockSpec((2, blk, D), lambda i, *_: (0, 0, 0), pipeline_mode=pl.Buffered(1))),
            scratch_shapes=[pltpu.VMEM(u.shape, u.dtype), pltpu.VMEM((2, M, D), wa.dtype), pltpu.VMEM((2, M, 128), jnp.float32), pltpu.VMEM((2, tb, D), pos.dtype),
                            pltpu.VMEM((8, D // 128 * 8, 128), jnp.float32), pltpu.VMEM((2, tb, D), jnp.bfloat16),
                            pltpu.SemaphoreType.DMA, pltpu.SemaphoreType.DMA((2,)), pltpu.SemaphoreType.DMA((2,))]),
        compiler_params=pltpu.CompilerParams(vmem_limit_bytes=63 * 2**20),
        cost_estimate=pl.CostEstimate(flops=4 * seq * M * D, bytes_accessed=50 * 2**20, transcendentals=0),
        name="project",
    )(at, u, pos, gain, bias, wa, wb, ba, bb)


def attend_kernel(n, scale, qb, nb, early, where, qkv_ref, emb_hbm, bias_ref, *refs):
    pieces, (out_ref, kk, vv, sc, ctx, got, w, a, acc, emb, load_sem, pass_send, pass_recv, emb_sem, send_sem, recv_sem) = refs[:len(where)], refs[len(where):]
    E, S = qkv_ref.shape[3:]
    heads = got.shape[1] // E
    N = S // qb
    c = scale * 1.4426950408889634
    q = Peers(n)
    me, core = q.me, q.core
    head = pl.program_id(0)
    cut = early * E // 256 * 256
    owners = {0: me, 1: q.plus, 2: q.opp, -1: q.minus}

    def loads():
        cs = []
        for i, (ref, (away, low)) in enumerate(zip(pieces, where)):
            dst = w.at[owners[away], pl.ds(low, ref.shape[0])]
            cs.append(pltpu.make_async_copy(ref, dst, load_sem.at[i]))
            cs.append(pltpu.make_async_remote_copy(src_ref=ref, dst_ref=dst, send_sem=pass_send.at[i], recv_sem=pass_recv.at[i], device_id={"tp": q.partner}, device_id_type=MESH))
        return cs

    def send(h, s):
        to = lax.rem(me + s, n)
        return pltpu.make_async_remote_copy(src_ref=ctx.at[h, to], dst_ref=got.at[me, pl.ds(pl.multiple_of(h * E, 32), E)],
                                            send_sem=send_sem.at[s], recv_sem=recv_sem.at[lax.div(h, early), s], device_id={"tp": to}, device_id_type=MESH)

    load_emb = pltpu.make_async_copy(emb_hbm, emb, emb_sem)

    @pl.when(head == 0)
    def _():
        q.greet([lax.rem(me + s, n) for s in range(1, n)])
        vv[E:, :] = jnp.where(lax.broadcasted_iota(jnp.int32, (vv.shape[0] - E, S), 0) == 0, 1.0, 0.0).astype(jnp.bfloat16)

    @pl.when(head > 0)
    def _():
        for s in range(1, n):
            send(head - 1, s).start()

    @pl.when(head == 1)
    def _():
        for c_ in loads():
            c_.start()
        load_emb.start()

    for t in range(0, S, 128):
        kk[t:t + 128, :] = qkv_ref[0, 1, 0, :, t:t + 128].astype(jnp.float32).T.astype(jnp.bfloat16)
    vv[0:E, :] = qkv_ref[0, 2, 0]
    keep = lax.broadcasted_iota(jnp.int32, (qb, qb), 0) <= lax.broadcasted_iota(jnp.int32, (qb, qb), 1)

    def scores(i, k, m):
        s = jnp.dot(kk[k * qb:(k + 1) * qb, :], qkv_ref[0, 0, 0, :, i * qb:(i + 1) * qb], preferred_element_type=jnp.float32)
        if k == i:
            s = jnp.where(keep, s, -jnp.inf)
        sc[i % 2, k * qb:(k + 1) * qb, :] = s
        top = jnp.max(s.reshape(qb // 8, 8, qb), axis=0)
        return top if m is None else jnp.maximum(m, top)

    def weigh(i, k, mc, o):
        s = sc[i % 2, k * qb:(k + 1) * qb, :]
        p = jnp.exp2(s * c - mc).astype(jnp.bfloat16)
        d = jnp.dot(vv[:, k * qb:(k + 1) * qb], p, preferred_element_type=jnp.float32)
        return d if o is None else o + d

    m = scores(0, 0, None)
    for i in range(N):
        mc = jnp.max(m, axis=0, keepdims=True) * c
        o = m = None
        for k in range(i + 2):
            if i + 1 < N:
                m = scores(i + 1, k, m)
            if k <= i:
                o = weigh(i, k, mc, o)
        ctx[head, i] = (o[0:E] * (1.0 / o[E:E + 1])).astype(jnp.bfloat16)
    got[me, pl.ds(pl.multiple_of(head * E, 32), E), :] = ctx[head, me]

    @pl.when(head == heads - 1)
    def _():
        for s in range(1, n):
            send(head, s).start()
        K = got.shape[1]

        def arrive(group, low, high):
            for s in range(1, n):
                fr = lax.rem(me - s + n, n)
                r = got.at[fr, pl.ds(low, high - low)]
                pltpu.make_async_remote_copy(src_ref=r, dst_ref=r, send_sem=send_sem.at[s], recv_sem=recv_sem.at[group, s], device_id={"tp": fr}, device_id_type=MESH).wait_recv()

        def turn_over(low, high):
            for s in range(n):
                for k in range(low, high, 128):
                    for t in range(0, qb, 128):
                        a[(s % 2) * qb + t:(s % 2) * qb + t + 128, (s // 2) * K + k:(s // 2) * K + k + 128] = got[s, k:k + 128, t:t + 128].astype(jnp.float32).T.astype(jnp.bfloat16)

        def part(low, high, cols):
            o = None
            for i in range(n // 2):
                d = jnp.dot(a[:, i * K + low:i * K + high], w[2 * i:2 * i + 2, :, cols].reshape(K, nb)[low:high], preferred_element_type=jnp.float32)
                o = d if o is None else o + d
            return o

        arrive(0, 0, early * E)
        turn_over(0, cut)
        for c_ in loads():
            c_.wait()
        load_emb.wait()

        @pl.loop(0, w.shape[2] // nb)
        def _(j):
            cols = pl.ds(pl.multiple_of(j * nb, nb), nb)
            acc[:, cols] = part(0, cut, cols) + bias_ref[:, cols]

        arrive(1, early * E, K)
        turn_over(cut, K)

        @pl.loop(0, w.shape[2] // nb)
        def _(j):
            cols = pl.ds(pl.multiple_of(j * nb, nb), nb)
            o = part(cut, K, cols) + acc[:, cols]
            for b in range(2):
                out_ref[b, :, cols] = (emb[b, :, cols].astype(jnp.float32) + o[b * qb:(b + 1) * qb]).astype(jnp.bfloat16)

        for s in range(1, n):
            r = got.at[lax.rem(me - s + n, n)]
            pltpu.make_async_remote_copy(src_ref=r, dst_ref=r, send_sem=send_sem.at[s], recv_sem=recv_sem.at[0, s], device_id={"tp": q.partner}, device_id_type=MESH).wait_send()


def attend(n, qkv, pieces, where, emb, bias, early=6, nb=256, cid=1, qb=256):
    heads, E, S = 2 * qkv.shape[2], *qkv.shape[3:]
    H = heads // 2
    D = emb.shape[2]
    A = pl.BlockSpec(memory_space=pl.ANY)
    one = lambda shape: pl.BlockSpec(shape, lambda h: (0,) * len(shape), pipeline_mode=pl.Buffered(1))
    bf = jnp.bfloat16
    return pl.pallas_call(
        functools.partial(attend_kernel, n, E ** -0.5, qb, nb, early, where),
        out_shape=jax.ShapeDtypeStruct(emb.shape, bf),
        grid=(heads,),
        in_specs=[pl.BlockSpec((1, 3, 1, E, S), lambda h: (h // H, 0, h % H, 0, 0)), A, one(bias.shape)] + [A] * len(pieces),
        out_specs=one(emb.shape),
        scratch_shapes=[pltpu.VMEM((S, E), bf), pltpu.VMEM((E + 16, S), bf), pltpu.VMEM((2, S, qb), jnp.float32),
                        pltpu.VMEM((heads, n, E, qb), bf), pltpu.VMEM((n, heads * E, qb), bf), pltpu.VMEM((n, H * E, D), bf), pltpu.VMEM((2 * qb, n * H * E), bf),
                        pltpu.VMEM((2 * qb, D), jnp.float32), pltpu.VMEM(emb.shape, bf),
                        *[pltpu.SemaphoreType.DMA((len(pieces),))] * 3, pltpu.SemaphoreType.DMA, pltpu.SemaphoreType.DMA((n,)), pltpu.SemaphoreType.DMA((2, n))],
        compiler_params=pltpu.CompilerParams(collective_id=cid, has_side_effects=True, vmem_limit_bytes=62 * 2**20),
        name="attend",
    )(qkv, emb, bias, *pieces)


CAP = 264


def place_kernel(code_ref, u_ref, x_ref, out_ref, sem):
    @pl.loop(0, code_ref.shape[0])
    def _(t):
        c = code_ref[t]

        @pl.when(c >= 0)
        def _():
            copy = pltpu.make_async_copy(u_ref.at[c], out_ref.at[t], sem)
            copy.start()
            copy.wait()


def place(at, u, x):
    A = pl.BlockSpec(memory_space=pl.ANY)
    return pl.pallas_call(
        place_kernel,
        out_shape=jax.ShapeDtypeStruct(x.shape, x.dtype),
        grid_spec=pltpu.PrefetchScalarGridSpec(num_scalar_prefetch=1, grid=(), in_specs=[A, A], out_specs=A, scratch_shapes=[pltpu.SemaphoreType.DMA]),
        input_output_aliases={2: 0},
        name="place",
    )(at, u, x)


def solution(mesh):
    n = mesh.shape["tp"]
    def local_step(token_ids, word_shard, pos_table, ln_gain, ln_bias, w_qkv, b_qkv, w_out, b_out):
        me = lax.axis_index("tp")
        core = lax.rem(me, 2)
        seq, D = pos_table.shape
        H, E = w_qkv.shape[2:]
        shard_rows = word_shard.shape[0]
        w_own = jnp.transpose(w_qkv, (1, 2, 3, 0)).reshape(3 * H * E, D)
        b_own = jnp.pad(b_qkv.reshape(3 * H, E), ((0, 4), (0, 128 - E)))
        v_own = w_out.reshape(H * E, D)
        swap = [(d, d ^ 1) for d in range(n)]
        ring = lambda step: [(d, (d + 2 * step) % n) for d in range(n)]
        w_par, b_par = lax.ppermute(w_own, "tp", swap), lax.ppermute(b_own, "tp", swap)
        send = lambda x, step: lax.ppermute(x, "tp", ring(step))
        v0, v1, v2 = w_out[0], w_out[1], w_out[2:].reshape((H - 2) * E, D)
        minus0, plus0, minus1, plus1 = send(v0, 1), send(v0, -1), send(v1, 1), send(v1, -1)
        blk = seq // n
        total = max(n * CAP, seq + blk)
        code, at, most, u = pick(n, shard_rows, CAP, token_ids, word_shard)
        code, at, most = code.reshape(-1), at.reshape(-1), most[0, 0]
        u = gather_all(n, u, total)

        rounds = jnp.where(most > CAP, (most + CAP - 1) // CAP, 0)

        def wanted(x):
            x = x.reshape(2, seq)
            own = lax.dynamic_index_in_dim(x, core, 0, keepdims=False)
            other = lax.dynamic_index_in_dim(x, 1 - core, 0, keepdims=False)
            return jnp.concatenate([own, lax.dynamic_slice_in_dim(other, me * blk, blk)])

        t = jnp.arange(2 * seq, dtype=jnp.int32)
        t = jnp.where(t // seq == core, t % seq, jnp.clip(t % seq - me * blk, 0, blk - 1) + seq)

        def more(carry):
            r, u, _ = carry
            slot = code % SPAN - r * CAP
            hit = (slot >= 0) & (slot < CAP)
            mine = jnp.where(hit & (code // SPAN == me), slot, -1)
            ids = token_ids.reshape(-1) - me * shard_rows
            chosen = jnp.max(jnp.where(mine[None, :] == jnp.arange(CAP)[:, None], ids[None, :], 0), axis=1)
            v = gather_all(n, rows(CAP, chosen, word_shard), total)
            return r + 1, place(wanted(jnp.where(hit, code // SPAN * CAP + slot, -1)), v, u), t

        _, u, at = lax.while_loop(lambda c: c[0] < rounds, more, (jnp.int32(0), u, at))

        v2, minus0_, plus1_, u = lax.optimization_barrier((v2, minus0, plus1, u))
        minus2, plus2, opp0, opp1, opp2 = send(v2, 1), send(v2, -1), send(minus0_, 1), send(plus1_, -1), send(v2, 2)
        pieces = [v_own, minus0, plus0, minus1, plus1, minus2, plus2, opp0, opp1, opp2]
        where = ((0, 0), (-1, 0), (1, 0), (-1, E), (1, E), (-1, 2 * E), (1, 2 * E), (2, 0), (2, E), (2, 2 * E))
        qkv, embed = project(n, at, u, pos_table, ln_gain[None], ln_bias[None], w_own, w_par, b_own, b_par)
        resid_out = attend(n, qkv.reshape(2, 3, H, E, seq), pieces, where, embed, b_out[None])
        return resid_out, embed

    in_specs = (P("dp", None), P("tp", None), P(None, None), P(None), P(None), P(None, None, "tp", None), P(None, "tp", None), P("tp", None, None), P(None))
    out_specs = (P("dp", "tp", None), P("dp", "tp", None))
    return jax.shard_map(local_step, mesh=mesh, in_specs=in_specs, out_specs=out_specs, check_vma=False)
```

```python
import functools

import jax
import jax.numpy as jnp
from jax import lax
from jax.experimental import pallas as pl
from jax.experimental.pallas import tpu as pltpu
from jax.sharding import PartitionSpec as P

MESH = pl.DeviceIdType.MESH
VMEM = 63 * 2**20


class Peers:
    def __init__(self, n):
        self.n = n
        self.me = lax.axis_index("tp")
        self.chip, self.core = lax.div(self.me, 2), lax.rem(self.me, 2)
        self.plus, self.minus, self.opp = self.near(1), self.near(-1), self.near(2)
        self.partner = self.other(self.me)

    def near(self, s):
        chips = self.n // 2
        return lax.rem(self.chip + s + chips, chips) * 2 + self.core

    def other(self, d):
        return d + 1 - 2 * self.core

    def greet(self, devices):
        barrier = pltpu.get_barrier_semaphore()
        for d in devices:
            pl.semaphore_signal(barrier, inc=1, device_id={"tp": d}, device_id_type=MESH)
        pl.semaphore_wait(barrier, len(devices))


class Spread:
    CHANNELS = 9

    def __init__(self, peers, own, place, send_sem, recv_sem):
        self.q, self.own, self.place, self.send_sem, self.recv_sem = peers, own, place, send_sem, recv_sem

    def half(self, ref, i):
        rows = ref.shape[0] // 2
        return ref.at[pl.ds(i * rows, rows)]

    def copy(self, channel, p, src, dst, to):
        return pltpu.make_async_remote_copy(src_ref=src, dst_ref=dst, send_sem=self.send_sem.at[channel, p], recv_sem=self.recv_sem.at[channel, p],
                                            device_id={"tp": to}, device_id_type=MESH)

    def got(self, channel, p, ref):
        self.copy(channel, p, ref, ref, self.q.partner).wait_recv()

    def begin(self, p):
        q = self.q
        for channel, to in ((0, q.plus), (1, q.minus), (4, q.partner)):
            self.copy(channel, p, self.own(p), self.place(q.me, p), to).start()

    def turn(self, p):
        q = self.q
        for i, (d, to) in enumerate(((q.minus, q.plus), (q.plus, q.minus))):
            ref = self.place(d, p)
            self.got(i, p, ref)
            self.copy(2 + i, p, self.half(ref, i), self.half(ref, i), to).start()
            self.copy(5 + i, p, ref, ref, q.partner).start()

    def last(self, p):
        q = self.q
        for i in range(2):
            c = self.half(self.place(q.opp, p), i)
            self.got(2 + i, p, c)
            self.copy(7 + i, p, c, c, q.partner).start()

    def finish(self, p):
        q = self.q
        own, a, b, c = (self.place(d, p) for d in (q.partner, q.other(q.minus), q.other(q.plus), q.other(q.opp)))
        for channel, ref in ((4, own), (5, a), (6, b), (7, self.half(c, 0)), (8, self.half(c, 1))):
            self.got(channel, p, ref)
        for channel, ref in ((0, own), (1, own), (4, own), (5, a), (6, b), (2, self.half(c, 0)), (3, self.half(c, 1)), (7, self.half(c, 0)), (8, self.half(c, 1))):
            self.copy(channel, p, ref, ref, q.partner).wait_send()


def gather_all_kernel(n, S, src_ref, all_ref, loc_sem, send_sem, recv_sem):
    cap = src_ref.shape[0]

    def of(d):
        return all_ref.at[pl.ds(d * cap, cap)]
    chips = n // 2
    me = lax.axis_index("tp")
    chip, core = me // 2, lax.rem(me, 2)
    def at(c):
        return lax.rem(c + chips, chips) * 2 + core
    plus, minus, opp = at(chip + 1), at(chip - 1), at(chip + 2)
    partner = me + 1 - 2 * core
    P = 2 * S
    step = src_ref.shape[0] // P

    barrier = pltpu.get_barrier_semaphore()
    for d in (plus, minus, partner):
        pl.semaphore_signal(barrier, inc=1, device_id={"tp": d}, device_id_type=MESH)
    pl.semaphore_wait(barrier, 3)

    started = []
    def rc(src, dst, ch, k, dev):
        return pltpu.make_async_remote_copy(src_ref=src, dst_ref=dst, send_sem=send_sem.at[ch, k], recv_sem=recv_sem.at[ch, k],
                                            device_id={"tp": dev}, device_id_type=MESH)
    def go(src, dst, ch, k, dev):
        c = rc(src, dst, ch, k, dev)
        c.start()
        started.append(c)
    def piece(ref, k):
        return ref.at[pl.ds(k * step, step)]
    first, last = list(range(S)), list(range(S, P))
    for a, b in zip(first, last):
        go(piece(src_ref, a), piece(of(me), a), 0, a, plus)
        go(piece(src_ref, b), piece(of(me), b), 1, b, minus)
    for a, b in zip(first, last):
        go(piece(src_ref, b), piece(of(me), b), 0, b, plus)
        go(piece(src_ref, a), piece(of(me), a), 1, a, minus)
    go(src_ref, of(me), 4, 0, partner)
    loc = pltpu.make_async_copy(src_ref, of(me), loc_sem)
    loc.start()
    def got(owner, ch, k):
        r = piece(of(owner), k)
        rc(r, r, ch, k, partner).wait_recv()
        return r
    for a, b in zip(first, last):
        r = got(minus, 0, a)
        go(r, r, 2, a, plus)
        go(r, r, 5, a, partner)
        r = got(plus, 1, b)
        go(r, r, 3, b, minus)
        go(r, r, 6, b, partner)
    for a, b in zip(first, last):
        r = got(minus, 0, b)
        go(r, r, 5, b, partner)
        r = got(plus, 1, a)
        go(r, r, 6, a, partner)
    for a, b in zip(first, last):
        r = got(opp, 2, a)
        go(r, r, 7, a, partner)
        r = got(opp, 3, b)
        go(r, r, 7, b, partner)
    other = lambda d: d + 1 - 2 * core
    r = of(partner)
    rc(r, r, 4, 0, partner).wait_recv()
    for k in range(P):
        got(other(minus), 5, k)
        got(other(plus), 6, k)
        got(other(opp), 7, k)
    loc.wait()
    for c in started:
        c.wait_send()


def gather_all(n, rows, total, S=2, cid=0):
    return pl.pallas_call(
        functools.partial(gather_all_kernel, n, S),
        out_shape=jax.ShapeDtypeStruct((total,) + rows.shape[1:], rows.dtype),
        in_specs=[pl.BlockSpec(memory_space=pltpu.VMEM)],
        out_specs=pl.BlockSpec(memory_space=pl.ANY),
        scratch_shapes=[pltpu.SemaphoreType.DMA, pltpu.SemaphoreType.DMA((8, 2 * S)), pltpu.SemaphoreType.DMA((8, 2 * S))],
        compiler_params=pltpu.CompilerParams(collective_id=cid, has_side_effects=True),
        name="gather_all",
    )(rows)


SPAN_BITS = 13
SPAN = 1 << SPAN_BITS


def pick_kernel(n, shard_rows, cap, soon, early, nb, ids_ref, table_ref, code_ref, at_ref, cnt_ref, out_ref,
                ids, col, wcol, first, wanted, list_ref, buf, scr, list_sem, sem):
    me = lax.axis_index("tp")
    R, L = ids.shape
    G, Q = 8, 4
    lane = lax.broadcasted_iota(jnp.int32, (8, L), 1)
    sub = lax.broadcasted_iota(jnp.int32, (8, L), 0)
    for r in range(R):
        o, b = divmod(r, ids_ref.shape[0])
        ids[r:r + 1, :] = ids_ref[b:b + 1, o * L:(o + 1) * L]

    def columns(*pairs):
        @pl.loop(0, R // Q)
        def _(g):
            for k in range(Q):
                a = g * Q + k
                for src, dst in pairs:
                    dst[pl.ds(pl.multiple_of(a * L, L), L), :] = jnp.broadcast_to(src[pl.ds(a, 1), :], (L, L)).T

    def against(bg, start, step):
        acc = start
        def body(a, acc):
            acc = list(acc)
            for k in range(L // 8):
                at = pl.ds(pl.multiple_of(a * L + k * 8, 8), 8)
                step(acc, at, k, range(G), -1)
            return tuple(acc)
        acc = list(lax.fori_loop(0, bg * G, body, tuple(acc)))
        for d in range(G):
            for k in range(L // 8):
                step(acc, pl.ds((bg * G + d) * L + k * 8, 8), k, range(d, G), d)
        return acc

    def wide(ref, bg):
        return [jnp.broadcast_to(ref[bg * G + i:bg * G + i + 1, :], (8, L)) for i in range(G)]

    columns((ids, col))
    for bg in range(R // G):
        rows = wide(ids, bg)
        def seen(acc, at, k, which, same):
            c = col[at, :]
            for i in which:
                hit = c == rows[i]
                if i == same:
                    hit = hit & (k * 8 + sub < lane)
                acc[i] = jnp.where(hit, 1, acc[i])
        acc = against(bg, [jnp.zeros((8, L), jnp.int32)] * G, seen)
        for i in range(G):
            first[bg * G + i:bg * G + i + 1, :] = 1 - jnp.max(acc[i], axis=0, keepdims=True)

    x = ids[...]
    owner = jnp.zeros((R, L), jnp.int32)
    for o in range(1, n):
        owner = owner + jnp.where(x >= o * shard_rows, 1, 0)
    isf = first[...] == 1
    one = jnp.concatenate([jnp.where(isf & (owner == o), 1.0, 0.0) for o in range(n)], axis=0).astype(jnp.bfloat16)
    up = (lax.broadcasted_iota(jnp.int32, (L, L), 0) < lax.broadcasted_iota(jnp.int32, (L, L), 1)).astype(jnp.float32).astype(jnp.bfloat16)
    prefix = jnp.dot(one, up, preferred_element_type=jnp.float32)
    tot = jnp.dot(one, jnp.ones((L, L), jnp.bfloat16), preferred_element_type=jnp.float32)
    r = lax.broadcasted_iota(jnp.int32, (n * R, n * R), 0)
    c = lax.broadcasted_iota(jnp.int32, (n * R, n * R), 1)
    low = ((r // R == c // R) & (c < r)).astype(jnp.float32).astype(jnp.bfloat16)
    off = jnp.dot(low, tot.astype(jnp.bfloat16), preferred_element_type=jnp.float32)
    pos = prefix + off
    slot = jnp.zeros((R, L), jnp.float32)
    most = jnp.zeros((1, L), jnp.float32)
    for o in range(n):
        slot = jnp.where(owner == o, pos[o * R:(o + 1) * R], slot)
        most = jnp.maximum(most, (off + tot)[(o + 1) * R - 1:(o + 1) * R])
    cnt_ref[0:1, :] = most.astype(jnp.int32)
    code_ref[...] = jnp.where(isf, owner * SPAN + slot.astype(jnp.int32), -1)
    first[...] = jnp.where(isf, x, -1)
    columns((first, col), (code_ref, wcol))

    for bg in range(R // G):
        rows = wide(ids, bg)
        def take(acc, at, k, which, same):
            c, w = col[at, :], wcol[at, :]
            for i in which:
                acc[i] = jnp.where(c == rows[i], w, acc[i])
        acc = against(bg, [jnp.zeros((8, L), jnp.int32)] * G, take)
        for i in range(G):
            code_ref[bg * G + i:bg * G + i + 1, :] = jnp.max(acc[i], axis=0, keepdims=True)
    code = code_ref[...]
    who, slot = lax.shift_right_logical(code, SPAN_BITS), lax.bitwise_and(code, SPAN - 1)
    at_ref[...] = jnp.where(slot < soon, who * soon + slot, n * soon + who * (cap - soon) + jnp.minimum(slot, cap - 1) - soon)
    seen = jnp.max(slot[0:early // L * ids_ref.shape[0], :], axis=0, keepdims=True)
    cnt_ref[1:2, :] = jnp.broadcast_to(jnp.max(seen, axis=1, keepdims=True) + 1, (1, L))

    K = wanted.shape[0]
    want = [me * SPAN + i * L + lane for i in range(K)]
    def body(a, acc):
        acc = list(acc)
        for k in range(L // 8):
            at = pl.ds(pl.multiple_of(a * L + k * 8, 8), 8)
            c, w = col[at, :], wcol[at, :]
            for i in range(K):
                acc[i] = jnp.where(w == want[i], c, acc[i])
        return tuple(acc)
    acc = lax.fori_loop(0, R, body, tuple(jnp.zeros((8, L), jnp.int32) for _ in range(K)))
    for i in range(K):
        wanted[i:i + 1, :] = jnp.maximum(jnp.max(acc[i], axis=0, keepdims=True) - me * shard_rows, 0)
    listed = pltpu.make_async_copy(wanted, list_ref, list_sem)
    listed.start()
    listed.wait()
    take_rows(cap, nb, lambda k: list_ref[lax.shift_right_logical(k, 7), lax.bitwise_and(k, L - 1)], table_ref, out_ref, buf, scr, sem)


def take_rows(cap, nb, row_of, table_ref, out_ref, buf, scr, sem):
    T = table_ref.shape[1] // 128
    U = 8

    def copy(k):
        base = pl.multiple_of(lax.bitwise_and(row_of(k), -8), 8)
        s = lax.bitwise_and(k, nb - 1)
        return pltpu.make_async_copy(table_ref.at[pl.ds(base, 8)], buf.at[s], sem.at[s])

    @pl.loop(0, nb)
    def _(k):
        copy(k).start()

    def group(q, more):
        for u in range(U):
            k = q * U + u
            s = lax.bitwise_and(k, nb - 1)
            copy(k).wait()
            for j in range(T):
                scr[u, j * 8:(j + 1) * 8, :] = buf[s, :, j * 128:(j + 1) * 128].astype(jnp.float32)
            r = lax.bitwise_and(row_of(k), 7)
            out_ref[k] = scr[u, pl.ds(r, T, stride=8), :].astype(jnp.bfloat16)
        if more:
            for u in range(U):
                copy(q * U + u + nb).start()

    pl.loop(0, (cap - nb) // U)(lambda q: group(q, True))
    pl.loop((cap - nb) // U, cap // U)(lambda q: group(q, False))


def pick(n, shard_rows, cap, soon, early, ids, table, nb=32):
    R, L = ids.size // 128, 128
    K = -(-cap // L)
    T = table.shape[1] // 128
    V = pl.BlockSpec(memory_space=pltpu.VMEM)
    i32 = lambda *shape: jax.ShapeDtypeStruct(shape, jnp.int32)
    vm = lambda *shape: pltpu.VMEM(shape, jnp.int32)
    return pl.pallas_call(
        functools.partial(pick_kernel, n, shard_rows, cap, soon, early, nb),
        out_shape=(i32(R, L), i32(R, L), i32(2, L), jax.ShapeDtypeStruct((cap, T, 128), table.dtype)),
        in_specs=[V, pl.BlockSpec(memory_space=pl.ANY)],
        out_specs=(V, V, V, V),
        scratch_shapes=[vm(R, L), vm(R * L, L), vm(R * L, L), vm(R, L), vm(K, L), pltpu.SMEM((K, L), jnp.int32),
                        pltpu.VMEM((nb, 8, T * 128), table.dtype), pltpu.VMEM((8, T * 8, 128), jnp.float32), pltpu.SemaphoreType.DMA, pltpu.SemaphoreType.DMA((nb,))],
        compiler_params=pltpu.CompilerParams(vmem_limit_bytes=VMEM),
        cost_estimate=pl.CostEstimate(flops=2 * 10**10, bytes_accessed=cap * 8 * T * 256, transcendentals=0),
        name="pick",
    )(ids, table)


def rows_kernel(cap, nb, list_ref, table_ref, out_ref, buf, scr, sem):
    take_rows(cap, nb, lambda k: list_ref[k], table_ref, out_ref, buf, scr, sem)


def rows(cap, lst, table, nb=32):
    T = table.shape[1] // 128
    return pl.pallas_call(
        functools.partial(rows_kernel, cap, nb),
        out_shape=jax.ShapeDtypeStruct((cap, T, 128), table.dtype),
        grid_spec=pltpu.PrefetchScalarGridSpec(
            num_scalar_prefetch=1, grid=(),
            in_specs=[pl.BlockSpec(memory_space=pl.ANY)],
            out_specs=pl.BlockSpec(memory_space=pltpu.VMEM),
            scratch_shapes=[pltpu.VMEM((nb, 8, table.shape[1]), table.dtype), pltpu.VMEM((8, T * 8, 128), jnp.float32), pltpu.SemaphoreType.DMA((nb,))]),
        name="rows",
    )(lst, table)


EPS = 1e-5
TOKENS = 256


class Norm:
    def __init__(self, me, core, at, pos_hbm, gain_ref, bias_ref, h_ref, emb_ref, pos, xs, out, pos_sem, out_sem):
        self.me, self.core, self.at = me, core, at
        self.pos_hbm, self.gain_ref, self.bias_ref, self.h_ref, self.emb_ref = pos_hbm, gain_ref, bias_ref, h_ref, emb_ref
        self.pos, self.xs, self.out, self.pos_sem, self.out_sem = pos, xs, out, pos_sem, out_sem
        self.T = xs.shape[1] // 8
        self.blocks = h_ref.shape[0] // TOKENS

    def load(self, i):
        block = jnp.where(i < self.blocks, i, self.me)
        s = lax.rem(i, 2)
        return pltpu.make_async_copy(self.pos_hbm.at[pl.ds(pl.multiple_of(block * TOKENS, TOKENS), TOKENS)], self.pos.at[s], self.pos_sem.at[s])

    def store(self, i):
        s = lax.rem(i, 2)
        return pltpu.make_async_copy(self.out.at[s], self.h_ref.at[pl.ds(pl.multiple_of(i * TOKENS, TOKENS), TOKENS)], self.out_sem.at[s])

    def store_own(self, b):
        return pltpu.make_async_copy(self.out.at[b], self.emb_ref.at[b], self.out_sem.at[b])

    def tile(self, slot, j):
        return self.xs[slot, j * 8:(j + 1) * 8, :]

    def fetch(self, slot, seq, t, row_of):
        first = (lax.shift_right_logical(t, 7) * 2 + seq) * 128 + lax.bitwise_and(t, 127)
        for r in range(8):
            self.xs[slot, pl.ds(r, self.T, stride=8), :] = row_of(self.at[first + r]).astype(jnp.float32)

    def lanes(self, j):
        return slice(j * 128, (j + 1) * 128)

    def norm(self, i, g, lane_slot, row_of):
        T, xs = self.T, self.xs
        inv = 1.0 / (T * 128)
        t = pl.multiple_of(g * 16, 16)
        out = []
        for half in range(2):
            slot = lane_slot * 2 + half
            self.fetch(slot, self.core, i * TOKENS + g * 16 + half * 8, row_of)
            p = self.pos.at[lax.rem(i, 2), pl.ds(t, 16), :]
            s = None
            for j in range(T):
                e = (self.tile(slot, j) + p[half * 8:half * 8 + 8, self.lanes(j)].astype(jnp.float32)).astype(jnp.bfloat16).astype(jnp.float32)
                xs[slot, j * 8:(j + 1) * 8, :] = e
                s = e if s is None else s + e
            mean = jnp.broadcast_to(jnp.sum(s, axis=1, keepdims=True) * inv, (8, 128))
            s = None
            for j in range(T):
                c = self.tile(slot, j) - mean
                s = c * c if s is None else s + c * c
            var = jnp.sum(s, axis=1, keepdims=True) * inv
            out.append((slot, mean, jnp.broadcast_to(lax.rsqrt(var + EPS), (8, 128))))
        for j in range(T):
            y = [(self.tile(slot, j) - mean) * rs * self.gain_ref[:, self.lanes(j)] + self.bias_ref[:, self.lanes(j)] for slot, mean, rs in out]
            self.out[lax.rem(i, 2), pl.ds(t, 16), self.lanes(j)] = jnp.concatenate(y, axis=0).astype(jnp.bfloat16)

    def embed(self, b, g, lane_slot, row_of):
        t = pl.multiple_of(g * 16, 16)
        for half in range(2):
            self.fetch(lane_slot * 2 + half, b, self.me * TOKENS + t + half * 8, row_of)
        p = self.pos.at[self.blocks % 2, pl.ds(t, 16), :]
        for j in range(self.T):
            e = jnp.concatenate([self.tile(lane_slot * 2, j), self.tile(lane_slot * 2 + 1, j)], axis=0) + p[:, self.lanes(j)].astype(jnp.float32)
            self.out[b, pl.ds(t, 16), self.lanes(j)] = e.astype(jnp.bfloat16)

    def run(self, low, high, row_of):
        @pl.loop(low, high)
        def _(i):
            self.load(i).wait()
            self.load(i + 1).start()

            @pl.when(i >= 2)
            def _():
                self.store(i - 2).wait()

            @pl.loop(0, TOKENS // 64)
            def _(g):
                for j in range(4):
                    self.norm(i, g * 4 + j, j, row_of)
            self.store(i).start()

    def close(self, row_of):
        self.load(self.blocks).wait()
        for b in range(2):
            self.store(self.blocks - 2 + b).wait()

            @pl.loop(0, TOKENS // 64)
            def _(g):
                for j in range(4):
                    self.embed(b, g * 4 + j, j, row_of)
            self.store_own(b).start()
        for b in range(2):
            self.store_own(b).wait()

    @staticmethod
    def scratch(D):
        return [pltpu.VMEM((2, TOKENS, D), jnp.bfloat16), pltpu.VMEM((8, D // 128 * 8, 128), jnp.float32), pltpu.VMEM((2, TOKENS, D), jnp.bfloat16),
                pltpu.SemaphoreType.DMA((2,)), pltpu.SemaphoreType.DMA((2,))]


def broadcast_kernel(n, soon, early, at, rows_ref, pos_hbm, gain_ref, bias_ref, v_ref, w_ref, b_ref,
                     h_ref, emb_ref, minus_ref, plus_ref, w_par_ref, b_par_ref, ua, ub, *rest):
    send_sem, recv_sem, pass_send, pass_recv = rest[-4:]
    q = Peers(n)
    me = q.me
    work = Norm(me, q.core, at, pos_hbm, gain_ref, bias_ref, h_ref, emb_ref, *rest[:-4])
    cap = rows_ref.shape[0]
    late = cap - soon
    spans = ((ua, soon, 0, soon // 2), (ua, soon, soon // 2, soon // 2), (ub, late, 0, late))

    def own(p):
        ref, _, low, size = spans[p]
        return rows_ref.at[pl.ds(low + (soon if ref is ub else 0), size)]

    def place(d, p):
        ref, per, low, size = spans[p]
        return ref.at[pl.ds(d * per + low, size)]

    moves = Spread(q, own, place, send_sem, recv_sem)
    last_rows = v_ref.at[pl.ds(v_ref.shape[0] - minus_ref.shape[0], minus_ref.shape[0])]
    passed = [pltpu.make_async_remote_copy(src_ref=src, dst_ref=dst, send_sem=pass_send.at[i], recv_sem=pass_recv.at[i], device_id={"tp": to}, device_id_type=MESH)
              for i, (src, dst, to) in enumerate(((last_rows, minus_ref, q.plus), (last_rows, plus_ref, q.minus), (w_ref, w_par_ref, q.partner), (b_ref, b_par_ref, q.partner)))]
    work.load(0).start()
    q.greet((q.plus, q.minus, q.partner))
    moves.begin(0)
    moves.begin(1)
    for ref, low, size in ((ua, 0, soon), (ub, soon, late)):
        @pl.loop(0, size // 8)
        def _(k):
            for r in range(8):
                ref[me * size + k * 8 + r] = rows_ref[low + k * 8 + r]
    for c in passed[2:]:
        c.start()
    moves.turn(0)
    moves.turn(1)
    moves.begin(2)
    for p in range(2):
        moves.last(p)
    for p in range(2):
        moves.finish(p)

    def first(i):
        return ua[i]

    def any_(i):
        here = i < n * soon
        a, b = ua[jnp.minimum(i, n * soon - 1)], ub[jnp.maximum(i - n * soon, 0)]
        return jnp.where(here, a.astype(jnp.float32), b.astype(jnp.float32))

    blocks = early // TOKENS
    work.run(0, blocks - 2, first)
    moves.turn(2)
    for c in passed[:2]:
        c.start()
    work.run(blocks - 2, blocks, first)
    moves.last(2)
    moves.finish(2)
    work.run(blocks, work.blocks, any_)
    work.close(any_)
    for c in passed:
        c.wait()


def broadcast(n, soon, early, at, rows, pos, gain, bias, v, last, w, b, cid=3):
    seq, D = pos.shape
    cap, T, L = rows.shape
    A = pl.BlockSpec(memory_space=pl.ANY)
    V = pl.BlockSpec(memory_space=pltpu.VMEM)
    sems = pltpu.SemaphoreType.DMA((Spread.CHANNELS, 3))
    of = lambda r: jax.ShapeDtypeStruct((r, D), v.dtype)
    return pl.pallas_call(
        functools.partial(broadcast_kernel, n, soon, early),
        out_shape=(jax.ShapeDtypeStruct((seq, D), jnp.bfloat16), jax.ShapeDtypeStruct((2, seq // n, D), jnp.bfloat16),
                   of(last), of(last), jax.ShapeDtypeStruct(w.shape, w.dtype), jax.ShapeDtypeStruct(b.shape, b.dtype)),
        grid_spec=pltpu.PrefetchScalarGridSpec(
            num_scalar_prefetch=1, grid=(), in_specs=[V, A, V, V, A, A, V], out_specs=(A, A, A, A, A, V),
            scratch_shapes=[pltpu.VMEM((n * soon, T, L), rows.dtype), pltpu.VMEM((n * (cap - soon), T, L), rows.dtype), *Norm.scratch(D), sems, sems, *[pltpu.SemaphoreType.DMA((4,))] * 2]),
        compiler_params=pltpu.CompilerParams(vmem_limit_bytes=VMEM, collective_id=cid, has_side_effects=True),
        name="broadcast",
    )(at, rows, pos, gain, bias, v, w, b)


def norm_kernel(at, x_hbm, pos_hbm, gain_ref, bias_ref, h_ref, emb_ref, x, sem, *rest):
    me = lax.axis_index("tp")
    work = Norm(me, lax.rem(me, 2), at, pos_hbm, gain_ref, bias_ref, h_ref, emb_ref, *rest)
    work.load(0).start()
    c = pltpu.make_async_copy(x_hbm, x, sem)
    c.start()
    c.wait()
    work.run(0, work.blocks, lambda i: x[i])
    work.close(lambda i: x[i])


def norm(n, at, x, pos, gain, bias):
    seq, D = pos.shape
    A = pl.BlockSpec(memory_space=pl.ANY)
    V = pl.BlockSpec(memory_space=pltpu.VMEM)
    return pl.pallas_call(
        norm_kernel,
        out_shape=(jax.ShapeDtypeStruct((seq, D), jnp.bfloat16), jax.ShapeDtypeStruct((2, seq // n, D), jnp.bfloat16)),
        grid_spec=pltpu.PrefetchScalarGridSpec(
            num_scalar_prefetch=1, grid=(), in_specs=[A, A, V, V], out_specs=(A, A),
            scratch_shapes=[pltpu.VMEM(x.shape, x.dtype), pltpu.SemaphoreType.DMA, *Norm.scratch(D)]),
        compiler_params=pltpu.CompilerParams(vmem_limit_bytes=VMEM),
        name="norm",
    )(at, x, pos, gain, bias)


def project_kernel(chunk, wa_hbm, wb_hbm, ba_ref, bb_ref, emb_hbm, h_ref, qkv_ref, emb_out, w, bc, emb, wsem, esem):
    step = pl.program_id(0)
    core = lax.rem(lax.axis_index("tp"), 2)
    M = wa_hbm.shape[0]
    tb = h_ref.shape[0]

    def load(k):
        return pltpu.make_async_copy((wa_hbm, wb_hbm)[k], w.at[lax.rem(core + k, 2)], wsem.at[lax.rem(core + k, 2)])

    def loaded(k):
        return pltpu.make_async_copy(wa_hbm, w.at[k], wsem.at[k])

    @pl.when(step == 0)
    def _():
        for k in range(2):
            load(k).start()
        pltpu.make_async_copy(emb_hbm, emb, esem).start()
        _, H, E = ba_ref.shape
        for k, b in enumerate((ba_ref, bb_ref)):
            for r in range(3 * H):
                bc[lax.rem(core + k, 2), r * E:(r + 1) * E, :] = jnp.broadcast_to(b[r // H, r % H:r % H + 1, :], (128, E)).T

    @pl.when(step == 1)
    def _():
        pltpu.make_async_copy(emb_hbm, emb, esem).wait()
        pltpu.make_async_copy(emb, emb_out, esem).start()

    @pl.when(step == pl.num_programs(0) - 1)
    def _():
        pltpu.make_async_copy(emb, emb_out, esem).wait()

    for k in range(2):
        @pl.when(step == 0)
        def _():
            loaded(k).wait()
        for m in range(0, M, chunk):
            o = lax.dot_general(w[k, m:m + chunk, :], h_ref[...], (((1,), (1,)), ((), ())), preferred_element_type=jnp.float32)
            b = jnp.concatenate([bc[k, m:m + chunk, :]] * (tb // 128), axis=1)
            qkv_ref[k, m:m + chunk, :] = (o + b).astype(jnp.bfloat16)


def project(h, emb, wa, wb, ba, bb, tb=512, chunk=384):
    seq, D = h.shape
    M = wa.shape[0]
    A = pl.BlockSpec(memory_space=pl.ANY)
    one = lambda shape: pl.BlockSpec(shape, lambda i: (0,) * len(shape), pipeline_mode=pl.Buffered(1))
    return pl.pallas_call(
        functools.partial(project_kernel, chunk),
        out_shape=(jax.ShapeDtypeStruct((2, M, seq), jnp.bfloat16), jax.ShapeDtypeStruct(emb.shape, emb.dtype)),
        grid=(seq // tb,),
        in_specs=[A, A, one(ba.shape), one(bb.shape), A, pl.BlockSpec((tb, D), lambda i: (i, 0))],
        out_specs=(pl.BlockSpec((2, M, tb), lambda i: (0, 0, i)), A),
        scratch_shapes=[pltpu.VMEM((2, M, D), wa.dtype), pltpu.VMEM((2, M, 128), jnp.float32), pltpu.VMEM(emb.shape, emb.dtype), pltpu.SemaphoreType.DMA((2,)), pltpu.SemaphoreType.DMA],
        compiler_params=pltpu.CompilerParams(vmem_limit_bytes=VMEM),
        cost_estimate=pl.CostEstimate(flops=4 * seq * M * D, bytes_accessed=50 * 2**20, transcendentals=0),
        name="project",
    )(wa, wb, ba, bb, emb, h)


def attend_kernel(n, scale, qb, nb, early, where, qkv_ref, emb_hbm, bias_ref, *refs):
    pieces, (out_ref, kk, vv, sc, ctx, got, w, a, acc, emb, load_sem, pass_send, pass_recv, emb_sem, send_sem, recv_sem) = refs[:len(where)], refs[len(where):]
    E, S = qkv_ref.shape[3:]
    heads = got.shape[1] // E
    N = S // qb
    c = scale * 1.4426950408889634
    q = Peers(n)
    me, core = q.me, q.core
    head = pl.program_id(0)
    cut = early * E // 256 * 256
    owners = {0: me, 1: q.plus, 2: q.opp, -1: q.minus}

    def loads():
        cs = []
        for i, (ref, (away, low)) in enumerate(zip(pieces, where)):
            dst = w.at[owners[away], pl.ds(low, ref.shape[0])]
            cs.append(pltpu.make_async_copy(ref, dst, load_sem.at[i]))
            cs.append(pltpu.make_async_remote_copy(src_ref=ref, dst_ref=dst, send_sem=pass_send.at[i], recv_sem=pass_recv.at[i], device_id={"tp": q.partner}, device_id_type=MESH))
        return cs

    def send(h, s):
        to = lax.rem(me + s, n)
        return pltpu.make_async_remote_copy(src_ref=ctx.at[h, to], dst_ref=got.at[me, pl.ds(pl.multiple_of(h * E, 32), E)],
                                            send_sem=send_sem.at[s], recv_sem=recv_sem.at[lax.div(h, early), s], device_id={"tp": to}, device_id_type=MESH)

    load_emb = pltpu.make_async_copy(emb_hbm, emb, emb_sem)

    @pl.when(head == 0)
    def _():
        q.greet([lax.rem(me + s, n) for s in range(1, n)])
        vv[E:, :] = jnp.where(lax.broadcasted_iota(jnp.int32, (vv.shape[0] - E, S), 0) == 0, 1.0, 0.0).astype(jnp.bfloat16)

    @pl.when(head > 0)
    def _():
        for s in range(1, n):
            send(head - 1, s).start()

    @pl.when(head == 1)
    def _():
        for c_ in loads():
            c_.start()
        load_emb.start()

    for t in range(0, S, 128):
        kk[t:t + 128, :] = qkv_ref[0, 1, 0, :, t:t + 128].astype(jnp.float32).T.astype(jnp.bfloat16)
    vv[0:E, :] = qkv_ref[0, 2, 0]
    keep = lax.broadcasted_iota(jnp.int32, (qb, qb), 0) <= lax.broadcasted_iota(jnp.int32, (qb, qb), 1)

    def scores(i, k, m):
        s = jnp.dot(kk[k * qb:(k + 1) * qb, :], qkv_ref[0, 0, 0, :, i * qb:(i + 1) * qb], preferred_element_type=jnp.float32)
        if k == i:
            s = jnp.where(keep, s, -jnp.inf)
        sc[i % 2, k * qb:(k + 1) * qb, :] = s
        top = jnp.max(s.reshape(qb // 8, 8, qb), axis=0)
        return top if m is None else jnp.maximum(m, top)

    def weigh(i, k, mc, o):
        s = sc[i % 2, k * qb:(k + 1) * qb, :]
        p = jnp.exp2(s * c - mc).astype(jnp.bfloat16)
        d = jnp.dot(vv[:, k * qb:(k + 1) * qb], p, preferred_element_type=jnp.float32)
        return d if o is None else o + d

    m = scores(0, 0, None)
    for i in range(N):
        mc = jnp.max(m, axis=0, keepdims=True) * c
        o = m = None
        for k in range(i + 2):
            if i + 1 < N:
                m = scores(i + 1, k, m)
            if k <= i:
                o = weigh(i, k, mc, o)
        ctx[head, i] = (o[0:E] * (1.0 / o[E:E + 1])).astype(jnp.bfloat16)
    got[me, pl.ds(pl.multiple_of(head * E, 32), E), :] = ctx[head, me]

    @pl.when(head == heads - 1)
    def _():
        for s in range(1, n):
            send(head, s).start()
        K = got.shape[1]

        def arrive(group, low, high):
            for s in range(1, n):
                fr = lax.rem(me - s + n, n)
                r = got.at[fr, pl.ds(low, high - low)]
                pltpu.make_async_remote_copy(src_ref=r, dst_ref=r, send_sem=send_sem.at[s], recv_sem=recv_sem.at[group, s], device_id={"tp": fr}, device_id_type=MESH).wait_recv()

        def turn_over(low, high):
            for s in range(n):
                for k in range(low, high, 128):
                    for t in range(0, qb, 128):
                        at = s // 2 * (high - low) + (k - low) + (n // 2) * low
                        a[(s % 2) * qb + t:(s % 2) * qb + t + 128, at:at + 128] = got[s, k:k + 128, t:t + 128].astype(jnp.float32).T.astype(jnp.bfloat16)

        def part(low, high, cols):
            rows = [w[2 * i:2 * i + 2, :, cols].reshape(K, nb)[low:high] for i in range(n // 2)]
            return jnp.dot(a[:, n // 2 * low:n // 2 * high], jnp.concatenate(rows, axis=0), preferred_element_type=jnp.float32)

        arrive(0, 0, early * E)
        turn_over(0, cut)
        for c_ in loads():
            c_.wait()
        load_emb.wait()

        @pl.loop(0, w.shape[2] // nb)
        def _(j):
            cols = pl.ds(pl.multiple_of(j * nb, nb), nb)
            acc[:, cols] = part(0, cut, cols) + bias_ref[:, cols]

        arrive(1, early * E, K)
        turn_over(cut, K)

        @pl.loop(0, w.shape[2] // nb)
        def _(j):
            cols = pl.ds(pl.multiple_of(j * nb, nb), nb)
            o = part(cut, K, cols) + acc[:, cols]
            for b in range(2):
                out_ref[b, :, cols] = (emb[b, :, cols].astype(jnp.float32) + o[b * qb:(b + 1) * qb]).astype(jnp.bfloat16)

        for s in range(1, n):
            r = got.at[lax.rem(me - s + n, n)]
            pltpu.make_async_remote_copy(src_ref=r, dst_ref=r, send_sem=send_sem.at[s], recv_sem=recv_sem.at[0, s], device_id={"tp": q.partner}, device_id_type=MESH).wait_send()


def attend(n, qkv, pieces, where, emb, bias, early=6, nb=1024, cid=1, qb=256):
    heads, E, S = 2 * qkv.shape[2], *qkv.shape[3:]
    H = heads // 2
    D = emb.shape[2]
    A = pl.BlockSpec(memory_space=pl.ANY)
    one = lambda shape: pl.BlockSpec(shape, lambda h: (0,) * len(shape), pipeline_mode=pl.Buffered(1))
    bf = jnp.bfloat16
    return pl.pallas_call(
        functools.partial(attend_kernel, n, E ** -0.5, qb, nb, early, where),
        out_shape=jax.ShapeDtypeStruct(emb.shape, bf),
        grid=(heads,),
        in_specs=[pl.BlockSpec((1, 3, 1, E, S), lambda h: (h // H, 0, h % H, 0, 0)), A, one(bias.shape)] + [A] * len(pieces),
        out_specs=one(emb.shape),
        scratch_shapes=[pltpu.VMEM((S, E), bf), pltpu.VMEM((E + 16, S), bf), pltpu.VMEM((2, S, qb), jnp.float32),
                        pltpu.VMEM((heads, n, E, qb), bf), pltpu.VMEM((n, heads * E, qb), bf), pltpu.VMEM((n, H * E, D), bf), pltpu.VMEM((2 * qb, n * H * E), bf),
                        pltpu.VMEM((2 * qb, D), jnp.float32), pltpu.VMEM(emb.shape, bf),
                        *[pltpu.SemaphoreType.DMA((len(pieces),))] * 3, pltpu.SemaphoreType.DMA, pltpu.SemaphoreType.DMA((n,)), pltpu.SemaphoreType.DMA((2, n))],
        compiler_params=pltpu.CompilerParams(collective_id=cid, has_side_effects=True, vmem_limit_bytes=VMEM),
        name="attend",
    )(qkv, emb, bias, *pieces)


CAP = 264
SOON, EARLY = 200, 1280


def place_kernel(code_ref, u_ref, x_ref, out_ref, sem):
    @pl.loop(0, code_ref.shape[0])
    def _(t):
        c = code_ref[t]

        @pl.when(c >= 0)
        def _():
            copy = pltpu.make_async_copy(u_ref.at[c], out_ref.at[t], sem)
            copy.start()
            copy.wait()


def place(at, u, x):
    A = pl.BlockSpec(memory_space=pl.ANY)
    return pl.pallas_call(
        place_kernel,
        out_shape=jax.ShapeDtypeStruct(x.shape, x.dtype),
        grid_spec=pltpu.PrefetchScalarGridSpec(num_scalar_prefetch=1, grid=(), in_specs=[A, A], out_specs=A, scratch_shapes=[pltpu.SemaphoreType.DMA]),
        input_output_aliases={2: 0},
        name="place",
    )(at, u, x)


def solution(mesh):
    n = mesh.shape["tp"]
    def local_step(token_ids, word_shard, pos_table, ln_gain, ln_bias, w_qkv, b_qkv, w_out, b_out):
        me = lax.axis_index("tp")
        core = lax.rem(me, 2)
        seq, D = pos_table.shape
        H, E = w_qkv.shape[2:]
        shard_rows = word_shard.shape[0]
        w_own = jnp.transpose(w_qkv, (1, 2, 3, 0)).reshape(3 * H * E, D)
        v_own = w_out.reshape(H * E, D)
        ring = lambda step: [(d, (d + 2 * step) % n) for d in range(n)]
        send = lambda x, step: lax.ppermute(x, "tp", ring(step))
        v_head = w_out[:2].reshape(2 * E, D)
        minus0, plus0 = send(v_head, 1), send(v_head, -1)
        blk = seq // n
        gain, bias = ln_gain[None], ln_bias[None]
        code, at, counts, mine = pick(n, shard_rows, CAP, SOON, EARLY, token_ids, word_shard)
        h, embed, minus1, plus1, w_par, b_par = broadcast(n, SOON, EARLY, at.reshape(-1), mine, pos_table, gain, bias, v_own, (H - 2) * E, w_own, b_qkv)
        counts, h = lax.optimization_barrier((counts, h))

        rounds = jnp.where((counts[0, 0] > CAP) | (counts[1, 0] > SOON), (counts[0, 0] + CAP - 1) // CAP, 0)
        total = max(n * CAP, seq + blk)

        def by_token(x):
            return x.reshape(seq // 128, 2, 128).transpose(1, 0, 2)

        def wanted(x):
            own = lax.dynamic_index_in_dim(x, core, 0, keepdims=False)
            other = lax.dynamic_index_in_dim(x, 1 - core, 0, keepdims=False)
            return jnp.concatenate([own, lax.dynamic_slice_in_dim(other, me * blk, blk)])

        def more(carry):
            def one_round(carry):
                r, x = carry
                codes = by_token(code).reshape(2, seq)
                slot = codes % SPAN - r * CAP
                hit = (slot >= 0) & (slot < CAP)
                here = jnp.where(hit & (codes // SPAN == me), slot, -1).reshape(-1)
                ids = token_ids.reshape(-1) - me * shard_rows
                chosen = jnp.max(jnp.where(here[None, :] == jnp.arange(CAP)[:, None], ids[None, :], 0), axis=1)
                v = gather_all(n, rows(CAP, chosen, word_shard), total)
                return r + 1, place(wanted(jnp.where(hit, codes // SPAN * CAP + slot, -1)), v, x)

            x = jnp.zeros((total,) + mine.shape[1:], mine.dtype)
            _, x = lax.while_loop(lambda c: c[0] < rounds, one_round, (jnp.int32(0), x))
            t = jnp.arange(seq, dtype=jnp.int32)
            t = jnp.stack([jnp.where(core == b, t, jnp.clip(t - me * blk, 0, blk - 1) + seq) for b in range(2)])
            t = t.reshape(2, seq // 128, 128).transpose(1, 0, 2).reshape(-1)
            return (jnp.int32(0),) + tuple(norm(n, t, x, pos_table, gain, bias))

        _, h, embed = lax.while_loop(lambda c: c[0] > 0, more, (rounds, h, embed))

        minus0, h = lax.optimization_barrier((minus0, h))
        opp0, opp1 = send(minus0, 1), send(plus1, -1)
        pieces = [v_own, minus0, plus0, minus1, plus1, opp0, opp1]
        where = ((0, 0), (-1, 0), (1, 0), (-1, 2 * E), (1, 2 * E), (2, 0), (2, 2 * E))
        qkv, embed = project(h, embed, w_own, w_par, b_qkv, b_par)
        resid_out = attend(n, qkv.reshape(2, 3, H, E, seq), pieces, where, embed, b_out[None])
        return resid_out, embed

    in_specs = (P("dp", None), P("tp", None), P(None, None), P(None), P(None), P(None, None, "tp", None), P(None, "tp", None), P("tp", None, None), P(None))
    out_specs = (P("dp", "tp", None), P("dp", "tp", None))
    return jax.shard_map(local_step, mesh=mesh, in_specs=in_specs, out_specs=out_specs, check_vma=False)
```

```python
import functools

import jax
import jax.numpy as jnp
from jax import lax
from jax.experimental import pallas as pl
from jax.experimental.pallas import tpu as pltpu
from jax.sharding import PartitionSpec as P

MESH = pl.DeviceIdType.MESH
VMEM = 63 * 2**20


class Peers:
    def __init__(self, n):
        self.n = n
        self.me = lax.axis_index("tp")
        self.chip, self.core = lax.div(self.me, 2), lax.rem(self.me, 2)
        self.plus, self.minus, self.opp = self.near(1), self.near(-1), self.near(2)
        self.partner = self.other(self.me)

    def near(self, s):
        chips = self.n // 2
        return lax.rem(self.chip + s + chips, chips) * 2 + self.core

    def other(self, d):
        return d + 1 - 2 * self.core

    def greet(self, devices):
        barrier = pltpu.get_barrier_semaphore()
        for d in devices:
            pl.semaphore_signal(barrier, inc=1, device_id={"tp": d}, device_id_type=MESH)
        pl.semaphore_wait(barrier, len(devices))


class Spread:
    CHANNELS = 9

    def __init__(self, peers, own, place, send_sem, recv_sem):
        self.q, self.own, self.place, self.send_sem, self.recv_sem = peers, own, place, send_sem, recv_sem

    def half(self, ref, i):
        rows = ref.shape[0] // 2
        return ref.at[pl.ds(i * rows, rows)]

    def copy(self, channel, p, src, dst, to):
        return pltpu.make_async_remote_copy(src_ref=src, dst_ref=dst, send_sem=self.send_sem.at[channel, p], recv_sem=self.recv_sem.at[channel, p],
                                            device_id={"tp": to}, device_id_type=MESH)

    def got(self, channel, p, ref):
        self.copy(channel, p, ref, ref, self.q.partner).wait_recv()

    def begin(self, p):
        q = self.q
        for channel, to in ((0, q.plus), (1, q.minus), (4, q.partner)):
            self.copy(channel, p, self.own(p), self.place(q.me, p), to).start()

    def turn(self, p):
        q = self.q
        for i, (d, to) in enumerate(((q.minus, q.plus), (q.plus, q.minus))):
            ref = self.place(d, p)
            self.got(i, p, ref)
            self.copy(2 + i, p, self.half(ref, i), self.half(ref, i), to).start()
            self.copy(5 + i, p, ref, ref, q.partner).start()

    def last(self, p):
        q = self.q
        for i in range(2):
            c = self.half(self.place(q.opp, p), i)
            self.got(2 + i, p, c)
            self.copy(7 + i, p, c, c, q.partner).start()

    def finish(self, p):
        q = self.q
        own, a, b, c = (self.place(d, p) for d in (q.partner, q.other(q.minus), q.other(q.plus), q.other(q.opp)))
        for channel, ref in ((4, own), (5, a), (6, b), (7, self.half(c, 0)), (8, self.half(c, 1))):
            self.got(channel, p, ref)
        for channel, ref in ((0, own), (1, own), (4, own), (5, a), (6, b), (2, self.half(c, 0)), (3, self.half(c, 1)), (7, self.half(c, 0)), (8, self.half(c, 1))):
            self.copy(channel, p, ref, ref, q.partner).wait_send()


def gather_all_kernel(n, S, src_ref, all_ref, loc_sem, send_sem, recv_sem):
    cap = src_ref.shape[0]

    def of(d):
        return all_ref.at[pl.ds(d * cap, cap)]
    chips = n // 2
    me = lax.axis_index("tp")
    chip, core = me // 2, lax.rem(me, 2)
    def at(c):
        return lax.rem(c + chips, chips) * 2 + core
    plus, minus, opp = at(chip + 1), at(chip - 1), at(chip + 2)
    partner = me + 1 - 2 * core
    P = 2 * S
    step = src_ref.shape[0] // P

    barrier = pltpu.get_barrier_semaphore()
    for d in (plus, minus, partner):
        pl.semaphore_signal(barrier, inc=1, device_id={"tp": d}, device_id_type=MESH)
    pl.semaphore_wait(barrier, 3)

    started = []
    def rc(src, dst, ch, k, dev):
        return pltpu.make_async_remote_copy(src_ref=src, dst_ref=dst, send_sem=send_sem.at[ch, k], recv_sem=recv_sem.at[ch, k],
                                            device_id={"tp": dev}, device_id_type=MESH)
    def go(src, dst, ch, k, dev):
        c = rc(src, dst, ch, k, dev)
        c.start()
        started.append(c)
    def piece(ref, k):
        return ref.at[pl.ds(k * step, step)]
    first, last = list(range(S)), list(range(S, P))
    for a, b in zip(first, last):
        go(piece(src_ref, a), piece(of(me), a), 0, a, plus)
        go(piece(src_ref, b), piece(of(me), b), 1, b, minus)
    for a, b in zip(first, last):
        go(piece(src_ref, b), piece(of(me), b), 0, b, plus)
        go(piece(src_ref, a), piece(of(me), a), 1, a, minus)
    go(src_ref, of(me), 4, 0, partner)
    loc = pltpu.make_async_copy(src_ref, of(me), loc_sem)
    loc.start()
    def got(owner, ch, k):
        r = piece(of(owner), k)
        rc(r, r, ch, k, partner).wait_recv()
        return r
    for a, b in zip(first, last):
        r = got(minus, 0, a)
        go(r, r, 2, a, plus)
        go(r, r, 5, a, partner)
        r = got(plus, 1, b)
        go(r, r, 3, b, minus)
        go(r, r, 6, b, partner)
    for a, b in zip(first, last):
        r = got(minus, 0, b)
        go(r, r, 5, b, partner)
        r = got(plus, 1, a)
        go(r, r, 6, a, partner)
    for a, b in zip(first, last):
        r = got(opp, 2, a)
        go(r, r, 7, a, partner)
        r = got(opp, 3, b)
        go(r, r, 7, b, partner)
    other = lambda d: d + 1 - 2 * core
    r = of(partner)
    rc(r, r, 4, 0, partner).wait_recv()
    for k in range(P):
        got(other(minus), 5, k)
        got(other(plus), 6, k)
        got(other(opp), 7, k)
    loc.wait()
    for c in started:
        c.wait_send()


def gather_all(n, rows, total, S=2, cid=0):
    return pl.pallas_call(
        functools.partial(gather_all_kernel, n, S),
        out_shape=jax.ShapeDtypeStruct((total,) + rows.shape[1:], rows.dtype),
        in_specs=[pl.BlockSpec(memory_space=pltpu.VMEM)],
        out_specs=pl.BlockSpec(memory_space=pl.ANY),
        scratch_shapes=[pltpu.SemaphoreType.DMA, pltpu.SemaphoreType.DMA((8, 2 * S)), pltpu.SemaphoreType.DMA((8, 2 * S))],
        compiler_params=pltpu.CompilerParams(collective_id=cid, has_side_effects=True),
        name="gather_all",
    )(rows)


SPAN_BITS = 13
SPAN = 1 << SPAN_BITS


def pick_kernel(n, shard_rows, cap, soon, early, nb, ids_ref, table_ref, code_ref, at_ref, cnt_ref, out_ref,
                ids, col, wcol, first, wanted, list_ref, buf, scr, list_sem, sem):
    me = lax.axis_index("tp")
    R, L = ids.shape
    G, Q = 8, 4
    lane = lax.broadcasted_iota(jnp.int32, (8, L), 1)
    sub = lax.broadcasted_iota(jnp.int32, (8, L), 0)
    for r in range(R):
        o, b = divmod(r, ids_ref.shape[0])
        ids[r:r + 1, :] = ids_ref[b:b + 1, o * L:(o + 1) * L]

    def columns(*pairs):
        @pl.loop(0, R // Q)
        def _(g):
            for k in range(Q):
                a = g * Q + k
                for src, dst in pairs:
                    dst[pl.ds(pl.multiple_of(a * L, L), L), :] = jnp.broadcast_to(src[pl.ds(a, 1), :], (L, L)).T

    def against(bg, start, step):
        acc = start
        def body(a, acc):
            acc = list(acc)
            for k in range(L // 8):
                at = pl.ds(pl.multiple_of(a * L + k * 8, 8), 8)
                step(acc, at, k, range(G), -1)
            return tuple(acc)
        acc = list(lax.fori_loop(0, bg * G, body, tuple(acc)))
        for d in range(G):
            for k in range(L // 8):
                step(acc, pl.ds((bg * G + d) * L + k * 8, 8), k, range(d, G), d)
        return acc

    def wide(ref, bg):
        return [jnp.broadcast_to(ref[bg * G + i:bg * G + i + 1, :], (8, L)) for i in range(G)]

    columns((ids, col))
    for bg in range(R // G):
        rows = wide(ids, bg)
        def seen(acc, at, k, which, same):
            c = col[at, :]
            for i in which:
                hit = c == rows[i]
                if i == same:
                    hit = hit & (k * 8 + sub < lane)
                acc[i] = jnp.where(hit, 1, acc[i])
        acc = against(bg, [jnp.zeros((8, L), jnp.int32)] * G, seen)
        for i in range(G):
            first[bg * G + i:bg * G + i + 1, :] = 1 - jnp.max(acc[i], axis=0, keepdims=True)

    x = ids[...]
    owner = jnp.zeros((R, L), jnp.int32)
    for o in range(1, n):
        owner = owner + jnp.where(x >= o * shard_rows, 1, 0)
    isf = first[...] == 1
    one = jnp.concatenate([jnp.where(isf & (owner == o), 1.0, 0.0) for o in range(n)], axis=0).astype(jnp.bfloat16)
    up = (lax.broadcasted_iota(jnp.int32, (L, L), 0) < lax.broadcasted_iota(jnp.int32, (L, L), 1)).astype(jnp.float32).astype(jnp.bfloat16)
    prefix = jnp.dot(one, up, preferred_element_type=jnp.float32)
    tot = jnp.dot(one, jnp.ones((L, L), jnp.bfloat16), preferred_element_type=jnp.float32)
    r = lax.broadcasted_iota(jnp.int32, (n * R, n * R), 0)
    c = lax.broadcasted_iota(jnp.int32, (n * R, n * R), 1)
    low = ((r // R == c // R) & (c < r)).astype(jnp.float32).astype(jnp.bfloat16)
    off = jnp.dot(low, tot.astype(jnp.bfloat16), preferred_element_type=jnp.float32)
    pos = prefix + off
    slot = jnp.zeros((R, L), jnp.float32)
    most = jnp.zeros((1, L), jnp.float32)
    for o in range(n):
        slot = jnp.where(owner == o, pos[o * R:(o + 1) * R], slot)
        most = jnp.maximum(most, (off + tot)[(o + 1) * R - 1:(o + 1) * R])
    cnt_ref[0:1, :] = most.astype(jnp.int32)
    code_ref[...] = jnp.where(isf, owner * SPAN + slot.astype(jnp.int32), -1)
    first[...] = jnp.where(isf, x, -1)
    columns((first, col), (code_ref, wcol))

    for bg in range(R // G):
        rows = wide(ids, bg)
        def take(acc, at, k, which, same):
            c, w = col[at, :], wcol[at, :]
            for i in which:
                acc[i] = jnp.where(c == rows[i], w, acc[i])
        acc = against(bg, [jnp.zeros((8, L), jnp.int32)] * G, take)
        for i in range(G):
            code_ref[bg * G + i:bg * G + i + 1, :] = jnp.max(acc[i], axis=0, keepdims=True)
    code = code_ref[...]
    who, slot = lax.shift_right_logical(code, SPAN_BITS), lax.bitwise_and(code, SPAN - 1)
    at_ref[...] = jnp.where(slot < soon, who * soon + slot, n * soon + who * (cap - soon) + jnp.minimum(slot, cap - 1) - soon)
    seen = jnp.max(slot[0:early // L * ids_ref.shape[0], :], axis=0, keepdims=True)
    cnt_ref[1:2, :] = jnp.broadcast_to(jnp.max(seen, axis=1, keepdims=True) + 1, (1, L))

    K = wanted.shape[0]
    want = [me * SPAN + i * L + lane for i in range(K)]
    def body(a, acc):
        acc = list(acc)
        for k in range(L // 8):
            at = pl.ds(pl.multiple_of(a * L + k * 8, 8), 8)
            c, w = col[at, :], wcol[at, :]
            for i in range(K):
                acc[i] = jnp.where(w == want[i], c, acc[i])
        return tuple(acc)
    acc = lax.fori_loop(0, R, body, tuple(jnp.zeros((8, L), jnp.int32) for _ in range(K)))
    for i in range(K):
        wanted[i:i + 1, :] = jnp.maximum(jnp.max(acc[i], axis=0, keepdims=True) - me * shard_rows, 0)
    listed = pltpu.make_async_copy(wanted, list_ref, list_sem)
    listed.start()
    listed.wait()
    take_rows(cap, nb, lambda k: list_ref[lax.shift_right_logical(k, 7), lax.bitwise_and(k, L - 1)], table_ref, out_ref, buf, scr, sem)


def take_rows(cap, nb, row_of, table_ref, out_ref, buf, scr, sem):
    T = table_ref.shape[1] // 128
    U = 8

    def copy(k):
        base = pl.multiple_of(lax.bitwise_and(row_of(k), -8), 8)
        s = lax.bitwise_and(k, nb - 1)
        return pltpu.make_async_copy(table_ref.at[pl.ds(base, 8)], buf.at[s], sem.at[s])

    @pl.loop(0, nb)
    def _(k):
        copy(k).start()

    def group(q, more):
        for u in range(U):
            k = q * U + u
            s = lax.bitwise_and(k, nb - 1)
            copy(k).wait()
            for j in range(T):
                scr[u, j * 8:(j + 1) * 8, :] = buf[s, :, j * 128:(j + 1) * 128].astype(jnp.float32)
            r = lax.bitwise_and(row_of(k), 7)
            out_ref[k] = scr[u, pl.ds(r, T, stride=8), :].astype(jnp.bfloat16)
        if more:
            for u in range(U):
                copy(q * U + u + nb).start()

    pl.loop(0, (cap - nb) // U)(lambda q: group(q, True))
    pl.loop((cap - nb) // U, cap // U)(lambda q: group(q, False))


def pick(n, shard_rows, cap, soon, early, ids, table, nb=32):
    R, L = ids.size // 128, 128
    K = -(-cap // L)
    T = table.shape[1] // 128
    V = pl.BlockSpec(memory_space=pltpu.VMEM)
    i32 = lambda *shape: jax.ShapeDtypeStruct(shape, jnp.int32)
    vm = lambda *shape: pltpu.VMEM(shape, jnp.int32)
    return pl.pallas_call(
        functools.partial(pick_kernel, n, shard_rows, cap, soon, early, nb),
        out_shape=(i32(R, L), i32(R, L), i32(2, L), jax.ShapeDtypeStruct((cap, T, 128), table.dtype)),
        in_specs=[V, pl.BlockSpec(memory_space=pl.ANY)],
        out_specs=(V, V, V, V),
        scratch_shapes=[vm(R, L), vm(R * L, L), vm(R * L, L), vm(R, L), vm(K, L), pltpu.SMEM((K, L), jnp.int32),
                        pltpu.VMEM((nb, 8, T * 128), table.dtype), pltpu.VMEM((8, T * 8, 128), jnp.float32), pltpu.SemaphoreType.DMA, pltpu.SemaphoreType.DMA((nb,))],
        compiler_params=pltpu.CompilerParams(vmem_limit_bytes=VMEM),
        cost_estimate=pl.CostEstimate(flops=2 * 10**10, bytes_accessed=cap * 8 * T * 256, transcendentals=0),
        name="pick",
    )(ids, table)


def rows_kernel(cap, nb, list_ref, table_ref, out_ref, buf, scr, sem):
    take_rows(cap, nb, lambda k: list_ref[k], table_ref, out_ref, buf, scr, sem)


def rows(cap, lst, table, nb=32):
    T = table.shape[1] // 128
    return pl.pallas_call(
        functools.partial(rows_kernel, cap, nb),
        out_shape=jax.ShapeDtypeStruct((cap, T, 128), table.dtype),
        grid_spec=pltpu.PrefetchScalarGridSpec(
            num_scalar_prefetch=1, grid=(),
            in_specs=[pl.BlockSpec(memory_space=pl.ANY)],
            out_specs=pl.BlockSpec(memory_space=pltpu.VMEM),
            scratch_shapes=[pltpu.VMEM((nb, 8, table.shape[1]), table.dtype), pltpu.VMEM((8, T * 8, 128), jnp.float32), pltpu.SemaphoreType.DMA((nb,))]),
        name="rows",
    )(lst, table)


EPS = 1e-5
TOKENS = 256


class Norm:
    def __init__(self, me, core, at, pos_hbm, gain_ref, bias_ref, h_ref, emb_ref, pos, xs, out, pos_sem, out_sem):
        self.me, self.core, self.at = me, core, at
        self.pos_hbm, self.gain_ref, self.bias_ref, self.h_ref, self.emb_ref = pos_hbm, gain_ref, bias_ref, h_ref, emb_ref
        self.pos, self.xs, self.out, self.pos_sem, self.out_sem = pos, xs, out, pos_sem, out_sem
        self.T = xs.shape[1] // 8
        self.blocks = h_ref.shape[0] // TOKENS

    def load(self, i):
        block = jnp.where(i < self.blocks, i, self.me)
        s = lax.rem(i, 2)
        return pltpu.make_async_copy(self.pos_hbm.at[pl.ds(pl.multiple_of(block * TOKENS, TOKENS), TOKENS)], self.pos.at[s], self.pos_sem.at[s])

    def store(self, i):
        s = lax.rem(i, 2)
        return pltpu.make_async_copy(self.out.at[s], self.h_ref.at[pl.ds(pl.multiple_of(i * TOKENS, TOKENS), TOKENS)], self.out_sem.at[s])

    def store_own(self, b):
        return pltpu.make_async_copy(self.out.at[b], self.emb_ref.at[b], self.out_sem.at[b])

    def tile(self, slot, j):
        return self.xs[slot, j * 8:(j + 1) * 8, :]

    def fetch(self, slot, seq, t, row_of):
        first = (lax.shift_right_logical(t, 7) * 2 + seq) * 128 + lax.bitwise_and(t, 127)
        for r in range(8):
            self.xs[slot, pl.ds(r, self.T, stride=8), :] = row_of(self.at[first + r]).astype(jnp.float32)

    def lanes(self, j):
        return slice(j * 128, (j + 1) * 128)

    def norm(self, i, g, lane_slot, row_of):
        T, xs = self.T, self.xs
        inv = 1.0 / (T * 128)
        t = pl.multiple_of(g * 16, 16)
        out = []
        for half in range(2):
            slot = lane_slot * 2 + half
            self.fetch(slot, self.core, i * TOKENS + g * 16 + half * 8, row_of)
            p = self.pos.at[lax.rem(i, 2), pl.ds(t, 16), :]
            s = None
            for j in range(T):
                e = (self.tile(slot, j) + p[half * 8:half * 8 + 8, self.lanes(j)].astype(jnp.float32)).astype(jnp.bfloat16).astype(jnp.float32)
                xs[slot, j * 8:(j + 1) * 8, :] = e
                s = e if s is None else s + e
            mean = jnp.broadcast_to(jnp.sum(s, axis=1, keepdims=True) * inv, (8, 128))
            s = None
            for j in range(T):
                c = self.tile(slot, j) - mean
                s = c * c if s is None else s + c * c
            var = jnp.sum(s, axis=1, keepdims=True) * inv
            out.append((slot, mean, jnp.broadcast_to(lax.rsqrt(var + EPS), (8, 128))))
        for j in range(T):
            y = [(self.tile(slot, j) - mean) * rs * self.gain_ref[:, self.lanes(j)] + self.bias_ref[:, self.lanes(j)] for slot, mean, rs in out]
            self.out[lax.rem(i, 2), pl.ds(t, 16), self.lanes(j)] = jnp.concatenate(y, axis=0).astype(jnp.bfloat16)

    def embed(self, b, g, lane_slot, row_of):
        t = pl.multiple_of(g * 16, 16)
        for half in range(2):
            self.fetch(lane_slot * 2 + half, b, self.me * TOKENS + t + half * 8, row_of)
        p = self.pos.at[self.blocks % 2, pl.ds(t, 16), :]
        for j in range(self.T):
            e = jnp.concatenate([self.tile(lane_slot * 2, j), self.tile(lane_slot * 2 + 1, j)], axis=0) + p[:, self.lanes(j)].astype(jnp.float32)
            self.out[b, pl.ds(t, 16), self.lanes(j)] = e.astype(jnp.bfloat16)

    def run(self, low, high, row_of):
        @pl.loop(low, high)
        def _(i):
            self.load(i).wait()
            self.load(i + 1).start()

            @pl.when(i >= 2)
            def _():
                self.store(i - 2).wait()

            @pl.loop(0, TOKENS // 64)
            def _(g):
                for j in range(4):
                    self.norm(i, g * 4 + j, j, row_of)
            self.store(i).start()

    def close(self, row_of):
        self.load(self.blocks).wait()
        for b in range(2):
            self.store(self.blocks - 2 + b).wait()

            @pl.loop(0, TOKENS // 64)
            def _(g):
                for j in range(4):
                    self.embed(b, g * 4 + j, j, row_of)
            self.store_own(b).start()
        for b in range(2):
            self.store_own(b).wait()

    @staticmethod
    def scratch(D):
        return [pltpu.VMEM((2, TOKENS, D), jnp.bfloat16), pltpu.VMEM((8, D // 128 * 8, 128), jnp.float32), pltpu.VMEM((2, TOKENS, D), jnp.bfloat16),
                pltpu.SemaphoreType.DMA((2,)), pltpu.SemaphoreType.DMA((2,))]


def broadcast_kernel(n, soon, early, at, rows_ref, pos_hbm, gain_ref, bias_ref, v_ref, w_ref, b_ref,
                     h_ref, emb_ref, minus_ref, plus_ref, w_par_ref, b_par_ref, rest_ref, ua, ub, *rest):
    send_sem, recv_sem, pass_send, pass_recv, vbuf, vsem = rest[-6:]
    q = Peers(n)
    me = q.me
    work = Norm(me, q.core, at, pos_hbm, gain_ref, bias_ref, h_ref, emb_ref, *rest[:-6])
    cap = rows_ref.shape[0]
    late = cap - soon
    spans = ((ua, soon, 0, soon // 2), (ua, soon, soon // 2, soon // 2), (ub, late, 0, late))

    def own(p):
        ref, _, low, size = spans[p]
        return rows_ref.at[pl.ds(low + (soon if ref is ub else 0), size)]

    def place(d, p):
        ref, per, low, size = spans[p]
        return ref.at[pl.ds(d * per + low, size)]

    moves = Spread(q, own, place, send_sem, recv_sem)
    left = vbuf.shape[0]
    last_rows = v_ref.at[pl.ds(v_ref.shape[0] - left - minus_ref.shape[0], minus_ref.shape[0])]
    rest_in = pltpu.make_async_copy(v_ref.at[pl.ds(v_ref.shape[0] - left, left)], vbuf, vsem)
    rest_out = pltpu.make_async_copy(vbuf, rest_ref, vsem)
    passed = [pltpu.make_async_remote_copy(src_ref=src, dst_ref=dst, send_sem=pass_send.at[i], recv_sem=pass_recv.at[i], device_id={"tp": to}, device_id_type=MESH)
              for i, (src, dst, to) in enumerate(((last_rows, minus_ref, q.plus), (last_rows, plus_ref, q.minus), (w_ref, w_par_ref, q.partner), (b_ref, b_par_ref, q.partner)))]
    work.load(0).start()
    q.greet((q.plus, q.minus, q.partner))
    moves.begin(0)
    moves.begin(1)
    for ref, low, size in ((ua, 0, soon), (ub, soon, late)):
        @pl.loop(0, size // 8)
        def _(k):
            for r in range(8):
                ref[me * size + k * 8 + r] = rows_ref[low + k * 8 + r]
    for c in passed[2:]:
        c.start()
    rest_in.start()
    rest_in.wait()
    rest_out.start()
    moves.turn(0)
    moves.turn(1)
    moves.begin(2)
    for p in range(2):
        moves.last(p)
    for p in range(2):
        moves.finish(p)

    def first(i):
        return ua[i]

    def any_(i):
        here = i < n * soon
        a, b = ua[jnp.minimum(i, n * soon - 1)], ub[jnp.maximum(i - n * soon, 0)]
        return jnp.where(here, a.astype(jnp.float32), b.astype(jnp.float32))

    blocks = early // TOKENS
    work.run(0, blocks - 2, first)
    moves.turn(2)
    for c in passed[:2]:
        c.start()
    work.run(blocks - 2, blocks, first)
    moves.last(2)
    moves.finish(2)
    work.run(blocks, work.blocks, any_)
    work.close(any_)
    for c in passed:
        c.wait()
    rest_out.wait()


def broadcast(n, soon, early, at, rows, pos, gain, bias, v, last, left, w, b, cid=3):
    seq, D = pos.shape
    cap, T, L = rows.shape
    A = pl.BlockSpec(memory_space=pl.ANY)
    V = pl.BlockSpec(memory_space=pltpu.VMEM)
    sems = pltpu.SemaphoreType.DMA((Spread.CHANNELS, 3))
    of = lambda r: jax.ShapeDtypeStruct((r, D), v.dtype)
    return pl.pallas_call(
        functools.partial(broadcast_kernel, n, soon, early),
        out_shape=(jax.ShapeDtypeStruct((seq, D), jnp.bfloat16), jax.ShapeDtypeStruct((2, seq // n, D), jnp.bfloat16),
                   of(last), of(last), jax.ShapeDtypeStruct(w.shape, w.dtype), jax.ShapeDtypeStruct(b.shape, b.dtype), of(left)),
        grid_spec=pltpu.PrefetchScalarGridSpec(
            num_scalar_prefetch=1, grid=(), in_specs=[V, A, V, V, A, A, V], out_specs=(A, A, A, A, A, V, A),
            scratch_shapes=[pltpu.VMEM((n * soon, T, L), rows.dtype), pltpu.VMEM((n * (cap - soon), T, L), rows.dtype), *Norm.scratch(D), sems, sems, *[pltpu.SemaphoreType.DMA((4,))] * 2, pltpu.VMEM((left, D), v.dtype), pltpu.SemaphoreType.DMA]),
        compiler_params=pltpu.CompilerParams(vmem_limit_bytes=VMEM, collective_id=cid, has_side_effects=True),
        name="broadcast",
    )(at, rows, pos, gain, bias, v, w, b)


def norm_kernel(at, x_hbm, pos_hbm, gain_ref, bias_ref, h_ref, emb_ref, x, sem, *rest):
    me = lax.axis_index("tp")
    work = Norm(me, lax.rem(me, 2), at, pos_hbm, gain_ref, bias_ref, h_ref, emb_ref, *rest)
    work.load(0).start()
    c = pltpu.make_async_copy(x_hbm, x, sem)
    c.start()
    c.wait()
    work.run(0, work.blocks, lambda i: x[i])
    work.close(lambda i: x[i])


def norm(n, at, x, pos, gain, bias):
    seq, D = pos.shape
    A = pl.BlockSpec(memory_space=pl.ANY)
    V = pl.BlockSpec(memory_space=pltpu.VMEM)
    return pl.pallas_call(
        norm_kernel,
        out_shape=(jax.ShapeDtypeStruct((seq, D), jnp.bfloat16), jax.ShapeDtypeStruct((2, seq // n, D), jnp.bfloat16)),
        grid_spec=pltpu.PrefetchScalarGridSpec(
            num_scalar_prefetch=1, grid=(), in_specs=[A, A, V, V], out_specs=(A, A),
            scratch_shapes=[pltpu.VMEM(x.shape, x.dtype), pltpu.SemaphoreType.DMA, *Norm.scratch(D)]),
        compiler_params=pltpu.CompilerParams(vmem_limit_bytes=VMEM),
        name="norm",
    )(at, x, pos, gain, bias)


def project_kernel(chunk, wa_hbm, wb_hbm, ba_ref, bb_ref, emb_hbm, h_ref, qkv_ref, emb_out, w, bc, emb, wsem, esem):
    step = pl.program_id(0)
    core = lax.rem(lax.axis_index("tp"), 2)
    M = wa_hbm.shape[0]
    tb = h_ref.shape[0]

    def load(k):
        return pltpu.make_async_copy((wa_hbm, wb_hbm)[k], w.at[lax.rem(core + k, 2)], wsem.at[lax.rem(core + k, 2)])

    def loaded(k):
        return pltpu.make_async_copy(wa_hbm, w.at[k], wsem.at[k])

    @pl.when(step == 0)
    def _():
        for k in range(2):
            load(k).start()
        pltpu.make_async_copy(emb_hbm, emb, esem).start()
        _, H, E = ba_ref.shape
        for k, b in enumerate((ba_ref, bb_ref)):
            for r in range(3 * H):
                bc[lax.rem(core + k, 2), r * E:(r + 1) * E, :] = jnp.broadcast_to(b[r // H, r % H:r % H + 1, :], (128, E)).T

    @pl.when(step == 1)
    def _():
        pltpu.make_async_copy(emb_hbm, emb, esem).wait()
        pltpu.make_async_copy(emb, emb_out, esem).start()

    @pl.when(step == pl.num_programs(0) - 1)
    def _():
        pltpu.make_async_copy(emb, emb_out, esem).wait()

    for k in range(2):
        @pl.when(step == 0)
        def _():
            loaded(k).wait()
        for m in range(0, M, chunk):
            o = lax.dot_general(w[k, m:m + chunk, :], h_ref[...], (((1,), (1,)), ((), ())), preferred_element_type=jnp.float32)
            b = jnp.concatenate([bc[k, m:m + chunk, :]] * (tb // 128), axis=1)
            qkv_ref[k, m:m + chunk, :] = (o + b).astype(jnp.bfloat16)


def project(h, emb, wa, wb, ba, bb, tb=512, chunk=384):
    seq, D = h.shape
    M = wa.shape[0]
    A = pl.BlockSpec(memory_space=pl.ANY)
    one = lambda shape: pl.BlockSpec(shape, lambda i: (0,) * len(shape), pipeline_mode=pl.Buffered(1))
    return pl.pallas_call(
        functools.partial(project_kernel, chunk),
        out_shape=(jax.ShapeDtypeStruct((2, M, seq), jnp.bfloat16), jax.ShapeDtypeStruct(emb.shape, emb.dtype)),
        grid=(seq // tb,),
        in_specs=[A, A, one(ba.shape), one(bb.shape), A, pl.BlockSpec((tb, D), lambda i: (i, 0))],
        out_specs=(pl.BlockSpec((2, M, tb), lambda i: (0, 0, i)), A),
        scratch_shapes=[pltpu.VMEM((2, M, D), wa.dtype), pltpu.VMEM((2, M, 128), jnp.float32), pltpu.VMEM(emb.shape, emb.dtype), pltpu.SemaphoreType.DMA((2,)), pltpu.SemaphoreType.DMA],
        compiler_params=pltpu.CompilerParams(vmem_limit_bytes=VMEM),
        cost_estimate=pl.CostEstimate(flops=4 * seq * M * D, bytes_accessed=50 * 2**20, transcendentals=0),
        name="project",
    )(wa, wb, ba, bb, emb, h)


def attend_kernel(n, scale, qb, nb, early, where, qkv_ref, emb_hbm, bias_ref, *refs):
    pieces, (out_ref, kk, vv, sc, ctx, got, w, a, acc, emb, load_sem, pass_send, pass_recv, emb_sem, send_sem, recv_sem, turn_send, turn_recv) = refs[:len(where)], refs[len(where):]
    E, S = qkv_ref.shape[3:]
    heads = got.shape[1] // E
    N = S // qb
    c = scale * 1.4426950408889634
    q = Peers(n)
    me, core = q.me, q.core
    head = pl.program_id(0)
    cut = early * E // 256 * 256
    owners = {0: me, 1: q.plus, 2: q.opp, -1: q.minus}

    def loads():
        cs = []
        for i, (ref, (away, low)) in enumerate(zip(pieces, where)):
            dst = w.at[owners[away], pl.ds(low, ref.shape[0])]
            cs.append(pltpu.make_async_copy(ref, dst, load_sem.at[i]))
            cs.append(pltpu.make_async_remote_copy(src_ref=ref, dst_ref=dst, send_sem=pass_send.at[i], recv_sem=pass_recv.at[i], device_id={"tp": q.partner}, device_id_type=MESH))
        return cs

    rest = pieces[-1].shape[0]
    half = rest // 2

    def across(i, owner, src, to, sem):
        dst = w.at[owner, pl.ds(w.shape[1] - rest + i * half, half)]
        return pltpu.make_async_remote_copy(src_ref=dst if src is None else src.at[pl.ds(i * half, half)], dst_ref=dst, send_sem=turn_send.at[sem], recv_sem=turn_recv.at[sem],
                                            device_id={"tp": to}, device_id_type=MESH)

    passing = ((q.minus, pieces[-2], q.plus), (q.plus, pieces[-1], q.minus))

    def send(h, s):
        to = lax.rem(me + s, n)
        return pltpu.make_async_remote_copy(src_ref=ctx.at[h, to], dst_ref=got.at[me, pl.ds(pl.multiple_of(h * E, 32), E)],
                                            send_sem=send_sem.at[s], recv_sem=recv_sem.at[lax.div(h, early), s], device_id={"tp": to}, device_id_type=MESH)

    load_emb = pltpu.make_async_copy(emb_hbm, emb, emb_sem)

    @pl.when(head == 0)
    def _():
        q.greet([lax.rem(me + s, n) for s in range(1, n)])
        for i, (owner, src, to) in enumerate(passing):
            across(i, owner, src, to, i).start()
        vv[E:, :] = jnp.where(lax.broadcasted_iota(jnp.int32, (vv.shape[0] - E, S), 0) == 0, 1.0, 0.0).astype(jnp.bfloat16)

    @pl.when(head > 0)
    def _():
        for s in range(1, n):
            send(head - 1, s).start()

    @pl.when(head == 1)
    def _():
        for c_ in loads():
            c_.start()
        load_emb.start()

    @pl.when(head == 4)
    def _():
        for i in range(2):
            across(i, q.opp, None, q.partner, i).wait_recv()
            across(i, q.opp, None, q.partner, 2 + i).start()

    for t in range(0, S, 128):
        kk[t:t + 128, :] = qkv_ref[0, 1, 0, :, t:t + 128].astype(jnp.float32).T.astype(jnp.bfloat16)
    vv[0:E, :] = qkv_ref[0, 2, 0]
    keep = lax.broadcasted_iota(jnp.int32, (qb, qb), 0) <= lax.broadcasted_iota(jnp.int32, (qb, qb), 1)

    def scores(i, k, m):
        s = jnp.dot(kk[k * qb:(k + 1) * qb, :], qkv_ref[0, 0, 0, :, i * qb:(i + 1) * qb], preferred_element_type=jnp.float32)
        if k == i:
            s = jnp.where(keep, s, -jnp.inf)
        sc[i % 2, k * qb:(k + 1) * qb, :] = s
        top = jnp.max(s.reshape(qb // 8, 8, qb), axis=0)
        return top if m is None else jnp.maximum(m, top)

    def weigh(i, k, mc, o):
        s = sc[i % 2, k * qb:(k + 1) * qb, :]
        p = jnp.exp2(s * c - mc).astype(jnp.bfloat16)
        d = jnp.dot(vv[:, k * qb:(k + 1) * qb], p, preferred_element_type=jnp.float32)
        return d if o is None else o + d

    m = scores(0, 0, None)
    for i in range(N):
        mc = jnp.max(m, axis=0, keepdims=True) * c
        o = m = None
        for k in range(i + 2):
            if i + 1 < N:
                m = scores(i + 1, k, m)
            if k <= i:
                o = weigh(i, k, mc, o)
        ctx[head, i] = (o[0:E] * (1.0 / o[E:E + 1])).astype(jnp.bfloat16)
    got[me, pl.ds(pl.multiple_of(head * E, 32), E), :] = ctx[head, me]

    @pl.when(head == heads - 1)
    def _():
        for s in range(1, n):
            send(head, s).start()
        K = got.shape[1]

        def arrive(group, low, high):
            for s in range(1, n):
                fr = lax.rem(me - s + n, n)
                r = got.at[fr, pl.ds(low, high - low)]
                pltpu.make_async_remote_copy(src_ref=r, dst_ref=r, send_sem=send_sem.at[s], recv_sem=recv_sem.at[group, s], device_id={"tp": fr}, device_id_type=MESH).wait_recv()

        def turn_over(low, high):
            for s in range(n):
                for k in range(low, high, 128):
                    for t in range(0, qb, 128):
                        at = s // 2 * (high - low) + (k - low) + (n // 2) * low
                        a[(s % 2) * qb + t:(s % 2) * qb + t + 128, at:at + 128] = got[s, k:k + 128, t:t + 128].astype(jnp.float32).T.astype(jnp.bfloat16)

        def part(low, high, cols):
            rows = [w[2 * i:2 * i + 2, :, cols].reshape(K, nb)[low:high] for i in range(n // 2)]
            return jnp.dot(a[:, n // 2 * low:n // 2 * high], jnp.concatenate(rows, axis=0), preferred_element_type=jnp.float32)

        arrive(0, 0, early * E)
        turn_over(0, cut)
        for c_ in loads():
            c_.wait()
        load_emb.wait()
        for i, (owner, src, to) in enumerate(passing):
            across(i, owner, src, to, i).wait_send()
            across(i, q.other(q.opp), None, q.partner, 2 + i).wait()

        @pl.loop(0, w.shape[2] // nb)
        def _(j):
            cols = pl.ds(pl.multiple_of(j * nb, nb), nb)
            acc[:, cols] = part(0, cut, cols) + bias_ref[:, cols]

        arrive(1, early * E, K)
        turn_over(cut, K)

        @pl.loop(0, w.shape[2] // nb)
        def _(j):
            cols = pl.ds(pl.multiple_of(j * nb, nb), nb)
            o = part(cut, K, cols) + acc[:, cols]
            for b in range(2):
                out_ref[b, :, cols] = (emb[b, :, cols].astype(jnp.float32) + o[b * qb:(b + 1) * qb]).astype(jnp.bfloat16)

        for s in range(1, n):
            r = got.at[lax.rem(me - s + n, n)]
            pltpu.make_async_remote_copy(src_ref=r, dst_ref=r, send_sem=send_sem.at[s], recv_sem=recv_sem.at[0, s], device_id={"tp": q.partner}, device_id_type=MESH).wait_send()


def attend(n, qkv, pieces, where, emb, bias, early=6, nb=1024, cid=1, qb=256):
    heads, E, S = 2 * qkv.shape[2], *qkv.shape[3:]
    H = heads // 2
    D = emb.shape[2]
    A = pl.BlockSpec(memory_space=pl.ANY)
    one = lambda shape: pl.BlockSpec(shape, lambda h: (0,) * len(shape), pipeline_mode=pl.Buffered(1))
    bf = jnp.bfloat16
    return pl.pallas_call(
        functools.partial(attend_kernel, n, E ** -0.5, qb, nb, early, where),
        out_shape=jax.ShapeDtypeStruct(emb.shape, bf),
        grid=(heads,),
        in_specs=[pl.BlockSpec((1, 3, 1, E, S), lambda h: (h // H, 0, h % H, 0, 0)), A, one(bias.shape)] + [A] * len(pieces),
        out_specs=one(emb.shape),
        scratch_shapes=[pltpu.VMEM((S, E), bf), pltpu.VMEM((E + 16, S), bf), pltpu.VMEM((2, S, qb), jnp.float32),
                        pltpu.VMEM((heads, n, E, qb), bf), pltpu.VMEM((n, heads * E, qb), bf), pltpu.VMEM((n, H * E, D), bf), pltpu.VMEM((2 * qb, n * H * E), bf),
                        pltpu.VMEM((2 * qb, D), jnp.float32), pltpu.VMEM(emb.shape, bf),
                        *[pltpu.SemaphoreType.DMA((len(pieces),))] * 3, pltpu.SemaphoreType.DMA, pltpu.SemaphoreType.DMA((n,)), pltpu.SemaphoreType.DMA((2, n)), *[pltpu.SemaphoreType.DMA((4,))] * 2],
        compiler_params=pltpu.CompilerParams(collective_id=cid, has_side_effects=True, vmem_limit_bytes=VMEM),
        name="attend",
    )(qkv, emb, bias, *pieces)


CAP = 264
SOON, EARLY = 200, 1280


def place_kernel(code_ref, u_ref, x_ref, out_ref, sem):
    @pl.loop(0, code_ref.shape[0])
    def _(t):
        c = code_ref[t]

        @pl.when(c >= 0)
        def _():
            copy = pltpu.make_async_copy(u_ref.at[c], out_ref.at[t], sem)
            copy.start()
            copy.wait()


def place(at, u, x):
    A = pl.BlockSpec(memory_space=pl.ANY)
    return pl.pallas_call(
        place_kernel,
        out_shape=jax.ShapeDtypeStruct(x.shape, x.dtype),
        grid_spec=pltpu.PrefetchScalarGridSpec(num_scalar_prefetch=1, grid=(), in_specs=[A, A], out_specs=A, scratch_shapes=[pltpu.SemaphoreType.DMA]),
        input_output_aliases={2: 0},
        name="place",
    )(at, u, x)


def solution(mesh):
    n = mesh.shape["tp"]
    def local_step(token_ids, word_shard, pos_table, ln_gain, ln_bias, w_qkv, b_qkv, w_out, b_out):
        me = lax.axis_index("tp")
        core = lax.rem(me, 2)
        seq, D = pos_table.shape
        H, E = w_qkv.shape[2:]
        shard_rows = word_shard.shape[0]
        w_own = jnp.transpose(w_qkv, (1, 2, 3, 0)).reshape(3 * H * E, D)
        v_own = w_out.reshape(H * E, D)
        ring = lambda step: [(d, (d + 2 * step) % n) for d in range(n)]
        send = lambda x, step: lax.ppermute(x, "tp", ring(step))
        v_head = w_out[:2].reshape(2 * E, D)
        minus0, plus0 = send(v_head, 1), send(v_head, -1)
        blk = seq // n
        gain, bias = ln_gain[None], ln_bias[None]
        code, at, counts, mine = pick(n, shard_rows, CAP, SOON, EARLY, token_ids, word_shard)
        mine, minus0, plus0 = lax.optimization_barrier((mine, minus0, plus0))
        h, embed, minus1, plus1, w_par, b_par, v_tail = broadcast(n, SOON, EARLY, at.reshape(-1), mine, pos_table, gain, bias, v_own, (H - 3) * E, E, w_own, b_qkv)
        counts, h = lax.optimization_barrier((counts, h))

        rounds = jnp.where((counts[0, 0] > CAP) | (counts[1, 0] > SOON), (counts[0, 0] + CAP - 1) // CAP, 0)
        total = max(n * CAP, seq + blk)

        def by_token(x):
            return x.reshape(seq // 128, 2, 128).transpose(1, 0, 2)

        def wanted(x):
            own = lax.dynamic_index_in_dim(x, core, 0, keepdims=False)
            other = lax.dynamic_index_in_dim(x, 1 - core, 0, keepdims=False)
            return jnp.concatenate([own, lax.dynamic_slice_in_dim(other, me * blk, blk)])

        def more(carry):
            def one_round(carry):
                r, x = carry
                codes = by_token(code).reshape(2, seq)
                slot = codes % SPAN - r * CAP
                hit = (slot >= 0) & (slot < CAP)
                here = jnp.where(hit & (codes // SPAN == me), slot, -1).reshape(-1)
                ids = token_ids.reshape(-1) - me * shard_rows
                chosen = jnp.max(jnp.where(here[None, :] == jnp.arange(CAP)[:, None], ids[None, :], 0), axis=1)
                v = gather_all(n, rows(CAP, chosen, word_shard), total)
                return r + 1, place(wanted(jnp.where(hit, codes // SPAN * CAP + slot, -1)), v, x)

            x = jnp.zeros((total,) + mine.shape[1:], mine.dtype)
            _, x = lax.while_loop(lambda c: c[0] < rounds, one_round, (jnp.int32(0), x))
            t = jnp.arange(seq, dtype=jnp.int32)
            t = jnp.stack([jnp.where(core == b, t, jnp.clip(t - me * blk, 0, blk - 1) + seq) for b in range(2)])
            t = t.reshape(2, seq // 128, 128).transpose(1, 0, 2).reshape(-1)
            return (jnp.int32(0),) + tuple(norm(n, t, x, pos_table, gain, bias))

        _, h, embed = lax.while_loop(lambda c: c[0] > 0, more, (rounds, h, embed))

        minus0, h = lax.optimization_barrier((minus0, h))
        minus2, plus2, opp0, opp1 = send(v_tail, 1), send(v_tail, -1), send(minus0, 1), send(plus1, -1)
        pieces = [v_own, minus0, plus0, minus1, plus1, opp0, opp1, minus2, plus2]
        where = ((0, 0), (-1, 0), (1, 0), (-1, 2 * E), (1, 2 * E), (2, 0), (2, 2 * E), (-1, (H - 1) * E), (1, (H - 1) * E))
        qkv, embed = project(h, embed, w_own, w_par, b_qkv, b_par)
        resid_out = attend(n, qkv.reshape(2, 3, H, E, seq), pieces, where, embed, b_out[None])
        return resid_out, embed

    in_specs = (P("dp", None), P("tp", None), P(None, None), P(None), P(None), P(None, None, "tp", None), P(None, "tp", None), P("tp", None, None), P(None))
    out_specs = (P("dp", "tp", None), P("dp", "tp", None))
    return jax.shard_map(local_step, mesh=mesh, in_specs=in_specs, out_specs=out_specs, check_vma=False)
```

```python
import functools

import jax
import jax.numpy as jnp
from jax import lax
from jax.experimental import pallas as pl
from jax.experimental.pallas import tpu as pltpu
from jax.sharding import PartitionSpec as P

MESH = pl.DeviceIdType.MESH
VMEM = 63 * 2**20


class Peers:
    def __init__(self, n):
        self.n = n
        self.me = lax.axis_index("tp")
        self.chip, self.core = lax.div(self.me, 2), lax.rem(self.me, 2)
        self.plus, self.minus, self.opp = self.near(1), self.near(-1), self.near(2)
        self.partner = self.other(self.me)

    def near(self, s):
        chips = self.n // 2
        return lax.rem(self.chip + s + chips, chips) * 2 + self.core

    def other(self, d):
        return d + 1 - 2 * self.core

    def greet(self, devices):
        barrier = pltpu.get_barrier_semaphore()
        for d in devices:
            pl.semaphore_signal(barrier, inc=1, device_id={"tp": d}, device_id_type=MESH)
        pl.semaphore_wait(barrier, len(devices))


class Spread:
    CHANNELS = 9

    def __init__(self, peers, own, place, send_sem, recv_sem):
        self.q, self.own, self.place, self.send_sem, self.recv_sem = peers, own, place, send_sem, recv_sem

    def half(self, ref, i):
        rows = ref.shape[0] // 2
        return ref.at[pl.ds(i * rows, rows)]

    def copy(self, channel, p, src, dst, to):
        return pltpu.make_async_remote_copy(src_ref=src, dst_ref=dst, send_sem=self.send_sem.at[channel, p], recv_sem=self.recv_sem.at[channel, p],
                                            device_id={"tp": to}, device_id_type=MESH)

    def got(self, channel, p, ref):
        self.copy(channel, p, ref, ref, self.q.partner).wait_recv()

    def begin(self, p):
        q = self.q
        for channel, to in ((0, q.plus), (1, q.minus), (4, q.partner)):
            self.copy(channel, p, self.own(p), self.place(q.me, p), to).start()

    def turn(self, p):
        q = self.q
        for i, (d, to) in enumerate(((q.minus, q.plus), (q.plus, q.minus))):
            ref = self.place(d, p)
            self.got(i, p, ref)
            self.copy(2 + i, p, self.half(ref, i), self.half(ref, i), to).start()
            self.copy(5 + i, p, ref, ref, q.partner).start()

    def last(self, p):
        q = self.q
        for i in range(2):
            c = self.half(self.place(q.opp, p), i)
            self.got(2 + i, p, c)
            self.copy(7 + i, p, c, c, q.partner).start()

    def finish(self, p):
        q = self.q
        own, a, b, c = (self.place(d, p) for d in (q.partner, q.other(q.minus), q.other(q.plus), q.other(q.opp)))
        for channel, ref in ((4, own), (5, a), (6, b), (7, self.half(c, 0)), (8, self.half(c, 1))):
            self.got(channel, p, ref)
        for channel, ref in ((0, own), (1, own), (4, own), (5, a), (6, b), (2, self.half(c, 0)), (3, self.half(c, 1)), (7, self.half(c, 0)), (8, self.half(c, 1))):
            self.copy(channel, p, ref, ref, q.partner).wait_send()


def gather_all_kernel(n, S, src_ref, all_ref, loc_sem, send_sem, recv_sem):
    cap = src_ref.shape[0]

    def of(d):
        return all_ref.at[pl.ds(d * cap, cap)]
    chips = n // 2
    me = lax.axis_index("tp")
    chip, core = me // 2, lax.rem(me, 2)
    def at(c):
        return lax.rem(c + chips, chips) * 2 + core
    plus, minus, opp = at(chip + 1), at(chip - 1), at(chip + 2)
    partner = me + 1 - 2 * core
    P = 2 * S
    step = src_ref.shape[0] // P

    barrier = pltpu.get_barrier_semaphore()
    for d in (plus, minus, partner):
        pl.semaphore_signal(barrier, inc=1, device_id={"tp": d}, device_id_type=MESH)
    pl.semaphore_wait(barrier, 3)

    started = []
    def rc(src, dst, ch, k, dev):
        return pltpu.make_async_remote_copy(src_ref=src, dst_ref=dst, send_sem=send_sem.at[ch, k], recv_sem=recv_sem.at[ch, k],
                                            device_id={"tp": dev}, device_id_type=MESH)
    def go(src, dst, ch, k, dev):
        c = rc(src, dst, ch, k, dev)
        c.start()
        started.append(c)
    def piece(ref, k):
        return ref.at[pl.ds(k * step, step)]
    first, last = list(range(S)), list(range(S, P))
    for a, b in zip(first, last):
        go(piece(src_ref, a), piece(of(me), a), 0, a, plus)
        go(piece(src_ref, b), piece(of(me), b), 1, b, minus)
    for a, b in zip(first, last):
        go(piece(src_ref, b), piece(of(me), b), 0, b, plus)
        go(piece(src_ref, a), piece(of(me), a), 1, a, minus)
    go(src_ref, of(me), 4, 0, partner)
    loc = pltpu.make_async_copy(src_ref, of(me), loc_sem)
    loc.start()
    def got(owner, ch, k):
        r = piece(of(owner), k)
        rc(r, r, ch, k, partner).wait_recv()
        return r
    for a, b in zip(first, last):
        r = got(minus, 0, a)
        go(r, r, 2, a, plus)
        go(r, r, 5, a, partner)
        r = got(plus, 1, b)
        go(r, r, 3, b, minus)
        go(r, r, 6, b, partner)
    for a, b in zip(first, last):
        r = got(minus, 0, b)
        go(r, r, 5, b, partner)
        r = got(plus, 1, a)
        go(r, r, 6, a, partner)
    for a, b in zip(first, last):
        r = got(opp, 2, a)
        go(r, r, 7, a, partner)
        r = got(opp, 3, b)
        go(r, r, 7, b, partner)
    other = lambda d: d + 1 - 2 * core
    r = of(partner)
    rc(r, r, 4, 0, partner).wait_recv()
    for k in range(P):
        got(other(minus), 5, k)
        got(other(plus), 6, k)
        got(other(opp), 7, k)
    loc.wait()
    for c in started:
        c.wait_send()


def gather_all(n, rows, total, S=2, cid=0):
    return pl.pallas_call(
        functools.partial(gather_all_kernel, n, S),
        out_shape=jax.ShapeDtypeStruct((total,) + rows.shape[1:], rows.dtype),
        in_specs=[pl.BlockSpec(memory_space=pltpu.VMEM)],
        out_specs=pl.BlockSpec(memory_space=pl.ANY),
        scratch_shapes=[pltpu.SemaphoreType.DMA, pltpu.SemaphoreType.DMA((8, 2 * S)), pltpu.SemaphoreType.DMA((8, 2 * S))],
        compiler_params=pltpu.CompilerParams(collective_id=cid, has_side_effects=True),
        name="gather_all",
    )(rows)


SPAN_BITS = 13
SPAN = 1 << SPAN_BITS


def pick_kernel(n, shard_rows, cap, soon, early, nb, ids_ref, table_ref, code_ref, at_ref, cnt_ref, out_ref,
                ids, col, wcol, first, wanted, list_ref, buf, scr, list_sem, sem):
    me = lax.axis_index("tp")
    R, L = ids.shape
    G, Q = 8, 4
    lane = lax.broadcasted_iota(jnp.int32, (8, L), 1)
    sub = lax.broadcasted_iota(jnp.int32, (8, L), 0)
    for r in range(R):
        o, b = divmod(r, ids_ref.shape[0])
        ids[r:r + 1, :] = ids_ref[b:b + 1, o * L:(o + 1) * L]

    def columns(*pairs):
        @pl.loop(0, R // Q)
        def _(g):
            for k in range(Q):
                a = g * Q + k
                for src, dst in pairs:
                    dst[pl.ds(pl.multiple_of(a * L, L), L), :] = jnp.broadcast_to(src[pl.ds(a, 1), :], (L, L)).T

    def against(bg, start, step):
        acc = start
        def body(a, acc):
            acc = list(acc)
            for k in range(L // 8):
                at = pl.ds(pl.multiple_of(a * L + k * 8, 8), 8)
                step(acc, at, k, range(G), -1)
            return tuple(acc)
        acc = list(lax.fori_loop(0, bg * G, body, tuple(acc)))
        for d in range(G):
            for k in range(L // 8):
                step(acc, pl.ds((bg * G + d) * L + k * 8, 8), k, range(d, G), d)
        return acc

    def wide(ref, bg):
        return [jnp.broadcast_to(ref[bg * G + i:bg * G + i + 1, :], (8, L)) for i in range(G)]

    columns((ids, col))
    for bg in range(R // G):
        rows = wide(ids, bg)
        def seen(acc, at, k, which, same):
            c = col[at, :]
            for i in which:
                hit = c == rows[i]
                if i == same:
                    hit = hit & (k * 8 + sub < lane)
                acc[i] = jnp.where(hit, 1, acc[i])
        acc = against(bg, [jnp.zeros((8, L), jnp.int32)] * G, seen)
        for i in range(G):
            first[bg * G + i:bg * G + i + 1, :] = 1 - jnp.max(acc[i], axis=0, keepdims=True)

    x = ids[...]
    owner = jnp.zeros((R, L), jnp.int32)
    for o in range(1, n):
        owner = owner + jnp.where(x >= o * shard_rows, 1, 0)
    isf = first[...] == 1
    one = jnp.concatenate([jnp.where(isf & (owner == o), 1.0, 0.0) for o in range(n)], axis=0).astype(jnp.bfloat16)
    up = (lax.broadcasted_iota(jnp.int32, (L, L), 0) < lax.broadcasted_iota(jnp.int32, (L, L), 1)).astype(jnp.float32).astype(jnp.bfloat16)
    prefix = jnp.dot(one, up, preferred_element_type=jnp.float32)
    tot = jnp.dot(one, jnp.ones((L, L), jnp.bfloat16), preferred_element_type=jnp.float32)
    r = lax.broadcasted_iota(jnp.int32, (n * R, n * R), 0)
    c = lax.broadcasted_iota(jnp.int32, (n * R, n * R), 1)
    low = ((r // R == c // R) & (c < r)).astype(jnp.float32).astype(jnp.bfloat16)
    off = jnp.dot(low, tot.astype(jnp.bfloat16), preferred_element_type=jnp.float32)
    pos = prefix + off
    slot = jnp.zeros((R, L), jnp.float32)
    most = jnp.zeros((1, L), jnp.float32)
    for o in range(n):
        slot = jnp.where(owner == o, pos[o * R:(o + 1) * R], slot)
        most = jnp.maximum(most, (off + tot)[(o + 1) * R - 1:(o + 1) * R])
    cnt_ref[0:1, :] = most.astype(jnp.int32)
    code_ref[...] = jnp.where(isf, owner * SPAN + slot.astype(jnp.int32), -1)
    first[...] = jnp.where(isf, x, -1)
    columns((first, col), (code_ref, wcol))

    for bg in range(R // G):
        rows = wide(ids, bg)
        def take(acc, at, k, which, same):
            c, w = col[at, :], wcol[at, :]
            for i in which:
                acc[i] = jnp.where(c == rows[i], w, acc[i])
        acc = against(bg, [jnp.zeros((8, L), jnp.int32)] * G, take)
        for i in range(G):
            code_ref[bg * G + i:bg * G + i + 1, :] = jnp.max(acc[i], axis=0, keepdims=True)
    code = code_ref[...]
    who, slot = lax.shift_right_logical(code, SPAN_BITS), lax.bitwise_and(code, SPAN - 1)
    at_ref[...] = jnp.where(slot < soon, who * soon + slot, n * soon + who * (cap - soon) + jnp.minimum(slot, cap - 1) - soon)
    seen = jnp.max(slot[0:early // L * ids_ref.shape[0], :], axis=0, keepdims=True)
    cnt_ref[1:2, :] = jnp.broadcast_to(jnp.max(seen, axis=1, keepdims=True) + 1, (1, L))

    K = wanted.shape[0]
    want = [me * SPAN + i * L + lane for i in range(K)]
    def body(a, acc):
        acc = list(acc)
        for k in range(L // 8):
            at = pl.ds(pl.multiple_of(a * L + k * 8, 8), 8)
            c, w = col[at, :], wcol[at, :]
            for i in range(K):
                acc[i] = jnp.where(w == want[i], c, acc[i])
        return tuple(acc)
    acc = lax.fori_loop(0, R, body, tuple(jnp.zeros((8, L), jnp.int32) for _ in range(K)))
    for i in range(K):
        wanted[i:i + 1, :] = jnp.maximum(jnp.max(acc[i], axis=0, keepdims=True) - me * shard_rows, 0)
    listed = pltpu.make_async_copy(wanted, list_ref, list_sem)
    listed.start()
    listed.wait()
    take_rows(cap, nb, lambda k: list_ref[lax.shift_right_logical(k, 7), lax.bitwise_and(k, L - 1)], table_ref, out_ref, buf, scr, sem)


def take_rows(cap, nb, row_of, table_ref, out_ref, buf, scr, sem):
    T = table_ref.shape[1] // 128
    U = 8

    def copy(k):
        base = pl.multiple_of(lax.bitwise_and(row_of(k), -8), 8)
        s = lax.bitwise_and(k, nb - 1)
        return pltpu.make_async_copy(table_ref.at[pl.ds(base, 8)], buf.at[s], sem.at[s])

    @pl.loop(0, nb)
    def _(k):
        copy(k).start()

    def group(q, more):
        for u in range(U):
            k = q * U + u
            s = lax.bitwise_and(k, nb - 1)
            copy(k).wait()
            for j in range(T):
                scr[u, j * 8:(j + 1) * 8, :] = buf[s, :, j * 128:(j + 1) * 128].astype(jnp.float32)
            r = lax.bitwise_and(row_of(k), 7)
            out_ref[k] = scr[u, pl.ds(r, T, stride=8), :].astype(jnp.bfloat16)
        if more:
            for u in range(U):
                copy(q * U + u + nb).start()

    pl.loop(0, (cap - nb) // U)(lambda q: group(q, True))
    pl.loop((cap - nb) // U, cap // U)(lambda q: group(q, False))


def pick(n, shard_rows, cap, soon, early, ids, table, nb=32):
    R, L = ids.size // 128, 128
    K = -(-cap // L)
    T = table.shape[1] // 128
    V = pl.BlockSpec(memory_space=pltpu.VMEM)
    i32 = lambda *shape: jax.ShapeDtypeStruct(shape, jnp.int32)
    vm = lambda *shape: pltpu.VMEM(shape, jnp.int32)
    return pl.pallas_call(
        functools.partial(pick_kernel, n, shard_rows, cap, soon, early, nb),
        out_shape=(i32(R, L), i32(R, L), i32(2, L), jax.ShapeDtypeStruct((cap, T, 128), table.dtype)),
        in_specs=[V, pl.BlockSpec(memory_space=pl.ANY)],
        out_specs=(V, V, V, V),
        scratch_shapes=[vm(R, L), vm(R * L, L), vm(R * L, L), vm(R, L), vm(K, L), pltpu.SMEM((K, L), jnp.int32),
                        pltpu.VMEM((nb, 8, T * 128), table.dtype), pltpu.VMEM((8, T * 8, 128), jnp.float32), pltpu.SemaphoreType.DMA, pltpu.SemaphoreType.DMA((nb,))],
        compiler_params=pltpu.CompilerParams(vmem_limit_bytes=VMEM),
        cost_estimate=pl.CostEstimate(flops=2 * 10**10, bytes_accessed=cap * 8 * T * 256, transcendentals=0),
        name="pick",
    )(ids, table)


def rows_kernel(cap, nb, list_ref, table_ref, out_ref, buf, scr, sem):
    take_rows(cap, nb, lambda k: list_ref[k], table_ref, out_ref, buf, scr, sem)


def rows(cap, lst, table, nb=32):
    T = table.shape[1] // 128
    return pl.pallas_call(
        functools.partial(rows_kernel, cap, nb),
        out_shape=jax.ShapeDtypeStruct((cap, T, 128), table.dtype),
        grid_spec=pltpu.PrefetchScalarGridSpec(
            num_scalar_prefetch=1, grid=(),
            in_specs=[pl.BlockSpec(memory_space=pl.ANY)],
            out_specs=pl.BlockSpec(memory_space=pltpu.VMEM),
            scratch_shapes=[pltpu.VMEM((nb, 8, table.shape[1]), table.dtype), pltpu.VMEM((8, T * 8, 128), jnp.float32), pltpu.SemaphoreType.DMA((nb,))]),
        name="rows",
    )(lst, table)


EPS = 1e-5
TOKENS = 256


class Norm:
    def __init__(self, me, core, at, pos_hbm, gain_ref, bias_ref, h_ref, emb_ref, pos, xs, out, pos_sem, out_sem):
        self.me, self.core, self.at = me, core, at
        self.pos_hbm, self.gain_ref, self.bias_ref, self.h_ref, self.emb_ref = pos_hbm, gain_ref, bias_ref, h_ref, emb_ref
        self.pos, self.xs, self.out, self.pos_sem, self.out_sem = pos, xs, out, pos_sem, out_sem
        self.T = xs.shape[1] // 8
        self.blocks = h_ref.shape[0] // TOKENS

    def load(self, i):
        block = jnp.where(i < self.blocks, i, self.me)
        s = lax.rem(i, 2)
        return pltpu.make_async_copy(self.pos_hbm.at[pl.ds(pl.multiple_of(block * TOKENS, TOKENS), TOKENS)], self.pos.at[s], self.pos_sem.at[s])

    def store(self, i):
        s = lax.rem(i, 2)
        return pltpu.make_async_copy(self.out.at[s], self.h_ref.at[pl.ds(pl.multiple_of(i * TOKENS, TOKENS), TOKENS)], self.out_sem.at[s])

    def store_own(self, b):
        return pltpu.make_async_copy(self.out.at[b], self.emb_ref.at[b], self.out_sem.at[b])

    def tile(self, slot, j):
        return self.xs[slot, j * 8:(j + 1) * 8, :]

    def fetch(self, slot, seq, t, row_of):
        first = (lax.shift_right_logical(t, 7) * 2 + seq) * 128 + lax.bitwise_and(t, 127)
        for r in range(8):
            self.xs[slot, pl.ds(r, self.T, stride=8), :] = row_of(self.at[first + r]).astype(jnp.float32)

    def lanes(self, j):
        return slice(j * 128, (j + 1) * 128)

    def norm(self, i, g, lane_slot, row_of):
        T, xs = self.T, self.xs
        inv = 1.0 / (T * 128)
        t = pl.multiple_of(g * 16, 16)
        out = []
        for half in range(2):
            slot = lane_slot * 2 + half
            self.fetch(slot, self.core, i * TOKENS + g * 16 + half * 8, row_of)
            p = self.pos.at[lax.rem(i, 2), pl.ds(t, 16), :]
            s = None
            for j in range(T):
                e = (self.tile(slot, j) + p[half * 8:half * 8 + 8, self.lanes(j)].astype(jnp.float32)).astype(jnp.bfloat16).astype(jnp.float32)
                xs[slot, j * 8:(j + 1) * 8, :] = e
                s = e if s is None else s + e
            mean = jnp.broadcast_to(jnp.sum(s, axis=1, keepdims=True) * inv, (8, 128))
            s = None
            for j in range(T):
                c = self.tile(slot, j) - mean
                s = c * c if s is None else s + c * c
            var = jnp.sum(s, axis=1, keepdims=True) * inv
            out.append((slot, mean, jnp.broadcast_to(lax.rsqrt(var + EPS), (8, 128))))
        for j in range(T):
            y = [(self.tile(slot, j) - mean) * rs * self.gain_ref[:, self.lanes(j)] + self.bias_ref[:, self.lanes(j)] for slot, mean, rs in out]
            self.out[lax.rem(i, 2), pl.ds(t, 16), self.lanes(j)] = jnp.concatenate(y, axis=0).astype(jnp.bfloat16)

    def embed(self, b, g, lane_slot, row_of):
        t = pl.multiple_of(g * 16, 16)
        for half in range(2):
            self.fetch(lane_slot * 2 + half, b, self.me * TOKENS + t + half * 8, row_of)
        p = self.pos.at[self.blocks % 2, pl.ds(t, 16), :]
        for j in range(self.T):
            e = jnp.concatenate([self.tile(lane_slot * 2, j), self.tile(lane_slot * 2 + 1, j)], axis=0) + p[:, self.lanes(j)].astype(jnp.float32)
            self.out[b, pl.ds(t, 16), self.lanes(j)] = e.astype(jnp.bfloat16)

    def run(self, low, high, row_of):
        @pl.loop(low, high)
        def _(i):
            self.load(i).wait()
            self.load(i + 1).start()

            @pl.when(i >= 2)
            def _():
                self.store(i - 2).wait()

            @pl.loop(0, TOKENS // 64)
            def _(g):
                for j in range(4):
                    self.norm(i, g * 4 + j, j, row_of)
            self.store(i).start()

    def close(self, row_of):
        self.load(self.blocks).wait()
        for b in range(2):
            self.store(self.blocks - 2 + b).wait()

            @pl.loop(0, TOKENS // 64)
            def _(g):
                for j in range(4):
                    self.embed(b, g * 4 + j, j, row_of)
            self.store_own(b).start()
        for b in range(2):
            self.store_own(b).wait()

    @staticmethod
    def scratch(D):
        return [pltpu.VMEM((2, TOKENS, D), jnp.bfloat16), pltpu.VMEM((8, D // 128 * 8, 128), jnp.float32), pltpu.VMEM((2, TOKENS, D), jnp.bfloat16),
                pltpu.SemaphoreType.DMA((2,)), pltpu.SemaphoreType.DMA((2,))]


def broadcast_kernel(n, soon, early, at, rows_ref, pos_hbm, gain_ref, bias_ref, v_ref, w_ref, b_ref,
                     h_ref, emb_ref, minus_ref, plus_ref, w_par_ref, b_par_ref, rest_ref, ua, ub, *rest):
    send_sem, recv_sem, pass_send, pass_recv, vbuf, vsem = rest[-6:]
    q = Peers(n)
    me = q.me
    work = Norm(me, q.core, at, pos_hbm, gain_ref, bias_ref, h_ref, emb_ref, *rest[:-6])
    cap = rows_ref.shape[0]
    late = cap - soon
    spans = ((ua, soon, 0, soon // 2), (ua, soon, soon // 2, soon // 2), (ub, late, 0, late))

    def own(p):
        ref, _, low, size = spans[p]
        return rows_ref.at[pl.ds(low + (soon if ref is ub else 0), size)]

    def place(d, p):
        ref, per, low, size = spans[p]
        return ref.at[pl.ds(d * per + low, size)]

    moves = Spread(q, own, place, send_sem, recv_sem)
    left = vbuf.shape[0]
    last_rows = v_ref.at[pl.ds(v_ref.shape[0] - left - minus_ref.shape[0], minus_ref.shape[0])]
    rest_in = pltpu.make_async_copy(v_ref.at[pl.ds(v_ref.shape[0] - left, left)], vbuf, vsem)
    rest_out = pltpu.make_async_copy(vbuf, rest_ref, vsem)
    passed = [pltpu.make_async_remote_copy(src_ref=src, dst_ref=dst, send_sem=pass_send.at[i], recv_sem=pass_recv.at[i], device_id={"tp": to}, device_id_type=MESH)
              for i, (src, dst, to) in enumerate(((last_rows, minus_ref, q.plus), (last_rows, plus_ref, q.minus), (w_ref, w_par_ref, q.partner), (b_ref, b_par_ref, q.partner)))]
    work.load(0).start()
    q.greet((q.plus, q.minus, q.partner))
    moves.begin(0)
    moves.begin(1)
    for ref, low, size in ((ua, 0, soon), (ub, soon, late)):
        @pl.loop(0, size // 8)
        def _(k):
            for r in range(8):
                ref[me * size + k * 8 + r] = rows_ref[low + k * 8 + r]
    for c in passed[2:]:
        c.start()
    rest_in.start()
    rest_in.wait()
    rest_out.start()
    moves.turn(0)
    moves.turn(1)
    moves.begin(2)
    for p in range(2):
        moves.last(p)
    for p in range(2):
        moves.finish(p)

    def first(i):
        return ua[i]

    def any_(i):
        here = i < n * soon
        a, b = ua[jnp.minimum(i, n * soon - 1)], ub[jnp.maximum(i - n * soon, 0)]
        return jnp.where(here, a.astype(jnp.float32), b.astype(jnp.float32))

    blocks = early // TOKENS
    work.run(0, blocks - 2, first)
    moves.turn(2)
    for c in passed[:2]:
        c.start()
    work.run(blocks - 2, blocks, first)
    moves.last(2)
    moves.finish(2)
    work.run(blocks, work.blocks, any_)
    work.close(any_)
    for c in passed:
        c.wait()
    rest_out.wait()


def broadcast(n, soon, early, at, rows, pos, gain, bias, v, last, left, w, b, cid=3):
    seq, D = pos.shape
    cap, T, L = rows.shape
    A = pl.BlockSpec(memory_space=pl.ANY)
    V = pl.BlockSpec(memory_space=pltpu.VMEM)
    sems = pltpu.SemaphoreType.DMA((Spread.CHANNELS, 3))
    of = lambda r: jax.ShapeDtypeStruct((r, D), v.dtype)
    return pl.pallas_call(
        functools.partial(broadcast_kernel, n, soon, early),
        out_shape=(jax.ShapeDtypeStruct((seq, D), jnp.bfloat16), jax.ShapeDtypeStruct((2, seq // n, D), jnp.bfloat16),
                   of(last), of(last), jax.ShapeDtypeStruct(w.shape, w.dtype), jax.ShapeDtypeStruct(b.shape, b.dtype), of(left)),
        grid_spec=pltpu.PrefetchScalarGridSpec(
            num_scalar_prefetch=1, grid=(), in_specs=[V, A, V, V, A, A, V], out_specs=(A, A, A, A, A, V, A),
            scratch_shapes=[pltpu.VMEM((n * soon, T, L), rows.dtype), pltpu.VMEM((n * (cap - soon), T, L), rows.dtype), *Norm.scratch(D), sems, sems, *[pltpu.SemaphoreType.DMA((4,))] * 2, pltpu.VMEM((left, D), v.dtype), pltpu.SemaphoreType.DMA]),
        compiler_params=pltpu.CompilerParams(vmem_limit_bytes=VMEM, collective_id=cid, has_side_effects=True),
        name="broadcast",
    )(at, rows, pos, gain, bias, v, w, b)


def norm_kernel(at, x_hbm, pos_hbm, gain_ref, bias_ref, h_ref, emb_ref, x, sem, *rest):
    me = lax.axis_index("tp")
    work = Norm(me, lax.rem(me, 2), at, pos_hbm, gain_ref, bias_ref, h_ref, emb_ref, *rest)
    work.load(0).start()
    c = pltpu.make_async_copy(x_hbm, x, sem)
    c.start()
    c.wait()
    work.run(0, work.blocks, lambda i: x[i])
    work.close(lambda i: x[i])


def norm(n, at, x, pos, gain, bias):
    seq, D = pos.shape
    A = pl.BlockSpec(memory_space=pl.ANY)
    V = pl.BlockSpec(memory_space=pltpu.VMEM)
    return pl.pallas_call(
        norm_kernel,
        out_shape=(jax.ShapeDtypeStruct((seq, D), jnp.bfloat16), jax.ShapeDtypeStruct((2, seq // n, D), jnp.bfloat16)),
        grid_spec=pltpu.PrefetchScalarGridSpec(
            num_scalar_prefetch=1, grid=(), in_specs=[A, A, V, V], out_specs=(A, A),
            scratch_shapes=[pltpu.VMEM(x.shape, x.dtype), pltpu.SemaphoreType.DMA, *Norm.scratch(D)]),
        compiler_params=pltpu.CompilerParams(vmem_limit_bytes=VMEM),
        name="norm",
    )(at, x, pos, gain, bias)


def project_kernel(chunk, wa_hbm, wb_hbm, ba_ref, bb_ref, emb_hbm, h_ref, qkv_ref, emb_out, w, bc, emb, wsem, esem):
    step = pl.program_id(0)
    core = lax.rem(lax.axis_index("tp"), 2)
    M = wa_hbm.shape[0]
    tb = h_ref.shape[0]

    def load(k):
        return pltpu.make_async_copy((wa_hbm, wb_hbm)[k], w.at[lax.rem(core + k, 2)], wsem.at[lax.rem(core + k, 2)])

    def loaded(k):
        return pltpu.make_async_copy(wa_hbm, w.at[k], wsem.at[k])

    @pl.when(step == 0)
    def _():
        for k in range(2):
            load(k).start()
        pltpu.make_async_copy(emb_hbm, emb, esem).start()
        _, H, E = ba_ref.shape
        for k, b in enumerate((ba_ref, bb_ref)):
            for r in range(3 * H):
                bc[lax.rem(core + k, 2), r * E:(r + 1) * E, :] = jnp.broadcast_to(b[r // H, r % H:r % H + 1, :], (128, E)).T

    @pl.when(step == 1)
    def _():
        pltpu.make_async_copy(emb_hbm, emb, esem).wait()
        pltpu.make_async_copy(emb, emb_out, esem).start()

    @pl.when(step == pl.num_programs(0) - 1)
    def _():
        pltpu.make_async_copy(emb, emb_out, esem).wait()

    for k in range(2):
        @pl.when(step == 0)
        def _():
            loaded(k).wait()
        for m in range(0, M, chunk):
            o = lax.dot_general(w[k, m:m + chunk, :], h_ref[...], (((1,), (1,)), ((), ())), preferred_element_type=jnp.float32)
            b = jnp.concatenate([bc[k, m:m + chunk, :]] * (tb // 128), axis=1)
            qkv_ref[k, m:m + chunk, :] = (o + b).astype(jnp.bfloat16)


def project(h, emb, wa, wb, ba, bb, tb=512, chunk=384):
    seq, D = h.shape
    M = wa.shape[0]
    A = pl.BlockSpec(memory_space=pl.ANY)
    one = lambda shape: pl.BlockSpec(shape, lambda i: (0,) * len(shape), pipeline_mode=pl.Buffered(1))
    return pl.pallas_call(
        functools.partial(project_kernel, chunk),
        out_shape=(jax.ShapeDtypeStruct((2, M, seq), jnp.bfloat16), jax.ShapeDtypeStruct(emb.shape, emb.dtype)),
        grid=(seq // tb,),
        in_specs=[A, A, one(ba.shape), one(bb.shape), A, pl.BlockSpec((tb, D), lambda i: (i, 0))],
        out_specs=(pl.BlockSpec((2, M, tb), lambda i: (0, 0, i)), A),
        scratch_shapes=[pltpu.VMEM((2, M, D), wa.dtype), pltpu.VMEM((2, M, 128), jnp.float32), pltpu.VMEM(emb.shape, emb.dtype), pltpu.SemaphoreType.DMA((2,)), pltpu.SemaphoreType.DMA],
        compiler_params=pltpu.CompilerParams(vmem_limit_bytes=VMEM),
        cost_estimate=pl.CostEstimate(flops=4 * seq * M * D, bytes_accessed=50 * 2**20, transcendentals=0),
        name="project",
    )(wa, wb, ba, bb, emb, h)


def attend_kernel(n, scale, qb, nb, early, where, qkv_ref, emb_hbm, bias_ref, *refs):
    pieces, (out_ref, kk, vv, sc, ctx, got, w, a, acc, emb, load_sem, pass_send, pass_recv, emb_sem, send_sem, recv_sem, turn_send, turn_recv) = refs[:len(where)], refs[len(where):]
    E, S = qkv_ref.shape[3:]
    heads = got.shape[1] // E
    N = S // qb
    c = scale * 1.4426950408889634
    q = Peers(n)
    me, core = q.me, q.core
    head = pl.program_id(0)
    cut = early * E // 256 * 256
    owners = {0: me, 1: q.plus, 2: q.opp, -1: q.minus}

    def loads():
        cs = []
        for i, (ref, (away, low)) in enumerate(zip(pieces, where)):
            dst = w.at[owners[away], pl.ds(low, ref.shape[0])]
            cs.append(pltpu.make_async_copy(ref, dst, load_sem.at[i]))
            cs.append(pltpu.make_async_remote_copy(src_ref=ref, dst_ref=dst, send_sem=pass_send.at[i], recv_sem=pass_recv.at[i], device_id={"tp": q.partner}, device_id_type=MESH))
        return cs

    rest = pieces[-1].shape[0]
    half = rest // 2

    def across(i, owner, src, to, sem):
        dst = w.at[owner, pl.ds(w.shape[1] - rest + i * half, half)]
        return pltpu.make_async_remote_copy(src_ref=dst if src is None else src.at[pl.ds(i * half, half)], dst_ref=dst, send_sem=turn_send.at[sem], recv_sem=turn_recv.at[sem],
                                            device_id={"tp": to}, device_id_type=MESH)

    passing = ((q.minus, pieces[-2], q.plus), (q.plus, pieces[-1], q.minus))

    def send(h, s):
        to = lax.rem(me + s, n)
        return pltpu.make_async_remote_copy(src_ref=ctx.at[h, to], dst_ref=got.at[me, pl.ds(pl.multiple_of(h * E, 32), E)],
                                            send_sem=send_sem.at[s], recv_sem=recv_sem.at[lax.div(h, early), s], device_id={"tp": to}, device_id_type=MESH)

    load_emb = pltpu.make_async_copy(emb_hbm, emb, emb_sem)

    @pl.when(head == 0)
    def _():
        q.greet([lax.rem(me + s, n) for s in range(1, n)])
        for i, (owner, src, to) in enumerate(passing):
            across(i, owner, src, to, i).start()
        vv[E:, :] = jnp.where(lax.broadcasted_iota(jnp.int32, (vv.shape[0] - E, S), 0) == 0, 1.0, 0.0).astype(jnp.bfloat16)

    @pl.when(head > 0)
    def _():
        for s in range(1, n):
            send(head - 1, s).start()

    @pl.when(head == 1)
    def _():
        for c_ in loads():
            c_.start()
        load_emb.start()

    @pl.when(head == 4)
    def _():
        for i in range(2):
            across(i, q.opp, None, q.partner, i).wait_recv()
            across(i, q.opp, None, q.partner, 2 + i).start()

    for t in range(0, S, 128):
        kk[t:t + 128, :] = qkv_ref[0, 1, 0, :, t:t + 128].astype(jnp.float32).T.astype(jnp.bfloat16)
    vv[0:E, :] = qkv_ref[0, 2, 0]
    keep = lax.broadcasted_iota(jnp.int32, (qb, qb), 0) <= lax.broadcasted_iota(jnp.int32, (qb, qb), 1)

    def scores(i, k, m):
        s = jnp.dot(kk[k * qb:(k + 1) * qb, :], qkv_ref[0, 0, 0, :, i * qb:(i + 1) * qb], preferred_element_type=jnp.float32)
        if k == i:
            s = jnp.where(keep, s, -jnp.inf)
        sc[i % 2, k * qb:(k + 1) * qb, :] = s
        top = jnp.max(s.reshape(qb // 8, 8, qb), axis=0)
        return top if m is None else jnp.maximum(m, top)

    def weigh(i, k, mc, o):
        s = sc[i % 2, k * qb:(k + 1) * qb, :]
        p = jnp.exp2(s * c - mc).astype(jnp.bfloat16)
        d = jnp.dot(vv[:, k * qb:(k + 1) * qb], p, preferred_element_type=jnp.float32)
        return d if o is None else o + d

    m = scores(0, 0, None)
    for i in range(N):
        mc = jnp.max(m, axis=0, keepdims=True) * c
        o = m = None
        for k in range(i + 2):
            if i + 1 < N:
                m = scores(i + 1, k, m)
            if k <= i:
                o = weigh(i, k, mc, o)
        ctx[head, i] = (o[0:E] * (1.0 / o[E:E + 1])).astype(jnp.bfloat16)
    got[me, pl.ds(pl.multiple_of(head * E, 32), E), :] = ctx[head, me]

    @pl.when(head == heads - 1)
    def _():
        for s in range(1, n):
            send(head, s).start()
        K = got.shape[1]

        def arrive(group, low, high):
            for s in range(1, n):
                fr = lax.rem(me - s + n, n)
                r = got.at[fr, pl.ds(low, high - low)]
                pltpu.make_async_remote_copy(src_ref=r, dst_ref=r, send_sem=send_sem.at[s], recv_sem=recv_sem.at[group, s], device_id={"tp": fr}, device_id_type=MESH).wait_recv()

        def turn_over(low, high):
            for s in range(n):
                for k in range(low, high, 128):
                    for t in range(0, qb, 128):
                        at = s // 2 * (high - low) + (k - low) + (n // 2) * low
                        a[(s % 2) * qb + t:(s % 2) * qb + t + 128, at:at + 128] = got[s, k:k + 128, t:t + 128].astype(jnp.float32).T.astype(jnp.bfloat16)

        def part(low, high, cols):
            rows = [w[2 * i:2 * i + 2, :, cols].reshape(K, nb)[low:high] for i in range(n // 2)]
            return jnp.dot(a[:, n // 2 * low:n // 2 * high], jnp.concatenate(rows, axis=0), preferred_element_type=jnp.float32)

        arrive(0, 0, early * E)
        turn_over(0, cut)
        for c_ in loads():
            c_.wait()
        load_emb.wait()
        for i, (owner, src, to) in enumerate(passing):
            across(i, owner, src, to, i).wait_send()
            across(i, q.other(q.opp), None, q.partner, 2 + i).wait()

        @pl.loop(0, w.shape[2] // nb)
        def _(j):
            cols = pl.ds(pl.multiple_of(j * nb, nb), nb)
            acc[:, cols] = part(0, cut, cols) + bias_ref[:, cols]

        arrive(1, early * E, K)
        turn_over(cut, K)

        @pl.loop(0, w.shape[2] // nb)
        def _(j):
            cols = pl.ds(pl.multiple_of(j * nb, nb), nb)
            o = part(cut, K, cols) + acc[:, cols]
            for b in range(2):
                out_ref[b, :, cols] = (emb[b, :, cols].astype(jnp.float32) + o[b * qb:(b + 1) * qb]).astype(jnp.bfloat16)

        for s in range(1, n):
            r = got.at[lax.rem(me - s + n, n)]
            pltpu.make_async_remote_copy(src_ref=r, dst_ref=r, send_sem=send_sem.at[s], recv_sem=recv_sem.at[0, s], device_id={"tp": q.partner}, device_id_type=MESH).wait_send()


def attend(n, qkv, pieces, where, emb, bias, early=6, nb=1024, cid=1, qb=256):
    heads, E, S = 2 * qkv.shape[2], *qkv.shape[3:]
    H = heads // 2
    D = emb.shape[2]
    A = pl.BlockSpec(memory_space=pl.ANY)
    one = lambda shape: pl.BlockSpec(shape, lambda h: (0,) * len(shape), pipeline_mode=pl.Buffered(1))
    bf = jnp.bfloat16
    return pl.pallas_call(
        functools.partial(attend_kernel, n, E ** -0.5, qb, nb, early, where),
        out_shape=jax.ShapeDtypeStruct(emb.shape, bf),
        grid=(heads,),
        in_specs=[pl.BlockSpec((1, 3, 1, E, S), lambda h: (h // H, 0, h % H, 0, 0)), A, one(bias.shape)] + [A] * len(pieces),
        out_specs=one(emb.shape),
        scratch_shapes=[pltpu.VMEM((S, E), bf), pltpu.VMEM((E + 16, S), bf), pltpu.VMEM((2, S, qb), jnp.float32),
                        pltpu.VMEM((heads, n, E, qb), bf), pltpu.VMEM((n, heads * E, qb), bf), pltpu.VMEM((n, H * E, D), bf), pltpu.VMEM((2 * qb, n * H * E), bf),
                        pltpu.VMEM((2 * qb, D), jnp.float32), pltpu.VMEM(emb.shape, bf),
                        *[pltpu.SemaphoreType.DMA((len(pieces),))] * 3, pltpu.SemaphoreType.DMA, pltpu.SemaphoreType.DMA((n,)), pltpu.SemaphoreType.DMA((2, n)), *[pltpu.SemaphoreType.DMA((4,))] * 2],
        compiler_params=pltpu.CompilerParams(collective_id=cid, has_side_effects=True, vmem_limit_bytes=VMEM),
        name="attend",
    )(qkv, emb, bias, *pieces)


CAP = 264
SOON, EARLY = 176, 1024


def place_kernel(code_ref, u_ref, x_ref, out_ref, sem):
    @pl.loop(0, code_ref.shape[0])
    def _(t):
        c = code_ref[t]

        @pl.when(c >= 0)
        def _():
            copy = pltpu.make_async_copy(u_ref.at[c], out_ref.at[t], sem)
            copy.start()
            copy.wait()


def place(at, u, x):
    A = pl.BlockSpec(memory_space=pl.ANY)
    return pl.pallas_call(
        place_kernel,
        out_shape=jax.ShapeDtypeStruct(x.shape, x.dtype),
        grid_spec=pltpu.PrefetchScalarGridSpec(num_scalar_prefetch=1, grid=(), in_specs=[A, A], out_specs=A, scratch_shapes=[pltpu.SemaphoreType.DMA]),
        input_output_aliases={2: 0},
        name="place",
    )(at, u, x)


def solution(mesh):
    n = mesh.shape["tp"]
    def local_step(token_ids, word_shard, pos_table, ln_gain, ln_bias, w_qkv, b_qkv, w_out, b_out):
        me = lax.axis_index("tp")
        core = lax.rem(me, 2)
        seq, D = pos_table.shape
        H, E = w_qkv.shape[2:]
        shard_rows = word_shard.shape[0]
        w_own = jnp.transpose(w_qkv, (1, 2, 3, 0)).reshape(3 * H * E, D)
        v_own = w_out.reshape(H * E, D)
        ring = lambda step: [(d, (d + 2 * step) % n) for d in range(n)]
        send = lambda x, step: lax.ppermute(x, "tp", ring(step))
        v_head = w_out[:2].reshape(2 * E, D)
        minus0, plus0 = send(v_head, 1), send(v_head, -1)
        blk = seq // n
        gain, bias = ln_gain[None], ln_bias[None]
        code, at, counts, mine = pick(n, shard_rows, CAP, SOON, EARLY, token_ids, word_shard)
        mine, minus0, plus0 = lax.optimization_barrier((mine, minus0, plus0))
        h, embed, minus1, plus1, w_par, b_par, v_tail = broadcast(n, SOON, EARLY, at.reshape(-1), mine, pos_table, gain, bias, v_own, (H - 3) * E, E, w_own, b_qkv)
        counts, h = lax.optimization_barrier((counts, h))

        rounds = jnp.where((counts[0, 0] > CAP) | (counts[1, 0] > SOON), (counts[0, 0] + CAP - 1) // CAP, 0)
        total = max(n * CAP, seq + blk)

        def by_token(x):
            return x.reshape(seq // 128, 2, 128).transpose(1, 0, 2)

        def wanted(x):
            own = lax.dynamic_index_in_dim(x, core, 0, keepdims=False)
            other = lax.dynamic_index_in_dim(x, 1 - core, 0, keepdims=False)
            return jnp.concatenate([own, lax.dynamic_slice_in_dim(other, me * blk, blk)])

        def more(carry):
            def one_round(carry):
                r, x = carry
                codes = by_token(code).reshape(2, seq)
                slot = codes % SPAN - r * CAP
                hit = (slot >= 0) & (slot < CAP)
                here = jnp.where(hit & (codes // SPAN == me), slot, -1).reshape(-1)
                ids = token_ids.reshape(-1) - me * shard_rows
                chosen = jnp.max(jnp.where(here[None, :] == jnp.arange(CAP)[:, None], ids[None, :], 0), axis=1)
                v = gather_all(n, rows(CAP, chosen, word_shard), total)
                return r + 1, place(wanted(jnp.where(hit, codes // SPAN * CAP + slot, -1)), v, x)

            x = jnp.zeros((total,) + mine.shape[1:], mine.dtype)
            _, x = lax.while_loop(lambda c: c[0] < rounds, one_round, (jnp.int32(0), x))
            t = jnp.arange(seq, dtype=jnp.int32)
            t = jnp.stack([jnp.where(core == b, t, jnp.clip(t - me * blk, 0, blk - 1) + seq) for b in range(2)])
            t = t.reshape(2, seq // 128, 128).transpose(1, 0, 2).reshape(-1)
            return (jnp.int32(0),) + tuple(norm(n, t, x, pos_table, gain, bias))

        _, h, embed = lax.while_loop(lambda c: c[0] > 0, more, (rounds, h, embed))

        minus0, h = lax.optimization_barrier((minus0, h))
        minus2, plus2, opp0, opp1 = send(v_tail, 1), send(v_tail, -1), send(minus0, 1), send(plus1, -1)
        pieces = [v_own, minus0, plus0, minus1, plus1, opp0, opp1, minus2, plus2]
        where = ((0, 0), (-1, 0), (1, 0), (-1, 2 * E), (1, 2 * E), (2, 0), (2, 2 * E), (-1, (H - 1) * E), (1, (H - 1) * E))
        qkv, embed = project(h, embed, w_own, w_par, b_qkv, b_par)
        resid_out = attend(n, qkv.reshape(2, 3, H, E, seq), pieces, where, embed, b_out[None])
        return resid_out, embed

    in_specs = (P("dp", None), P("tp", None), P(None, None), P(None), P(None), P(None, None, "tp", None), P(None, "tp", None), P("tp", None, None), P(None))
    out_specs = (P("dp", "tp", None), P("dp", "tp", None))
    return jax.shard_map(local_step, mesh=mesh, in_specs=in_specs, out_specs=out_specs, check_vma=False)
```
